16 devices in a mesh: dz: 2 (over z), dy: 2 (over y), dx: 4 (over x, core).
Axes of the slice: x: 2, y: 2, z: 2, core: 2. Of those that a mesh axis runs over, the one named last changes fastest.
Arguments:
- g_emb: float32 [16, 2048, 768], P(('dz', 'dy', 'dx'))
- g_attn: float32 [16, 1, 4, 768, 768], P(('dz', 'dy', 'dx'))
- g_in: float32 [16, 1, 768, 2048], P(('dz', 'dy', 'dx'))
- g_out: float32 [16, 1, 2048, 768], P(('dz', 'dy', 'dx'))
- g_vecd: float32 [16, 1, 9, 768], P(('dz', 'dy', 'dx'))
- g_vecf: float32 [16, 1, 2048], P(('dz', 'dy', 'dx'))
- opt_m: float32 [7088128], P(('dz', 'dy', 'dx'))
- opt_v: float32 [7088128], P(('dz', 'dy', 'dx'))
- master: float32 [7088128], P(('dz', 'dy', 'dx'))
- tok_ids: int32 [262144], P(('dz', 'dy', 'dx'))
- act_in: bfloat16 [262144, 768], P(('dz', 'dy', 'dx'))
Outputs:
- output 1: float32 [7088128], P(('dz', 'dy', 'dx'))
- output 2: float32 [7088128], P(('dz', 'dy', 'dx'))
- output 3: float32 [7088128], P(('dz', 'dy', 'dx'))
- output 4: bfloat16 [2048, 768], replicated
- output 5: bfloat16 [1, 4, 768, 768], replicated
- output 6: bfloat16 [1, 768, 2048], replicated
- output 7: bfloat16 [1, 2048, 768], replicated
- output 8: bfloat16 [1, 9, 768], replicated
- output 9: bfloat16 [1, 2048], replicated
- output 10: bfloat16 [262144, 768], P(('dz', 'dy', 'dx'))
All inputs are finite; a program needn't handle non-finite values.
Results may differ from the reference program's by a relative error of at most 0.001.
Values are sent between devices in bfloat16 or wider.
A program may use at most 1 GiB of HBM per device.

```python
import math
import jax
import jax.numpy as jnp
from jax import lax

D = 768
FF = 2048
LAYERS = 1
VOCAB = 2048
TOKENS_DEV = 16384
DEVICES = 16
ADAM_STEP = 2

LEARN_RATE = 0.002
BETA_ONE = 0.9
BETA_TWO = 0.95
ADAM_EPS = 1e-8
PARAM_COUNT = VOCAB * D + LAYERS * (4 * D * D + 2 * D * FF + 9 * D + FF)
PADDED_COUNT = -(-PARAM_COUNT // (128 * DEVICES)) * (128 * DEVICES)
TENSOR_SHAPES = [(VOCAB, D), (LAYERS, 4, D, D), (LAYERS, D, FF), (LAYERS, FF, D), (LAYERS, 9, D), (LAYERS, FF)]
ARG_NAMES = ["g_emb", "g_attn", "g_in", "g_out", "g_vecd", "g_vecf"]


def setup_inputs(seed: int = 0) -> dict:
    rand_keys = jax.random.split(jax.random.key(seed), 12)
    dev_scale = jax.random.uniform(rand_keys[0], (DEVICES,), jnp.float32, 0.5, 1.5) * math.sqrt(DEVICES)
    inputs = {}
    for tensor_index, tensor_shape in enumerate(TENSOR_SHAPES):
        grad_noise = jax.random.normal(rand_keys[1 + tensor_index], (DEVICES,) + tensor_shape, jnp.float32)
        inputs[ARG_NAMES[tensor_index]] = grad_noise * dev_scale.reshape((DEVICES,) + (1,) * len(tensor_shape))
    weight_scales = [D ** -0.5, D ** -0.5, D ** -0.5, FF ** -0.5, 0.2, 0.3]
    scale_parts = [jnp.full((math.prod(tensor_shape),), weight_scale, jnp.float32) for tensor_shape, weight_scale in zip(TENSOR_SHAPES, weight_scales)]
    scale_parts.append(jnp.full((PADDED_COUNT - PARAM_COUNT,), 0.1, jnp.float32))
    m_noise = jax.random.normal(rand_keys[7], (PADDED_COUNT,), jnp.float32)
    v_noise = jax.random.normal(rand_keys[8], (PADDED_COUNT,), jnp.float32)
    w_noise = jax.random.normal(rand_keys[9], (PADDED_COUNT,), jnp.float32)
    inputs["opt_m"] = 0.1 * m_noise
    inputs["opt_v"] = 0.05 * (v_noise * v_noise + 0.25)
    inputs["master"] = w_noise * jnp.concatenate(scale_parts)
    tok_ids = jax.random.randint(rand_keys[10], (DEVICES * TOKENS_DEV,), 0, VOCAB, jnp.int32)
    inputs["tok_ids"] = tok_ids.at[0].set(0).at[1].set(VOCAB - 1)
    inputs["act_in"] = jax.random.normal(rand_keys[11], (DEVICES * TOKENS_DEV, D), jnp.float32).astype(jnp.bfloat16)
    return inputs


def ffn_block(wb_emb, w_in, b_in, w_out, b_out, tok_ids, act_in):
    emb_rows = jnp.take(wb_emb, tok_ids, axis=0).astype(jnp.float32)
    hidden = (emb_rows * math.sqrt(D) + act_in.astype(jnp.float32)).astype(jnp.bfloat16)
    pre_act = jnp.dot(hidden, w_in, preferred_element_type=jnp.float32) + b_in.astype(jnp.float32)
    inner_act = jax.nn.gelu(pre_act, approximate=True).astype(jnp.bfloat16)
    return (jnp.dot(inner_act, w_out, preferred_element_type=jnp.float32) + b_out.astype(jnp.float32)).astype(jnp.bfloat16)


def reference(g_emb, g_attn, g_in, g_out, g_vecd, g_vecf, opt_m, opt_v, master, tok_ids, act_in):
    grad_list = [g_emb, g_attn, g_in, g_out, g_vecd, g_vecf]
    flat_grad = jnp.concatenate([jnp.sum(grad_arr, axis=0).reshape(-1) for grad_arr in grad_list]) / DEVICES
    flat_grad = jnp.pad(flat_grad, (0, PADDED_COUNT - PARAM_COUNT))
    m_new = BETA_ONE * opt_m + (1.0 - BETA_ONE) * flat_grad
    v_new = BETA_TWO * opt_v + (1.0 - BETA_TWO) * flat_grad * flat_grad
    m_hat = m_new / (1.0 - BETA_ONE ** ADAM_STEP)
    v_hat = v_new / (1.0 - BETA_TWO ** ADAM_STEP)
    w_new = master - LEARN_RATE * m_hat / (jnp.sqrt(v_hat) + ADAM_EPS)
    w_half = w_new.astype(jnp.bfloat16)
    pieces = []
    offset = 0
    for tensor_shape in TENSOR_SHAPES:
        elem_count = math.prod(tensor_shape)
        pieces.append(w_half[offset:offset + elem_count].reshape(tensor_shape))
        offset = offset + elem_count
    wb_emb, wb_attn, wb_in, wb_out, wb_vecd, wb_vecf = pieces
    tok_blocks = tok_ids.reshape(DEVICES, TOKENS_DEV)
    act_blocks = act_in.reshape(DEVICES, TOKENS_DEV, D)

    def token_block(tok_pair):
        return ffn_block(wb_emb, wb_in[0], wb_vecf[0], wb_out[0], wb_vecd[0, 8], tok_pair[0], tok_pair[1])

    y_blocks = lax.map(token_block, (tok_blocks, act_blocks))
    y_out = y_blocks.reshape(DEVICES * TOKENS_DEV, D)
    return (m_new, v_new, w_new, wb_emb, wb_attn, wb_in, wb_out, wb_vecd, wb_vecf, y_out)
```

```python
import functools
import math

import jax
import jax.numpy as jnp
from jax import lax
from jax.experimental import pallas as pl
from jax.experimental.pallas import tpu as pltpu
from jax.sharding import PartitionSpec as P

LEARN_RATE = 0.002
BETA_ONE = 0.9
BETA_TWO = 0.95
ADAM_EPS = 1e-8
ADAM_STEP = 2
AXES = ("dz", "dy", "dx")
GRAD_RANKS = (3, 5, 4, 4, 4, 3)
MESH = pl.DeviceIdType.MESH

D = 768
FF = 2048
VOCAB = 2048
DEVICES = 16
LANES = 128
SHARD = 3461
PAD = 3472
PART_START = (0, 1152, 2304)
PART_ROWS = (1152, 1152, 1168)
PART_MAX = 1168
VMEM_MAX = 67_000_000

TENSORS = (
    (VOCAB, D, 0),
    (4 * D, D, VOCAB * D // LANES),
    (D, FF, (VOCAB * D + 4 * D * D) // LANES),
    (FF, D, (VOCAB * D + 4 * D * D + D * FF) // LANES),
)
VEC_BASE = (VOCAB * D + 4 * D * D + 2 * D * FF) // LANES
VEC_ROWS = DEVICES * SHARD - VEC_BASE


def flat_chunks():
    chunks = []
    for index, (rows, cols, base) in enumerate(TENSORS):
        step = 256 if cols == D else 128
        for start in range(0, rows, step):
            chunks.append((index, start, step))
    return chunks


def flatten_kernel(g_emb, g_attn, g_in, g_out, vec, flat_out, s_emb, s_attn, s_in, s_out, s_vec, flat, in_sem, out_sem):
    sources = (g_emb, g_attn, g_in, g_out)
    stages = (s_emb, s_attn, s_in, s_out)
    chunks = flat_chunks()

    def load(k):
        index, start, step = chunks[k]
        return pltpu.make_async_copy(
            sources[index].at[pl.ds(start, step)], stages[index].at[pl.ds(start, step)], in_sem.at[k])

    vec_load = pltpu.make_async_copy(vec, s_vec, in_sem.at[len(chunks)])
    for k in range(len(chunks)):
        load(k).start()
    vec_load.start()

    def put(owner):
        return pltpu.make_async_copy(flat.at[pl.ds(owner * PAD, PAD)], flat_out.at[owner], out_sem.at[owner])

    sent = 0
    for k, (index, start, step) in enumerate(chunks):
        _, cols, base = TENSORS[index]
        groups = cols // LANES
        stage = stages[index]
        load(k).wait()
        tile = start // 8
        last = (start + step) // 8
        while tile < last:
            first_row = base + tile * 8 * groups
            owner = first_row // SHARD
            fit = (SHARD * (owner + 1) - first_row) // (8 * groups)
            run = min(fit, last - tile)
            if run > 0:
                shift = base + (PAD - SHARD) * owner

                def body(t, carry, shift=shift, groups=groups, stage=stage):
                    row = pl.multiple_of(t * 8, 8)
                    for j in range(groups):
                        flat[pl.ds(shift + row * groups + j, 8, stride=groups), :] = (
                            stage[pl.ds(row, 8), j * LANES:(j + 1) * LANES])
                    return carry

                lax.fori_loop(tile, tile + run, body, 0, unroll=2)
                tile = tile + run
            else:
                for i in range(8):
                    for j in range(groups):
                        q = first_row + i * groups + j
                        p = q + (PAD - SHARD) * (q // SHARD)
                        flat[p:p + 1, :] = stage[tile * 8 + i:tile * 8 + i + 1, j * LANES:(j + 1) * LANES]
                tile = tile + 1
        done = (base + last * 8 * groups) // SHARD
        while sent < min(done, DEVICES - 1):
            put(sent).start()
            sent = sent + 1
    vec_load.wait()
    last_row = VEC_BASE + (PAD - SHARD) * (DEVICES - 1)
    flat[last_row:last_row + VEC_ROWS, :] = s_vec[...]
    while sent < DEVICES:
        put(sent).start()
        sent = sent + 1
    for owner in range(DEVICES):
        put(owner).wait()


def flatten(g_emb, g_attn, g_in, g_out, vec):
    chunk_count = len(flat_chunks())
    scratch = [pltpu.VMEM((rows, cols), jnp.float32) for rows, cols, _ in TENSORS]
    scratch += [
        pltpu.VMEM((VEC_ROWS, LANES), jnp.float32),
        pltpu.VMEM((DEVICES * PAD, LANES), jnp.float32),
        pltpu.SemaphoreType.DMA((chunk_count + 1,)),
        pltpu.SemaphoreType.DMA((DEVICES,)),
    ]
    return pl.pallas_call(
        flatten_kernel,
        out_shape=jax.ShapeDtypeStruct((DEVICES, PAD, LANES), jnp.float32),
        in_specs=[pl.BlockSpec(memory_space=pl.ANY)] * 5,
        out_specs=pl.BlockSpec(memory_space=pl.ANY),
        scratch_shapes=scratch,
        compiler_params=pltpu.CompilerParams(vmem_limit_bytes=VMEM_MAX),
        name="flatten",
    )(g_emb, g_attn, g_in, g_out, vec)


ORDERS = (("x", "y", "z"), ("y", "z", "x"), ("z", "x", "y"))
WEIGHT = {"z": 4, "y": 2, "x": 1}
HALF_ORDER = ((1, 1), (1, 0), (0, 1), (0, 0))
GATHER_ORDER = ((1, 0, 0), (0, 1, 0), (0, 0, 1), (1, 1, 0), (1, 0, 1), (0, 1, 1), (1, 1, 1))


def exchange_kernel(grad, opt_m, opt_v, master, m_new, v_new, w_new, gathered,
                    acc, pair, half, quarter, eighth, m_buf, v_buf, w_buf, wb,
                    load_sem, pair_send, pair_recv, half_send, half_recv, quarter_send, quarter_recv,
                    eighth_send, eighth_recv, state_sem, store_sem,
                    ring_send, ring_recv, share_send, share_recv, keep_sem):
    z, y, dx = lax.axis_index("dz"), lax.axis_index("dy"), lax.axis_index("dx")
    x, c = dx // 2, dx % 2
    mine = {"z": z, "y": y, "x": x}
    peers = {
        "c": {"dz": z, "dy": y, "dx": 2 * x + (1 - c)},
        "x": {"dz": z, "dy": y, "dx": 2 * (1 - x) + c},
        "y": {"dz": z, "dy": 1 - y, "dx": dx},
        "z": {"dz": 1 - z, "dy": y, "dx": dx},
    }

    def chip(part, bits):
        index = 0
        for axis, bit in zip(ORDERS[part], bits):
            index = index + WEIGHT[axis] * ((1 - mine[axis]) if bit else mine[axis])
        return index

    def rows(part):
        return pl.ds(PART_START[part], PART_ROWS[part])

    barrier = pltpu.get_barrier_semaphore()
    for peer in peers.values():
        pl.semaphore_signal(barrier, inc=1, device_id=peer, device_id_type=MESH)
    pl.semaphore_wait(barrier, 4)

    state = [
        pltpu.make_async_copy(opt_m, m_buf, state_sem.at[0]),
        pltpu.make_async_copy(opt_v, v_buf, state_sem.at[1]),
        pltpu.make_async_copy(master, w_buf, state_sem.at[2]),
    ]

    units = [(b1,) + rest for b1 in (1, 0) for rest in HALF_ORDER]
    parts = (0, 1, 2)

    def load(n, part):
        where = chip(part, units[n])
        return pltpu.make_async_copy(
            grad.at[where, c, rows(part)], acc.at[where, rows(part)], load_sem.at[n, part])

    def pair_copy(n, part):
        where = chip(part, units[n])
        return pltpu.make_async_remote_copy(
            src_ref=grad.at[where, 1 - c, rows(part)], dst_ref=pair.at[where, rows(part)],
            send_sem=pair_send.at[n, part], recv_sem=pair_recv.at[n, part],
            device_id=peers["c"], device_id_type=MESH)

    def half_copy(k, part):
        return pltpu.make_async_remote_copy(
            src_ref=acc.at[chip(part, (1,) + HALF_ORDER[k]), rows(part)],
            dst_ref=half.at[part, k, pl.ds(0, PART_ROWS[part])],
            send_sem=half_send.at[k, part], recv_sem=half_recv.at[k, part],
            device_id=peers[ORDERS[part][0]], device_id_type=MESH)

    def quarter_copy(k, part):
        return pltpu.make_async_remote_copy(
            src_ref=acc.at[chip(part, (0, 1, 1 - k)), rows(part)],
            dst_ref=quarter.at[part, k, pl.ds(0, PART_ROWS[part])],
            send_sem=quarter_send.at[k, part], recv_sem=quarter_recv.at[k, part],
            device_id=peers[ORDERS[part][1]], device_id_type=MESH)

    def eighth_copy(part):
        return pltpu.make_async_remote_copy(
            src_ref=acc.at[chip(part, (0, 0, 1)), rows(part)],
            dst_ref=eighth.at[part, pl.ds(0, PART_ROWS[part])],
            send_sem=eighth_send.at[part], recv_sem=eighth_recv.at[part],
            device_id=peers[ORDERS[part][2]], device_id_type=MESH)

    for n in range(8):
        for part in parts:
            load(n, part).start()
            pair_copy(n, part).start()
    for copy in state:
        copy.start()

    for n in range(8):
        for part in parts:
            load(n, part).wait()
            pair_copy(n, part).wait_recv()
            where = chip(part, units[n])
            acc[where, rows(part)] += pair[where, rows(part)]
            if n < 4:
                half_copy(n, part).start()
    for k in range(4):
        for part in parts:
            half_copy(k, part).wait_recv()
            where = chip(part, (0,) + HALF_ORDER[k])
            acc[where, rows(part)] += half[part, k, pl.ds(0, PART_ROWS[part])]
            if k < 2:
                quarter_copy(k, part).start()
    for k in range(2):
        for part in parts:
            quarter_copy(k, part).wait_recv()
            where = chip(part, (0, 0, 1 - k))
            acc[where, rows(part)] += quarter[part, k, pl.ds(0, PART_ROWS[part])]
            if k == 0:
                eighth_copy(part).start()

    for copy in state:
        copy.wait()

    here = 4 * z + 2 * y + x

    def ring_copy(bits, hop, part):
        flipped = tuple(1 - bit if n == hop else bit for n, bit in enumerate(bits))
        slot = flipped[0] * 4 + flipped[1] * 2 + flipped[2]
        where = chip(part, bits)
        return pltpu.make_async_remote_copy(
            src_ref=wb.at[where, rows(part)], dst_ref=wb.at[where, rows(part)],
            send_sem=ring_send.at[slot, part], recv_sem=ring_recv.at[slot, part],
            device_id=peers[ORDERS[part][hop]], device_id_type=MESH)

    def share_copy(bits, part):
        slot = bits[0] * 4 + bits[1] * 2 + bits[2]
        where = chip(part, bits)
        return pltpu.make_async_remote_copy(
            src_ref=wb.at[where, rows(part)], dst_ref=gathered.at[where, c, rows(part)],
            send_sem=share_send.at[slot, part], recv_sem=share_recv.at[slot, part],
            device_id=peers["c"], device_id_type=MESH)

    def keep_copy(bits, part):
        slot = bits[0] * 4 + bits[1] * 2 + bits[2]
        where = chip(part, bits)
        return pltpu.make_async_copy(
            wb.at[where, rows(part)], gathered.at[where, c, rows(part)], keep_sem.at[slot, part])

    for part in parts:
        eighth_copy(part).wait_recv()
        start, count = PART_START[part], min(PART_ROWS[part], SHARD - PART_START[part])
        pieces = [(start, count)] if count % 16 == 0 else [(start, count // 16 * 16), (start + count // 16 * 16, count % 16)]
        for first, size in pieces:
            span = pl.ds(first, size)
            grad_sum = (acc[here, span] + eighth[part, pl.ds(first - start, size)]) / DEVICES
            m_val = BETA_ONE * m_buf[span] + (1.0 - BETA_ONE) * grad_sum
            v_val = BETA_TWO * v_buf[span] + (1.0 - BETA_TWO) * grad_sum * grad_sum
            m_hat = m_val / (1.0 - BETA_ONE ** ADAM_STEP)
            v_hat = v_val / (1.0 - BETA_TWO ** ADAM_STEP)
            w_val = w_buf[span] - LEARN_RATE * m_hat / (jnp.sqrt(v_hat) + ADAM_EPS)
            m_buf[span] = m_val
            v_buf[span] = v_val
            w_buf[span] = w_val
            if size % 16:
                w_val = jnp.concatenate([w_val, jnp.zeros((16 - size % 16, LANES), jnp.float32)], axis=0)
                span = pl.ds(first, 16)
            wb[here, span] = w_val.astype(jnp.bfloat16)
        for hop in range(3):
            ring_copy((0, 0, 0), hop, part).start()
        share_copy((0, 0, 0), part).start()
        keep_copy((0, 0, 0), part).start()

    store = [
        pltpu.make_async_copy(m_buf, m_new, store_sem.at[0]),
        pltpu.make_async_copy(v_buf, v_new, store_sem.at[1]),
        pltpu.make_async_copy(w_buf, w_new, store_sem.at[2]),
    ]
    for copy in store:
        copy.start()

    def last_hop(bits):
        return max(n for n in range(3) if bits[n])

    for bits in GATHER_ORDER:
        hop = last_hop(bits)
        came = tuple(1 - bit if n == hop else bit for n, bit in enumerate(bits))
        for part in parts:
            ring_copy(came, hop, part).wait_recv()
            for later in range(hop + 1, 3):
                ring_copy(bits, later, part).start()
            share_copy(bits, part).start()
            keep_copy(bits, part).start()

    for n in range(8):
        for part in parts:
            pair_copy(n, part).wait_send()
    for part in parts:
        for k in range(4):
            half_copy(k, part).wait_send()
        for k in range(2):
            quarter_copy(k, part).wait_send()
        eighth_copy(part).wait_send()
        for bits in ((0, 0, 0),) + GATHER_ORDER:
            for later in range(0 if not any(bits) else last_hop(bits) + 1, 3):
                ring_copy(bits, later, part).wait_send()
            share_copy(bits, part).wait()
            keep_copy(bits, part).wait()
    for copy in store:
        copy.wait()


def exchange(grad, opt_m, opt_v, master):
    shape = jax.ShapeDtypeStruct
    state_shape = shape((SHARD, LANES), jnp.float32)
    f32 = functools.partial(pltpu.VMEM, dtype=jnp.float32)
    dma = pltpu.SemaphoreType.DMA
    scratch = [
        f32((8, PAD, LANES)), f32((8, PAD, LANES)),
        f32((3, 4, PART_MAX, LANES)), f32((3, 2, PART_MAX, LANES)), f32((3, PART_MAX, LANES)),
        f32((SHARD, LANES)), f32((SHARD, LANES)), f32((SHARD, LANES)),
        pltpu.VMEM((8, PAD, LANES), jnp.bfloat16),
        dma((8, 3)), dma((8, 3)), dma((8, 3)), dma((4, 3)), dma((4, 3)), dma((2, 3)), dma((2, 3)),
        dma((3,)), dma((3,)), dma((3,)), dma((3,)),
        dma((8, 3)), dma((8, 3)), dma((8, 3)), dma((8, 3)), dma((8, 3)),
    ]
    return pl.pallas_call(
        exchange_kernel,
        out_shape=(state_shape, state_shape, state_shape, shape((8, 2, PAD, LANES), jnp.bfloat16)),
        in_specs=[pl.BlockSpec(memory_space=pl.ANY)] * 4,
        out_specs=(pl.BlockSpec(memory_space=pl.ANY),) * 4,
        scratch_shapes=scratch,
        compiler_params=pltpu.CompilerParams(vmem_limit_bytes=VMEM_MAX, collective_id=0, has_side_effects=True),
        name="exchange",
    )(grad, opt_m, opt_v, master)


def unflatten_kernel(flat_in, o_emb, o_attn, o_in, o_out, halves, flat, b_emb, b_attn, b_in, b_out, in_sem, out_sem):
    outs = (o_emb, o_attn, o_in, o_out)
    bufs = (b_emb, b_attn, b_in, b_out)
    chunks = flat_chunks()

    def load(owner):
        return pltpu.make_async_copy(flat_in.at[owner], halves.at[owner], in_sem.at[owner])

    def put(k):
        index, start, step = chunks[k]
        return pltpu.make_async_copy(
            bufs[index].at[pl.ds(start, step)], outs[index].at[pl.ds(start, step)], out_sem.at[k])

    for owner in range(DEVICES):
        load(owner).start()
    ready = 0
    for k, (index, start, step) in enumerate(chunks):
        _, cols, base = TENSORS[index]
        groups = cols // LANES
        buf = bufs[index]
        need = base + (start + step) * groups
        while ready * SHARD < need:
            load(ready).wait()
            at = ready * SHARD
            whole = SHARD // 16

            def widen(t, carry, at=at, ready=ready):
                row = pl.multiple_of(t * 16, 16)
                flat[pl.ds(at + row, 16), :] = halves[ready, pl.ds(row, 16), :].astype(jnp.float32)
                return carry

            lax.fori_loop(0, whole, widen, 0, unroll=8)
            tail = halves[ready, whole * 16:whole * 16 + 16, :].astype(jnp.float32)
            flat[at + whole * 16:at + SHARD, :] = tail[:SHARD - whole * 16]
            ready = ready + 1

        def body(t, carry, base=base, groups=groups, buf=buf):
            row = pl.multiple_of(t * 16, 16)
            for j in range(groups):
                q = base + row * groups + j
                top = flat[pl.ds(q, 8, stride=groups), :]
                low = flat[pl.ds(q + 8 * groups, 8, stride=groups), :]
                buf[pl.ds(row, 16), j * LANES:(j + 1) * LANES] = (
                    jnp.concatenate([top, low], axis=0).astype(jnp.bfloat16))
            return carry

        lax.fori_loop(start // 16, (start + step) // 16, body, 0, unroll=2)
        put(k).start()
    for k in range(len(chunks)):
        put(k).wait()
    while ready < DEVICES:
        load(ready).wait()
        ready = ready + 1


def unflatten(flat):
    bf16 = jnp.bfloat16
    return pl.pallas_call(
        unflatten_kernel,
        out_shape=tuple(jax.ShapeDtypeStruct((rows, cols), bf16) for rows, cols, _ in TENSORS),
        in_specs=[pl.BlockSpec(memory_space=pl.ANY)],
        out_specs=(pl.BlockSpec(memory_space=pl.ANY),) * 4,
        scratch_shapes=[pltpu.VMEM((DEVICES, PAD, LANES), bf16), pltpu.VMEM((DEVICES * SHARD, LANES), jnp.float32)]
        + [pltpu.VMEM((rows, cols), bf16) for rows, cols, _ in TENSORS]
        + [pltpu.SemaphoreType.DMA((DEVICES,)), pltpu.SemaphoreType.DMA((len(flat_chunks()),))],
        compiler_params=pltpu.CompilerParams(vmem_limit_bytes=VMEM_MAX),
        name="unflatten",
    )(flat)


SUB = 256
BLOCK = 2048
COLS = 512
GELU_A = math.sqrt(2.0 / math.pi)
GELU_B = GELU_A * 0.044715


def ffn_kernel(ids, act, flat, w_in, b_in, w_out, b_out, y_out, table, rows_buf, h_buf, u_buf, halves, sem):
    step = pl.program_id(0)

    @pl.when(step == 0)
    def _():
        for owner in range(4):
            pltpu.make_async_copy(flat.at[owner], halves.at[owner], sem.at[owner]).start()
        for owner in range(4):
            pltpu.make_async_copy(flat.at[owner], halves.at[owner], sem.at[owner]).wait()
            at = owner * SHARD
            count = min(SHARD, VOCAB * D // LANES - at)
            whole = count // 16

            def widen(t, carry, at=at, owner=owner):
                row = pl.multiple_of(t * 16, 16)
                table[pl.ds(at + row, 16), :] = halves[owner, pl.ds(row, 16), :].astype(jnp.float32) * math.sqrt(D)
                return carry

            lax.fori_loop(0, whole, widen, 0, unroll=8)
            if count % 16:
                tail = halves[owner, whole * 16:whole * 16 + 16, :].astype(jnp.float32) * math.sqrt(D)
                table[at + whole * 16:at + count, :] = tail[:count - whole * 16]

    def sub_block(s, carry):
        first = pl.multiple_of(s * SUB, SUB)
        token = step * BLOCK + first
        for tile in range(SUB // 8):
            for i in range(8):
                row = ids[token + tile * 8 + i] * 6
                rows_buf[pl.ds(tile * 48 + i, 6, stride=8), :] = table[pl.ds(row, 6), :]
        for pair in range(SUB // 16):
            for j in range(6):
                top = rows_buf[pair * 96 + j * 8:pair * 96 + j * 8 + 8, :]
                low = rows_buf[pair * 96 + 48 + j * 8:pair * 96 + 48 + j * 8 + 8, :]
                both = jnp.concatenate([top, low], axis=0)
                a_val = act[pl.ds(first + pair * 16, 16), j * LANES:(j + 1) * LANES].astype(jnp.float32)
                h_buf[pair * 16:pair * 16 + 16, j * LANES:(j + 1) * LANES] = (both + a_val).astype(jnp.bfloat16)
        h_val = h_buf[...]
        for f in range(0, FF, COLS):
            pre = jnp.dot(h_val, w_in[:, f:f + COLS], preferred_element_type=jnp.float32) + b_in[:, f:f + COLS]
            bent = jnp.tanh(pre * (GELU_A + GELU_B * (pre * pre)))
            part = 0.5 * pre
            u_buf[:, f:f + COLS] = (part + part * bent).astype(jnp.bfloat16)
        y_val = jnp.dot(u_buf[...], w_out[...], preferred_element_type=jnp.float32) + b_out[...]
        y_out[pl.ds(first, SUB), :] = y_val.astype(jnp.bfloat16)
        return carry

    lax.fori_loop(0, BLOCK // SUB, sub_block, 0)


def ffn(ids, act, flat, w_in, b_in, w_out, b_out):
    tokens = act.shape[0]
    whole = lambda i, ids: (0, 0)
    grid_spec = pltpu.PrefetchScalarGridSpec(
        num_scalar_prefetch=1,
        grid=(tokens // BLOCK,),
        in_specs=[
            pl.BlockSpec((BLOCK, D), lambda i, ids: (i, 0)),
            pl.BlockSpec(memory_space=pl.ANY),
            pl.BlockSpec((D, FF), whole),
            pl.BlockSpec((1, FF), whole),
            pl.BlockSpec((FF, D), whole),
            pl.BlockSpec((1, D), whole),
        ],
        out_specs=pl.BlockSpec((BLOCK, D), lambda i, ids: (i, 0)),
        scratch_shapes=[
            pltpu.VMEM((VOCAB * D // LANES, LANES), jnp.float32),
            pltpu.VMEM((SUB * 6, LANES), jnp.float32),
            pltpu.VMEM((SUB, D), jnp.bfloat16),
            pltpu.VMEM((SUB, FF), jnp.bfloat16),
            pltpu.VMEM((4, PAD, LANES), jnp.bfloat16),
            pltpu.SemaphoreType.DMA((4,)),
        ],
    )
    return pl.pallas_call(
        ffn_kernel,
        out_shape=jax.ShapeDtypeStruct((tokens, D), jnp.bfloat16),
        grid_spec=grid_spec,
        compiler_params=pltpu.CompilerParams(vmem_limit_bytes=VMEM_MAX),
        name="ffn",
    )(ids, act, flat, w_in, b_in, w_out, b_out)


def solution(mesh):
    def device_step(g_emb, g_attn, g_in, g_out, g_vecd, g_vecf, opt_m, opt_v, master, tok_ids, act_in):
        vec = jnp.concatenate([
            g_vecd.reshape(-1, LANES), g_vecf.reshape(-1, LANES),
            jnp.zeros((VEC_ROWS - (9 * D + FF) // LANES, LANES), jnp.float32)], axis=0)
        grad = flatten(g_emb.reshape(VOCAB, D), g_attn.reshape(4 * D, D), g_in.reshape(D, FF), g_out.reshape(FF, D), vec)
        m_new, v_new, w_new, gathered = exchange(
            grad.reshape(8, 2, PAD, LANES), opt_m.reshape(SHARD, LANES),
            opt_v.reshape(SHARD, LANES), master.reshape(SHARD, LANES))
        flat = gathered.reshape(DEVICES, PAD, LANES)
        wb_emb, wb_attn, wb_in, wb_out = unflatten(flat)
        first = VEC_BASE - SHARD * (DEVICES - 1)
        wb_vecd = flat[DEVICES - 1, first:first + 9 * D // LANES].reshape(9, D)
        wb_vecf = flat[DEVICES - 1, first + 9 * D // LANES:first + (9 * D + FF) // LANES].reshape(1, FF)
        y_out = ffn(tok_ids, act_in, flat, wb_in, wb_vecf.astype(jnp.float32), wb_out,
                    wb_vecd[8:9].astype(jnp.float32))
        return (m_new.reshape(-1), v_new.reshape(-1), w_new.reshape(-1), wb_emb, wb_attn.reshape(1, 4, D, D),
                wb_in[None], wb_out[None], wb_vecd[None], wb_vecf, y_out)

    grad_specs = tuple(P(AXES, *([None] * (grad_rank - 1))) for grad_rank in GRAD_RANKS)
    in_specs = grad_specs + (P(AXES), P(AXES), P(AXES), P(AXES), P(AXES, None))
    out_specs = (P(AXES), P(AXES), P(AXES), P(), P(), P(), P(), P(), P(), P(AXES, None))
    return jax.shard_map(device_step, mesh=mesh, in_specs=in_specs, out_specs=out_specs, check_vma=False)
```

```python
import functools
import math

import jax
import jax.numpy as jnp
from jax import lax
from jax.experimental import pallas as pl
from jax.experimental.pallas import tpu as pltpu
from jax.sharding import PartitionSpec as P

LEARN_RATE = 0.002
BETA_ONE = 0.9
BETA_TWO = 0.95
ADAM_EPS = 1e-8
ADAM_STEP = 2
AXES = ("dz", "dy", "dx")
GRAD_RANKS = (3, 5, 4, 4, 4, 3)
MESH = pl.DeviceIdType.MESH

D = 768
FF = 2048
VOCAB = 2048
DEVICES = 16
LANES = 128
SHARD = 3461
PAD = 3472
PART_START = (0, 1152, 2304)
PART_ROWS = (1152, 1152, 1168)
PART_MAX = 1168
VMEM_MAX = 67_000_000

TENSORS = (
    (VOCAB, D, 0),
    (4 * D, D, VOCAB * D // LANES),
    (D, FF, (VOCAB * D + 4 * D * D) // LANES),
    (FF, D, (VOCAB * D + 4 * D * D + D * FF) // LANES),
)
VEC_BASE = (VOCAB * D + 4 * D * D + 2 * D * FF) // LANES
VEC_ROWS = DEVICES * SHARD - VEC_BASE


def flat_chunks():
    chunks = []
    for index, (rows, cols, base) in enumerate(TENSORS):
        step = 256 if cols == D else 128
        for start in range(0, rows, step):
            chunks.append((index, start, step))
    return chunks


def flatten_kernel(g_emb, g_attn, g_in, g_out, vec, flat_out, s_emb, s_attn, s_in, s_out, s_vec, flat, in_sem, out_sem):
    sources = (g_emb, g_attn, g_in, g_out)
    stages = (s_emb, s_attn, s_in, s_out)
    chunks = flat_chunks()

    def load(k):
        index, start, step = chunks[k]
        return pltpu.make_async_copy(
            sources[index].at[pl.ds(start, step)], stages[index].at[pl.ds(start, step)], in_sem.at[k])

    vec_load = pltpu.make_async_copy(vec, s_vec, in_sem.at[len(chunks)])
    for k in range(len(chunks)):
        load(k).start()
    vec_load.start()

    def put(owner):
        return pltpu.make_async_copy(flat.at[pl.ds(owner * PAD, PAD)], flat_out.at[owner], out_sem.at[owner])

    sent = 0
    for k, (index, start, step) in enumerate(chunks):
        _, cols, base = TENSORS[index]
        groups = cols // LANES
        stage = stages[index]
        load(k).wait()
        tile = start // 8
        last = (start + step) // 8
        while tile < last:
            first_row = base + tile * 8 * groups
            owner = first_row // SHARD
            fit = (SHARD * (owner + 1) - first_row) // (8 * groups)
            run = min(fit, last - tile)
            if run > 0:
                shift = base + (PAD - SHARD) * owner

                def body(t, carry, shift=shift, groups=groups, stage=stage):
                    row = pl.multiple_of(t * 8, 8)
                    for j in range(groups):
                        flat[pl.ds(shift + row * groups + j, 8, stride=groups), :] = (
                            stage[pl.ds(row, 8), j * LANES:(j + 1) * LANES])
                    return carry

                lax.fori_loop(tile, tile + run, body, 0, unroll=2)
                tile = tile + run
            else:
                for i in range(8):
                    for j in range(groups):
                        q = first_row + i * groups + j
                        p = q + (PAD - SHARD) * (q // SHARD)
                        flat[p:p + 1, :] = stage[tile * 8 + i:tile * 8 + i + 1, j * LANES:(j + 1) * LANES]
                tile = tile + 1
        done = (base + last * 8 * groups) // SHARD
        while sent < min(done, DEVICES - 1):
            put(sent).start()
            sent = sent + 1
    vec_load.wait()
    last_row = VEC_BASE + (PAD - SHARD) * (DEVICES - 1)
    flat[last_row:last_row + VEC_ROWS, :] = s_vec[...]
    while sent < DEVICES:
        put(sent).start()
        sent = sent + 1
    for owner in range(DEVICES):
        put(owner).wait()


def flatten(g_emb, g_attn, g_in, g_out, vec):
    chunk_count = len(flat_chunks())
    scratch = [pltpu.VMEM((rows, cols), jnp.float32) for rows, cols, _ in TENSORS]
    scratch += [
        pltpu.VMEM((VEC_ROWS, LANES), jnp.float32),
        pltpu.VMEM((DEVICES * PAD, LANES), jnp.float32),
        pltpu.SemaphoreType.DMA((chunk_count + 1,)),
        pltpu.SemaphoreType.DMA((DEVICES,)),
    ]
    return pl.pallas_call(
        flatten_kernel,
        out_shape=jax.ShapeDtypeStruct((DEVICES, PAD, LANES), jnp.float32),
        in_specs=[pl.BlockSpec(memory_space=pl.ANY)] * 5,
        out_specs=pl.BlockSpec(memory_space=pl.ANY),
        scratch_shapes=scratch,
        compiler_params=pltpu.CompilerParams(vmem_limit_bytes=VMEM_MAX),
        name="flatten",
    )(g_emb, g_attn, g_in, g_out, vec)


ORDERS = (("x", "y", "z"), ("y", "z", "x"), ("z", "x", "y"))
WEIGHT = {"z": 4, "y": 2, "x": 1}
HALF_ORDER = ((1, 1), (1, 0), (0, 1), (0, 0))
GATHER_ORDER = ((1, 0, 0), (0, 1, 0), (0, 0, 1), (1, 1, 0), (1, 0, 1), (0, 1, 1), (1, 1, 1))


def exchange_kernel(grad, opt_m, opt_v, master, m_new, v_new, w_new, gathered,
                    acc, pair, half, quarter, eighth, m_buf, v_buf, w_buf, wb,
                    load_sem, pair_send, pair_recv, half_send, half_recv, quarter_send, quarter_recv,
                    eighth_send, eighth_recv, state_sem, store_sem,
                    ring_send, ring_recv, share_send, share_recv, keep_sem):
    z, y, dx = lax.axis_index("dz"), lax.axis_index("dy"), lax.axis_index("dx")
    x, c = dx // 2, dx % 2
    mine = {"z": z, "y": y, "x": x}
    peers = {
        "c": {"dz": z, "dy": y, "dx": 2 * x + (1 - c)},
        "x": {"dz": z, "dy": y, "dx": 2 * (1 - x) + c},
        "y": {"dz": z, "dy": 1 - y, "dx": dx},
        "z": {"dz": 1 - z, "dy": y, "dx": dx},
    }

    def chip(part, bits):
        index = 0
        for axis, bit in zip(ORDERS[part], bits):
            index = index + WEIGHT[axis] * ((1 - mine[axis]) if bit else mine[axis])
        return index

    def rows(part):
        return pl.ds(PART_START[part], PART_ROWS[part])

    barrier = pltpu.get_barrier_semaphore()
    for peer in peers.values():
        pl.semaphore_signal(barrier, inc=1, device_id=peer, device_id_type=MESH)
    pl.semaphore_wait(barrier, 4)

    state = [
        pltpu.make_async_copy(opt_m, m_buf, state_sem.at[0]),
        pltpu.make_async_copy(opt_v, v_buf, state_sem.at[1]),
        pltpu.make_async_copy(master, w_buf, state_sem.at[2]),
    ]

    units = [(b1,) + rest for b1 in (1, 0) for rest in HALF_ORDER]
    parts = (0, 1, 2)

    def load(n, part):
        where = chip(part, units[n])
        return pltpu.make_async_copy(
            grad.at[where, c, rows(part)], acc.at[where, rows(part)], load_sem.at[n, part])

    def pair_copy(n, part):
        where = chip(part, units[n])
        return pltpu.make_async_remote_copy(
            src_ref=grad.at[where, 1 - c, rows(part)], dst_ref=pair.at[where, rows(part)],
            send_sem=pair_send.at[n, part], recv_sem=pair_recv.at[n, part],
            device_id=peers["c"], device_id_type=MESH)

    def half_copy(k, part):
        return pltpu.make_async_remote_copy(
            src_ref=acc.at[chip(part, (1,) + HALF_ORDER[k]), rows(part)],
            dst_ref=half.at[part, k, pl.ds(0, PART_ROWS[part])],
            send_sem=half_send.at[k, part], recv_sem=half_recv.at[k, part],
            device_id=peers[ORDERS[part][0]], device_id_type=MESH)

    def quarter_copy(k, part):
        return pltpu.make_async_remote_copy(
            src_ref=acc.at[chip(part, (0, 1, 1 - k)), rows(part)],
            dst_ref=quarter.at[part, k, pl.ds(0, PART_ROWS[part])],
            send_sem=quarter_send.at[k, part], recv_sem=quarter_recv.at[k, part],
            device_id=peers[ORDERS[part][1]], device_id_type=MESH)

    def eighth_copy(part):
        return pltpu.make_async_remote_copy(
            src_ref=acc.at[chip(part, (0, 0, 1)), rows(part)],
            dst_ref=eighth.at[part, pl.ds(0, PART_ROWS[part])],
            send_sem=eighth_send.at[part], recv_sem=eighth_recv.at[part],
            device_id=peers[ORDERS[part][2]], device_id_type=MESH)

    for n in range(8):
        for part in parts:
            load(n, part).start()
            pair_copy(n, part).start()
    for copy in state:
        copy.start()

    for n in range(8):
        for part in parts:
            load(n, part).wait()
            pair_copy(n, part).wait_recv()
            where = chip(part, units[n])
            acc[where, rows(part)] += pair[where, rows(part)]
            if n < 4:
                half_copy(n, part).start()
    for k in range(4):
        for part in parts:
            half_copy(k, part).wait_recv()
            where = chip(part, (0,) + HALF_ORDER[k])
            acc[where, rows(part)] += half[part, k, pl.ds(0, PART_ROWS[part])]
            if k < 2:
                quarter_copy(k, part).start()
    for k in range(2):
        for part in parts:
            quarter_copy(k, part).wait_recv()
            where = chip(part, (0, 0, 1 - k))
            acc[where, rows(part)] += quarter[part, k, pl.ds(0, PART_ROWS[part])]
            if k == 0:
                eighth_copy(part).start()

    for copy in state:
        copy.wait()

    here = 4 * z + 2 * y + x

    def ring_copy(bits, hop, part):
        flipped = tuple(1 - bit if n == hop else bit for n, bit in enumerate(bits))
        slot = flipped[0] * 4 + flipped[1] * 2 + flipped[2]
        where = chip(part, bits)
        return pltpu.make_async_remote_copy(
            src_ref=wb.at[where, rows(part)], dst_ref=wb.at[where, rows(part)],
            send_sem=ring_send.at[slot, part], recv_sem=ring_recv.at[slot, part],
            device_id=peers[ORDERS[part][hop]], device_id_type=MESH)

    def share_copy(bits, part):
        slot = bits[0] * 4 + bits[1] * 2 + bits[2]
        where = chip(part, bits)
        return pltpu.make_async_remote_copy(
            src_ref=wb.at[where, rows(part)], dst_ref=gathered.at[where, c, rows(part)],
            send_sem=share_send.at[slot, part], recv_sem=share_recv.at[slot, part],
            device_id=peers["c"], device_id_type=MESH)

    def keep_copy(bits, part):
        slot = bits[0] * 4 + bits[1] * 2 + bits[2]
        where = chip(part, bits)
        return pltpu.make_async_copy(
            wb.at[where, rows(part)], gathered.at[where, c, rows(part)], keep_sem.at[slot, part])

    for part in parts:
        eighth_copy(part).wait_recv()
        start, count = PART_START[part], min(PART_ROWS[part], SHARD - PART_START[part])
        pieces = [(start, count)] if count % 16 == 0 else [(start, count // 16 * 16), (start + count // 16 * 16, count % 16)]
        for first, size in pieces:
            span = pl.ds(first, size)
            grad_sum = (acc[here, span] + eighth[part, pl.ds(first - start, size)]) / DEVICES
            m_val = BETA_ONE * m_buf[span] + (1.0 - BETA_ONE) * grad_sum
            v_val = BETA_TWO * v_buf[span] + (1.0 - BETA_TWO) * grad_sum * grad_sum
            m_hat = m_val / (1.0 - BETA_ONE ** ADAM_STEP)
            v_hat = v_val / (1.0 - BETA_TWO ** ADAM_STEP)
            w_val = w_buf[span] - LEARN_RATE * m_hat / (jnp.sqrt(v_hat) + ADAM_EPS)
            m_buf[span] = m_val
            v_buf[span] = v_val
            w_buf[span] = w_val
            if size % 16:
                w_val = jnp.concatenate([w_val, jnp.zeros((16 - size % 16, LANES), jnp.float32)], axis=0)
                span = pl.ds(first, 16)
            wb[here, span] = w_val.astype(jnp.bfloat16)
        for hop in range(3):
            ring_copy((0, 0, 0), hop, part).start()
        share_copy((0, 0, 0), part).start()
        keep_copy((0, 0, 0), part).start()

    store = [
        pltpu.make_async_copy(m_buf, m_new, store_sem.at[0]),
        pltpu.make_async_copy(v_buf, v_new, store_sem.at[1]),
        pltpu.make_async_copy(w_buf, w_new, store_sem.at[2]),
    ]
    for copy in store:
        copy.start()

    def last_hop(bits):
        return max(n for n in range(3) if bits[n])

    for bits in GATHER_ORDER:
        hop = last_hop(bits)
        came = tuple(1 - bit if n == hop else bit for n, bit in enumerate(bits))
        for part in parts:
            ring_copy(came, hop, part).wait_recv()
            for later in range(hop + 1, 3):
                ring_copy(bits, later, part).start()
            share_copy(bits, part).start()
            keep_copy(bits, part).start()

    for n in range(8):
        for part in parts:
            pair_copy(n, part).wait_send()
    for part in parts:
        for k in range(4):
            half_copy(k, part).wait_send()
        for k in range(2):
            quarter_copy(k, part).wait_send()
        eighth_copy(part).wait_send()
        for bits in ((0, 0, 0),) + GATHER_ORDER:
            for later in range(0 if not any(bits) else last_hop(bits) + 1, 3):
                ring_copy(bits, later, part).wait_send()
            share_copy(bits, part).wait()
            keep_copy(bits, part).wait()
    for copy in store:
        copy.wait()


def exchange(grad, opt_m, opt_v, master):
    shape = jax.ShapeDtypeStruct
    state_shape = shape((SHARD, LANES), jnp.float32)
    f32 = functools.partial(pltpu.VMEM, dtype=jnp.float32)
    dma = pltpu.SemaphoreType.DMA
    scratch = [
        f32((8, PAD, LANES)), f32((8, PAD, LANES)),
        f32((3, 4, PART_MAX, LANES)), f32((3, 2, PART_MAX, LANES)), f32((3, PART_MAX, LANES)),
        f32((SHARD, LANES)), f32((SHARD, LANES)), f32((SHARD, LANES)),
        pltpu.VMEM((8, PAD, LANES), jnp.bfloat16),
        dma((8, 3)), dma((8, 3)), dma((8, 3)), dma((4, 3)), dma((4, 3)), dma((2, 3)), dma((2, 3)),
        dma((3,)), dma((3,)), dma((3,)), dma((3,)),
        dma((8, 3)), dma((8, 3)), dma((8, 3)), dma((8, 3)), dma((8, 3)),
    ]
    return pl.pallas_call(
        exchange_kernel,
        out_shape=(state_shape, state_shape, state_shape, shape((8, 2, PAD, LANES), jnp.bfloat16)),
        in_specs=[pl.BlockSpec(memory_space=pl.ANY)] * 4,
        out_specs=(pl.BlockSpec(memory_space=pl.ANY),) * 4,
        scratch_shapes=scratch,
        compiler_params=pltpu.CompilerParams(vmem_limit_bytes=VMEM_MAX, collective_id=0, has_side_effects=True),
        name="exchange",
    )(grad, opt_m, opt_v, master)


SUB = 512
CHUNK = 2 * SUB
RING = 6
ACT_SLOTS = 3
GELU_A = math.sqrt(2.0 / math.pi)
GELU_B = GELU_A * 0.044715
WIDEN_ORDER = (8, 9, 10, 11, 12, 13, 14, 15, 0, 1, 2, 3, 4, 5, 6, 7)


def ffn_kernel(steps, ids, act, flat, m_in, v_in, master_in,
               y_out, o_emb, o_attn, o_in, o_out, o_vecd, o_vecf, m_out, v_out, master_out,
               dense, ring, act_buf, y_buf, w_in, w_out, b_in, b_out, vecd_wide, vecd_buf, vecf_buf,
               rows_one, rows_two, h_one, h_two, u_one, u_two, emb_buf, attn_buf, state_buf,
               ring_sem, act_sem, y_sem, emb_sem, attn_sem, weight_sem, state_sem):
    emb_rows, attn_rows = VOCAB // steps, 4 * D // steps

    def load_act(it):
        return pltpu.make_async_copy(
            act.at[pl.ds(it * CHUNK, CHUNK)], act_buf.at[lax.rem(it, ACT_SLOTS)], act_sem.at[lax.rem(it, ACT_SLOTS)])

    def store_y(it):
        return pltpu.make_async_copy(
            y_buf.at[lax.rem(it, 2)], y_out.at[pl.ds(it * CHUNK, CHUNK)], y_sem.at[lax.rem(it, 2)])

    def store_emb(it):
        return pltpu.make_async_copy(
            emb_buf.at[lax.rem(it, 2)], o_emb.at[pl.ds(it * emb_rows, emb_rows)], emb_sem.at[lax.rem(it, 2)])

    def store_attn(it):
        return pltpu.make_async_copy(
            attn_buf.at[lax.rem(it, 2)], o_attn.at[pl.ds(it * attn_rows, attn_rows)], attn_sem.at[lax.rem(it, 2)])

    def load_flat(n):
        return pltpu.make_async_copy(flat.at[WIDEN_ORDER[n]], ring.at[n % RING], ring_sem.at[n % RING])

    for n in range(RING):
        load_flat(n).start()
    load_act(0).start()
    load_act(1).start()

    def relayout(base, groups, row, buf, at):
        for j in range(groups):
            q = base + row * groups + j
            top = dense[pl.ds(q, 8, stride=groups), :]
            low = dense[pl.ds(q + 8 * groups, 8, stride=groups), :]
            buf[pl.ds(at, 16), j * LANES:(j + 1) * LANES] = jnp.concatenate([top, low], axis=0).astype(jnp.bfloat16)

    for n, owner in enumerate(WIDEN_ORDER):
        load_flat(n).wait()
        at = owner * SHARD
        whole = SHARD // 16

        def widen(t, carry, at=at, slot=n % RING):
            row = pl.multiple_of(t * 16, 16)
            dense[pl.ds(at + row, 16), :] = ring[slot, pl.ds(row, 16), :].astype(jnp.float32)
            return carry

        lax.fori_loop(0, whole, widen, 0, unroll=24)
        tail = ring[n % RING, whole * 16:whole * 16 + 16, :].astype(jnp.float32)
        dense[at + whole * 16:at + SHARD, :] = tail[:SHARD - whole * 16]
        if n + RING < DEVICES:
            load_flat(n + RING).start()
        if owner == 12:
            def fill_in(t, carry):
                row = pl.multiple_of(t * 16, 16)
                relayout(TENSORS[2][2], FF // LANES, row, w_in, row)
                return carry

            lax.fori_loop(0, D // 16, fill_in, 0, unroll=2)
            pltpu.make_async_copy(w_in, o_in, weight_sem.at[0]).start()
        if owner == 15:
            def fill_out(t, carry):
                row = pl.multiple_of(t * 16, 16)
                relayout(TENSORS[3][2], D // LANES, row, w_out, row)
                return carry

            lax.fori_loop(0, FF // 16, fill_out, 0, unroll=4)
            pltpu.make_async_copy(w_out, o_out, weight_sem.at[1]).start()
            for i in range(9):
                for j in range(D // LANES):
                    q = VEC_BASE + i * (D // LANES) + j
                    vecd_wide[i:i + 1, j * LANES:(j + 1) * LANES] = dense[q:q + 1, :]
            for j in range(D // LANES):
                q = VEC_BASE + 8 * (D // LANES) + j
                b_out[:, j * LANES:(j + 1) * LANES] = dense[q:q + 1, :]
            for j in range(FF // LANES):
                q = VEC_BASE + 9 * (D // LANES) + j
                b_in[:, j * LANES:(j + 1) * LANES] = dense[q:q + 1, :]
            vecd_buf[...] = vecd_wide[...].astype(jnp.bfloat16)
            vecf_buf[...] = b_in[...].astype(jnp.bfloat16)
            pltpu.make_async_copy(vecd_buf, o_vecd, weight_sem.at[2]).start()
            pltpu.make_async_copy(vecf_buf, o_vecf, weight_sem.at[3]).start()

    def lookup(it, half, h_buf, rows_buf):
        slot = lax.rem(it, ACT_SLOTS)
        token = jnp.minimum(it, steps - 1) * CHUNK + half * SUB
        for tile in range(SUB // 8):
            for i in range(8):
                row = ids[token + tile * 8 + i] * (D // LANES)
                rows_buf[pl.ds(tile * 56 + i * 7, 8), :] = dense[pl.ds(row, 8), :]
        for pair in range(SUB // 16):
            for j in range(D // LANES):
                top = rows_buf[pl.ds(pair * 112 + j, 8, stride=7), :]
                low = rows_buf[pl.ds(pair * 112 + 56 + j, 8, stride=7), :]
                both = jnp.concatenate([top, low], axis=0) * math.sqrt(D)
                first = half * SUB + pair * 16
                a_val = act_buf[slot, first:first + 16, j * LANES:(j + 1) * LANES].astype(jnp.float32)
                h_buf[pair * 16:pair * 16 + 16, j * LANES:(j + 1) * LANES] = (both + a_val).astype(jnp.bfloat16)

    def multiply(it, half, h_buf, u_buf):
        pre = jnp.dot(h_buf[...], w_in[...], preferred_element_type=jnp.float32) + b_in[...]
        bent = jnp.tanh(pre * (GELU_A + GELU_B * (pre * pre)))
        part = 0.5 * pre
        u_buf[...] = (part + part * bent).astype(jnp.bfloat16)
        y_val = jnp.dot(u_buf[...], w_out[...], preferred_element_type=jnp.float32) + b_out[...]
        y_buf[lax.rem(it, 2), half * SUB:half * SUB + SUB, :] = y_val.astype(jnp.bfloat16)

    load_act(0).wait()
    lookup(0, 0, h_one, rows_one)

    moves = []
    for n, (source, target) in enumerate(((m_in, m_out), (v_in, v_out), (master_in, master_out))):
        moves.append(pltpu.make_async_copy(source, state_buf, state_sem.at[2 * n]))
        moves.append(pltpu.make_async_copy(state_buf, target, state_sem.at[2 * n + 1]))

    def body(it, carry):
        @pl.when(it + 1 < steps)
        def _():
            load_act(it + 1).wait()

        @pl.when(it + 2 < steps)
        def _():
            load_act(it + 2).start()

        @pl.when(it >= 2)
        def _():
            store_y(it - 2).wait()
            store_emb(it - 2).wait()
            store_attn(it - 2).wait()

        for n, move in enumerate(moves):
            @pl.when(it == 1 + 2 * n)
            def _(n=n, move=move):
                if n:
                    moves[n - 1].wait()
                move.start()

        lookup(it, 1, h_two, rows_two)
        multiply(it, 0, h_one, u_one)
        lookup(it + 1, 0, h_one, rows_one)
        multiply(it, 1, h_two, u_two)
        for t in range(emb_rows // 16):
            relayout(TENSORS[0][2], D // LANES, it * emb_rows + t * 16, emb_buf.at[lax.rem(it, 2)], t * 16)
        for t in range(attn_rows // 16):
            relayout(TENSORS[1][2], D // LANES, it * attn_rows + t * 16, attn_buf.at[lax.rem(it, 2)], t * 16)
        store_y(it).start()
        store_emb(it).start()
        store_attn(it).start()
        return carry

    lax.fori_loop(0, steps, body, 0)
    for it in (steps - 2, steps - 1):
        store_y(it).wait()
        store_emb(it).wait()
        store_attn(it).wait()
    moves[-1].wait()
    pltpu.make_async_copy(w_in, o_in, weight_sem.at[0]).wait()
    pltpu.make_async_copy(w_out, o_out, weight_sem.at[1]).wait()
    pltpu.make_async_copy(vecd_buf, o_vecd, weight_sem.at[2]).wait()
    pltpu.make_async_copy(vecf_buf, o_vecf, weight_sem.at[3]).wait()


def ffn(ids, act, flat, m_new, v_new, w_new):
    tokens = act.shape[0]
    steps = tokens // CHUNK
    f32, bf16 = jnp.float32, jnp.bfloat16
    shape = jax.ShapeDtypeStruct
    dma = pltpu.SemaphoreType.DMA
    anywhere = pl.BlockSpec(memory_space=pl.ANY)
    state = shape((SHARD, LANES), f32)
    return pl.pallas_call(
        functools.partial(ffn_kernel, steps),
        out_shape=(shape((tokens, D), bf16), shape((VOCAB, D), bf16), shape((4 * D, D), bf16), shape((D, FF), bf16),
                   shape((FF, D), bf16), shape((9, D), bf16), shape((1, FF), bf16), state, state, state),
        in_specs=[pl.BlockSpec(memory_space=pltpu.SMEM)] + [anywhere] * 5,
        out_specs=(anywhere,) * 10,
        scratch_shapes=[
            pltpu.VMEM((DEVICES * SHARD, LANES), f32),
            pltpu.VMEM((RING, PAD, LANES), bf16),
            pltpu.VMEM((ACT_SLOTS, CHUNK, D), bf16),
            pltpu.VMEM((2, CHUNK, D), bf16),
            pltpu.VMEM((D, FF), bf16),
            pltpu.VMEM((FF, D), bf16),
            pltpu.VMEM((1, FF), f32),
            pltpu.VMEM((1, D), f32),
            pltpu.VMEM((9, D), f32),
            pltpu.VMEM((9, D), bf16),
            pltpu.VMEM((1, FF), bf16),
            pltpu.VMEM((SUB * 7 + 8, LANES), f32),
            pltpu.VMEM((SUB * 7 + 8, LANES), f32),
            pltpu.VMEM((SUB, D), bf16),
            pltpu.VMEM((SUB, D), bf16),
            pltpu.VMEM((SUB, FF), bf16),
            pltpu.VMEM((SUB, FF), bf16),
            pltpu.VMEM((2, VOCAB // steps, D), bf16),
            pltpu.VMEM((2, 4 * D // steps, D), bf16),
            pltpu.VMEM((SHARD, LANES), f32),
            dma((RING,)), dma((ACT_SLOTS,)), dma((2,)), dma((2,)), dma((2,)), dma((4,)), dma((6,)),
        ],
        compiler_params=pltpu.CompilerParams(vmem_limit_bytes=VMEM_MAX),
        name="ffn",
    )(ids, act, flat, m_new, v_new, w_new)


def solution(mesh):
    def device_step(g_emb, g_attn, g_in, g_out, g_vecd, g_vecf, opt_m, opt_v, master, tok_ids, act_in):
        vec = jnp.concatenate([
            g_vecd.reshape(-1, LANES), g_vecf.reshape(-1, LANES),
            jnp.zeros((VEC_ROWS - (9 * D + FF) // LANES, LANES), jnp.float32)], axis=0)
        grad = flatten(g_emb.reshape(VOCAB, D), g_attn.reshape(4 * D, D), g_in.reshape(D, FF), g_out.reshape(FF, D), vec)
        m_new, v_new, w_new, gathered = exchange(
            grad.reshape(8, 2, PAD, LANES), opt_m.reshape(SHARD, LANES),
            opt_v.reshape(SHARD, LANES), master.reshape(SHARD, LANES))
        flat = gathered.reshape(DEVICES, PAD, LANES)
        y_out, wb_emb, wb_attn, wb_in, wb_out, wb_vecd, wb_vecf, m_new, v_new, w_new = ffn(
            tok_ids, act_in, flat, m_new, v_new, w_new)
        return (m_new.reshape(-1), v_new.reshape(-1), w_new.reshape(-1), wb_emb, wb_attn.reshape(1, 4, D, D),
                wb_in[None], wb_out[None], wb_vecd[None], wb_vecf, y_out)

    grad_specs = tuple(P(AXES, *([None] * (grad_rank - 1))) for grad_rank in GRAD_RANKS)
    in_specs = grad_specs + (P(AXES), P(AXES), P(AXES), P(AXES), P(AXES, None))
    out_specs = (P(AXES), P(AXES), P(AXES), P(), P(), P(), P(), P(), P(), P(AXES, None))
    return jax.shard_map(device_step, mesh=mesh, in_specs=in_specs, out_specs=out_specs, check_vma=False)
```

```python
import functools
import math

import jax
import jax.numpy as jnp
from jax import lax
from jax.experimental import pallas as pl
from jax.experimental.pallas import tpu as pltpu
from jax.sharding import PartitionSpec as P

LEARN_RATE = 0.002
BETA_ONE = 0.9
BETA_TWO = 0.95
ADAM_EPS = 1e-8
ADAM_STEP = 2
AXES = ("dz", "dy", "dx")
GRAD_RANKS = (3, 5, 4, 4, 4, 3)
MESH = pl.DeviceIdType.MESH

D = 768
FF = 2048
VOCAB = 2048
DEVICES = 16
LANES = 128
SHARD = 3461
PAD = 3472
PART_START = (0, 1152, 2304)
PART_ROWS = (1152, 1152, 1168)
PART_MAX = 1168
VMEM_MAX = 67_000_000

TENSORS = (
    (VOCAB, D, 0),
    (4 * D, D, VOCAB * D // LANES),
    (D, FF, (VOCAB * D + 4 * D * D) // LANES),
    (FF, D, (VOCAB * D + 4 * D * D + D * FF) // LANES),
)
TILES = 48
FLAT_ROWS = 8 * TILES
CHUNKS = 144
SPAN = 11
MARGIN = FLAT_ROWS
SLOT = 2 * MARGIN + 3464
STAGES = 4
VEC_BASE = (VOCAB * D + 4 * D * D + 2 * D * FF) // LANES
VEC_ROWS = DEVICES * SHARD - VEC_BASE


ORDERS = (("x", "y", "z"), ("y", "z", "x"), ("z", "x", "y"))
WEIGHT = {"z": 4, "y": 2, "x": 1}
CHIP_ORDER = ("xyz", "xy", "yz", "zx", "x", "y", "z", "")
HALF_ORDER = ((1, 1), (1, 0), (0, 1), (0, 0))
GATHER_ORDER = ((1, 0, 0), (0, 1, 0), (0, 0, 1), (1, 1, 0), (1, 0, 1), (0, 1, 1), (1, 1, 1))


def exchange_kernel(g_emb, g_attn, g_in, g_out, g_vec, opt_m, opt_v, master, m_new, v_new, w_new, gathered,
                    stage, vec_buf, acc, pair, half, quarter, eighth, m_buf, v_buf, w_buf, wb,
                    stage_sem, vec_sem, pair_send, pair_recv, half_send, half_recv, quarter_send, quarter_recv,
                    eighth_send, eighth_recv, state_sem, store_sem,
                    ring_send, ring_recv, share_send, share_recv, keep_sem):
    z, y, dx = lax.axis_index("dz"), lax.axis_index("dy"), lax.axis_index("dx")
    x, c = dx // 2, dx % 2
    mine = {"z": z, "y": y, "x": x}
    peers = {
        "c": {"dz": z, "dy": y, "dx": 2 * x + (1 - c)},
        "x": {"dz": z, "dy": y, "dx": 2 * (1 - x) + c},
        "y": {"dz": z, "dy": 1 - y, "dx": dx},
        "z": {"dz": 1 - z, "dy": y, "dx": dx},
    }

    def chip(part, bits):
        index = 0
        for axis, bit in zip(ORDERS[part], bits):
            index = index + WEIGHT[axis] * ((1 - mine[axis]) if bit else mine[axis])
        return index

    def rows(part):
        return pl.ds(PART_START[part], PART_ROWS[part])

    def acc_rows(part):
        return pl.ds(MARGIN + PART_START[part], PART_ROWS[part])

    vec_load = pltpu.make_async_copy(g_vec, vec_buf, vec_sem)
    state = [
        pltpu.make_async_copy(opt_m, m_buf, state_sem.at[0]),
        pltpu.make_async_copy(opt_v, v_buf, state_sem.at[1]),
        pltpu.make_async_copy(master, w_buf, state_sem.at[2]),
    ]

    parts = (0, 1, 2)

    def chip_at(n):
        index = 0
        for axis in "zyx":
            index = index + WEIGHT[axis] * ((1 - mine[axis]) if axis in CHIP_ORDER[n] else mine[axis])
        return index

    def shard_at(n):
        return 2 * chip_at(n % 8) + (1 - c if n < 8 else c)

    def chunk_bounds(owner):
        low = (owner * SHARD) // FLAT_ROWS
        high = (owner * SHARD + SHARD + FLAT_ROWS - 1 - (owner // (DEVICES - 1)) * VEC_ROWS) // FLAT_ROWS
        return low, high

    def by_tensor(k, act):
        @pl.when(k < 32)
        def _():
            act(0, 0)

        @pl.when(k >= 32)
        def _():
            @pl.when(k < 80)
            def _():
                act(1, 32)

            @pl.when(k >= 80)
            def _():
                @pl.when(k < 112)
                def _():
                    act(2, 80)

                @pl.when(k >= 112)
                def _():
                    act(3, 112)

    grads = (g_emb, g_attn, g_in, g_out)

    def load_shard(n):
        low, high = chunk_bounds(shard_at(n))
        slot = n % STAGES

        def one(k, carry):
            where = k - low

            def start(tensor, first):
                pltpu.make_async_copy(
                    grads[tensor].at[pl.ds((k - first) * TILES, TILES)], stage.at[slot, pl.ds(where * TILES, TILES)],
                    stage_sem.at[slot, where]).start()

            by_tensor(k, start)
            return carry

        lax.fori_loop(low, high, one, 0)

    def flatten_shard(n):
        owner = shard_at(n)
        low, high = chunk_bounds(owner)
        slot = n % STAGES
        where = chip_at(n % 8)

        def one(k, carry):
            at = k - low
            pltpu.make_async_copy(
                g_emb.at[pl.ds(0, TILES)], stage.at[slot, pl.ds(at * TILES, TILES)], stage_sem.at[slot, at]).wait()
            base = MARGIN + k * FLAT_ROWS - owner * SHARD

            def spread(tensor, first):
                groups = TENSORS[tensor][1] // LANES
                bands = TILES // groups
                for j in range(groups):
                    tile = stage[slot, pl.ds(at * TILES + j, bands, stride=groups)]
                    acc[where, pl.ds(base + j, 8 * bands, stride=groups), :] = tile.reshape(8 * bands, LANES)

            by_tensor(k, spread)
            return carry

        lax.fori_loop(low, high, one, 0)

        @pl.when(owner == DEVICES - 1)
        def _():
            first = MARGIN + SHARD - VEC_ROWS
            acc[where, first:first + VEC_ROWS, :] = vec_buf[...]

    def pair_copy(n, part):
        where = chip_at(n)
        return pltpu.make_async_remote_copy(
            src_ref=acc.at[where, acc_rows(part)], dst_ref=pair.at[where, rows(part)],
            send_sem=pair_send.at[n, part], recv_sem=pair_recv.at[n, part],
            device_id=peers["c"], device_id_type=MESH)

    def half_copy(k, part):
        return pltpu.make_async_remote_copy(
            src_ref=acc.at[chip(part, (1,) + HALF_ORDER[k]), acc_rows(part)],
            dst_ref=half.at[part, k, pl.ds(0, PART_ROWS[part])],
            send_sem=half_send.at[k, part], recv_sem=half_recv.at[k, part],
            device_id=peers[ORDERS[part][0]], device_id_type=MESH)

    def quarter_copy(k, part):
        return pltpu.make_async_remote_copy(
            src_ref=acc.at[chip(part, (0, 1, 1 - k)), acc_rows(part)],
            dst_ref=quarter.at[part, k, pl.ds(0, PART_ROWS[part])],
            send_sem=quarter_send.at[k, part], recv_sem=quarter_recv.at[k, part],
            device_id=peers[ORDERS[part][1]], device_id_type=MESH)

    def eighth_copy(part):
        return pltpu.make_async_remote_copy(
            src_ref=acc.at[chip(part, (0, 0, 1)), acc_rows(part)],
            dst_ref=eighth.at[part, pl.ds(0, PART_ROWS[part])],
            send_sem=eighth_send.at[part], recv_sem=eighth_recv.at[part],
            device_id=peers[ORDERS[part][2]], device_id_type=MESH)

    vec_load.start()
    for n in range(STAGES):
        load_shard(n)
    barrier = pltpu.get_barrier_semaphore()
    for peer in peers.values():
        pl.semaphore_signal(barrier, inc=1, device_id=peer, device_id_type=MESH)
    pl.semaphore_wait(barrier, 4)
    vec_load.wait()

    for n in range(8):
        flatten_shard(n)
        for part in parts:
            pair_copy(n, part).start()
        if n + STAGES < 16:
            load_shard(n + STAGES)
    for copy in state:
        copy.start()

    for n in range(8):
        for part in parts:
            pair_copy(n, part).wait_send()
        flatten_shard(8 + n)
        if 8 + n + STAGES < 16:
            load_shard(8 + n + STAGES)
        where = chip_at(n)
        for part in parts:
            pair_copy(n, part).wait_recv()
            acc[where, acc_rows(part)] += pair[where, rows(part)]
            bits = tuple(int(axis in CHIP_ORDER[n]) for axis in ORDERS[part])
            if bits[0]:
                half_copy(HALF_ORDER.index(bits[1:]), part).start()
    for k in range(4):
        for part in parts:
            half_copy(k, part).wait_recv()
            where = chip(part, (0,) + HALF_ORDER[k])
            acc[where, acc_rows(part)] += half[part, k, pl.ds(0, PART_ROWS[part])]
            if k < 2:
                quarter_copy(k, part).start()
    for k in range(2):
        for part in parts:
            quarter_copy(k, part).wait_recv()
            where = chip(part, (0, 0, 1 - k))
            acc[where, acc_rows(part)] += quarter[part, k, pl.ds(0, PART_ROWS[part])]
            if k == 0:
                eighth_copy(part).start()

    for copy in state:
        copy.wait()

    here = 4 * z + 2 * y + x

    def ring_copy(bits, hop, part):
        flipped = tuple(1 - bit if n == hop else bit for n, bit in enumerate(bits))
        slot = flipped[0] * 4 + flipped[1] * 2 + flipped[2]
        where = chip(part, bits)
        return pltpu.make_async_remote_copy(
            src_ref=wb.at[where, rows(part)], dst_ref=wb.at[where, rows(part)],
            send_sem=ring_send.at[slot, part], recv_sem=ring_recv.at[slot, part],
            device_id=peers[ORDERS[part][hop]], device_id_type=MESH)

    def share_copy(bits, part):
        slot = bits[0] * 4 + bits[1] * 2 + bits[2]
        where = chip(part, bits)
        return pltpu.make_async_remote_copy(
            src_ref=wb.at[where, rows(part)], dst_ref=gathered.at[where, c, rows(part)],
            send_sem=share_send.at[slot, part], recv_sem=share_recv.at[slot, part],
            device_id=peers["c"], device_id_type=MESH)

    def keep_copy(bits, part):
        slot = bits[0] * 4 + bits[1] * 2 + bits[2]
        where = chip(part, bits)
        return pltpu.make_async_copy(
            wb.at[where, rows(part)], gathered.at[where, c, rows(part)], keep_sem.at[slot, part])

    for part in parts:
        eighth_copy(part).wait_recv()
        start, count = PART_START[part], min(PART_ROWS[part], SHARD - PART_START[part])
        pieces = [(start, count)] if count % 16 == 0 else [(start, count // 16 * 16), (start + count // 16 * 16, count % 16)]
        for first, size in pieces:
            span = pl.ds(first, size)
            grad_sum = (acc[here, pl.ds(MARGIN + first, size)] + eighth[part, pl.ds(first - start, size)]) / DEVICES
            m_val = BETA_ONE * m_buf[span] + (1.0 - BETA_ONE) * grad_sum
            v_val = BETA_TWO * v_buf[span] + (1.0 - BETA_TWO) * grad_sum * grad_sum
            m_hat = m_val / (1.0 - BETA_ONE ** ADAM_STEP)
            v_hat = v_val / (1.0 - BETA_TWO ** ADAM_STEP)
            w_val = w_buf[span] - LEARN_RATE * m_hat / (jnp.sqrt(v_hat) + ADAM_EPS)
            m_buf[span] = m_val
            v_buf[span] = v_val
            w_buf[span] = w_val
            if size % 16:
                w_val = jnp.concatenate([w_val, jnp.zeros((16 - size % 16, LANES), jnp.float32)], axis=0)
                span = pl.ds(first, 16)
            wb[here, span] = w_val.astype(jnp.bfloat16)
        for hop in range(3):
            ring_copy((0, 0, 0), hop, part).start()
        share_copy((0, 0, 0), part).start()
        keep_copy((0, 0, 0), part).start()

    store = [
        pltpu.make_async_copy(m_buf, m_new, store_sem.at[0]),
        pltpu.make_async_copy(v_buf, v_new, store_sem.at[1]),
        pltpu.make_async_copy(w_buf, w_new, store_sem.at[2]),
    ]
    for copy in store:
        copy.start()

    def last_hop(bits):
        return max(n for n in range(3) if bits[n])

    for bits in GATHER_ORDER:
        hop = last_hop(bits)
        came = tuple(1 - bit if n == hop else bit for n, bit in enumerate(bits))
        for part in parts:
            ring_copy(came, hop, part).wait_recv()
            for later in range(hop + 1, 3):
                ring_copy(bits, later, part).start()
            share_copy(bits, part).start()
            keep_copy(bits, part).start()

    for part in parts:
        for k in range(4):
            half_copy(k, part).wait_send()
        for k in range(2):
            quarter_copy(k, part).wait_send()
        eighth_copy(part).wait_send()
        for bits in ((0, 0, 0),) + GATHER_ORDER:
            for later in range(0 if not any(bits) else last_hop(bits) + 1, 3):
                ring_copy(bits, later, part).wait_send()
            share_copy(bits, part).wait()
            keep_copy(bits, part).wait()
    for copy in store:
        copy.wait()


def exchange(*operands):
    shape = jax.ShapeDtypeStruct
    state_shape = shape((SHARD, LANES), jnp.float32)
    f32 = functools.partial(pltpu.VMEM, dtype=jnp.float32)
    dma = pltpu.SemaphoreType.DMA
    scratch = [
        f32((STAGES, SPAN * TILES, 8, LANES)), f32((VEC_ROWS, LANES)),
        f32((8, SLOT, LANES)), f32((8, PAD, LANES)),
        f32((3, 4, PART_MAX, LANES)), f32((3, 2, PART_MAX, LANES)), f32((3, PART_MAX, LANES)),
        f32((SHARD, LANES)), f32((SHARD, LANES)), f32((SHARD, LANES)),
        pltpu.VMEM((8, PAD, LANES), jnp.bfloat16),
        dma((STAGES, SPAN)), dma, dma((8, 3)), dma((8, 3)), dma((4, 3)), dma((4, 3)), dma((2, 3)), dma((2, 3)),
        dma((3,)), dma((3,)), dma((3,)), dma((3,)),
        dma((8, 3)), dma((8, 3)), dma((8, 3)), dma((8, 3)), dma((8, 3)),
    ]
    return pl.pallas_call(
        exchange_kernel,
        out_shape=(state_shape, state_shape, state_shape, shape((8, 2, PAD, LANES), jnp.bfloat16)),
        in_specs=[pl.BlockSpec(memory_space=pl.ANY)] * 8,
        out_specs=(pl.BlockSpec(memory_space=pl.ANY),) * 4,
        scratch_shapes=scratch,
        compiler_params=pltpu.CompilerParams(vmem_limit_bytes=VMEM_MAX, collective_id=0, has_side_effects=True),
        name="exchange",
    )(*operands)


SUB = 512
CHUNK = 2 * SUB
RING = 6
ACT_SLOTS = 3
GELU_A = math.sqrt(2.0 / math.pi)
GELU_B = GELU_A * 0.044715
WIDEN_ORDER = (8, 9, 10, 11, 12, 13, 14, 15, 0, 1, 2, 3, 4, 5, 6, 7)


def ffn_kernel(steps, ids, act, flat, m_in, v_in, master_in,
               y_out, o_emb, o_attn, o_in, o_out, o_vecd, o_vecf, m_out, v_out, master_out,
               dense, ring, act_buf, y_buf, w_in, w_out, b_in, b_out, vecd_wide, vecd_buf, vecf_buf,
               rows_one, rows_two, h_one, h_two, u_one, u_two, emb_buf, attn_buf, state_buf,
               ring_sem, act_sem, y_sem, emb_sem, attn_sem, weight_sem, state_sem):
    emb_rows, attn_rows = VOCAB // steps, 4 * D // steps

    def load_act(it):
        return pltpu.make_async_copy(
            act.at[pl.ds(it * CHUNK, CHUNK)], act_buf.at[lax.rem(it, ACT_SLOTS)], act_sem.at[lax.rem(it, ACT_SLOTS)])

    def store_y(it):
        return pltpu.make_async_copy(
            y_buf.at[lax.rem(it, 2)], y_out.at[pl.ds(it * CHUNK, CHUNK)], y_sem.at[lax.rem(it, 2)])

    def store_emb(it):
        return pltpu.make_async_copy(
            emb_buf.at[lax.rem(it, 2)], o_emb.at[pl.ds(it * emb_rows, emb_rows)], emb_sem.at[lax.rem(it, 2)])

    def store_attn(it):
        return pltpu.make_async_copy(
            attn_buf.at[lax.rem(it, 2)], o_attn.at[pl.ds(it * attn_rows, attn_rows)], attn_sem.at[lax.rem(it, 2)])

    def load_flat(n):
        return pltpu.make_async_copy(flat.at[WIDEN_ORDER[n]], ring.at[n % RING], ring_sem.at[n % RING])

    for n in range(RING):
        load_flat(n).start()
    load_act(0).start()
    load_act(1).start()

    def relayout(base, groups, row, buf, at):
        for j in range(groups):
            q = base + row * groups + j
            top = dense[pl.ds(q, 8, stride=groups), :]
            low = dense[pl.ds(q + 8 * groups, 8, stride=groups), :]
            buf[pl.ds(at, 16), j * LANES:(j + 1) * LANES] = jnp.concatenate([top, low], axis=0).astype(jnp.bfloat16)

    for n, owner in enumerate(WIDEN_ORDER):
        load_flat(n).wait()
        at = owner * SHARD
        whole = SHARD // 16

        def widen(t, carry, at=at, slot=n % RING):
            row = pl.multiple_of(t * 16, 16)
            dense[pl.ds(at + row, 16), :] = ring[slot, pl.ds(row, 16), :].astype(jnp.float32)
            return carry

        lax.fori_loop(0, whole, widen, 0, unroll=24)
        tail = ring[n % RING, whole * 16:whole * 16 + 16, :].astype(jnp.float32)
        dense[at + whole * 16:at + SHARD, :] = tail[:SHARD - whole * 16]
        if n + RING < DEVICES:
            load_flat(n + RING).start()
        if owner == 12:
            def fill_in(t, carry):
                row = pl.multiple_of(t * 16, 16)
                relayout(TENSORS[2][2], FF // LANES, row, w_in, row)
                return carry

            lax.fori_loop(0, D // 16, fill_in, 0, unroll=2)
            pltpu.make_async_copy(w_in, o_in, weight_sem.at[0]).start()
        if owner == 15:
            def fill_out(t, carry):
                row = pl.multiple_of(t * 16, 16)
                relayout(TENSORS[3][2], D // LANES, row, w_out, row)
                return carry

            lax.fori_loop(0, FF // 16, fill_out, 0, unroll=4)
            pltpu.make_async_copy(w_out, o_out, weight_sem.at[1]).start()
            for i in range(9):
                for j in range(D // LANES):
                    q = VEC_BASE + i * (D // LANES) + j
                    vecd_wide[i:i + 1, j * LANES:(j + 1) * LANES] = dense[q:q + 1, :]
            for j in range(D // LANES):
                q = VEC_BASE + 8 * (D // LANES) + j
                b_out[:, j * LANES:(j + 1) * LANES] = dense[q:q + 1, :]
            for j in range(FF // LANES):
                q = VEC_BASE + 9 * (D // LANES) + j
                b_in[:, j * LANES:(j + 1) * LANES] = dense[q:q + 1, :]
            vecd_buf[...] = vecd_wide[...].astype(jnp.bfloat16)
            vecf_buf[...] = b_in[...].astype(jnp.bfloat16)
            pltpu.make_async_copy(vecd_buf, o_vecd, weight_sem.at[2]).start()
            pltpu.make_async_copy(vecf_buf, o_vecf, weight_sem.at[3]).start()

    def lookup(it, half, h_buf, rows_buf):
        slot = lax.rem(it, ACT_SLOTS)
        token = jnp.minimum(it, steps - 1) * CHUNK + half * SUB
        for tile in range(SUB // 8):
            for i in range(8):
                row = ids[token + tile * 8 + i] * (D // LANES)
                rows_buf[pl.ds(tile * 56 + i * 7, 8), :] = dense[pl.ds(row, 8), :]
        for pair in range(SUB // 16):
            for j in range(D // LANES):
                top = rows_buf[pl.ds(pair * 112 + j, 8, stride=7), :]
                low = rows_buf[pl.ds(pair * 112 + 56 + j, 8, stride=7), :]
                both = jnp.concatenate([top, low], axis=0) * math.sqrt(D)
                first = half * SUB + pair * 16
                a_val = act_buf[slot, first:first + 16, j * LANES:(j + 1) * LANES].astype(jnp.float32)
                h_buf[pair * 16:pair * 16 + 16, j * LANES:(j + 1) * LANES] = (both + a_val).astype(jnp.bfloat16)

    def multiply(it, half, h_buf, u_buf):
        pre = jnp.dot(h_buf[...], w_in[...], preferred_element_type=jnp.float32) + b_in[...]
        bent = jnp.tanh(pre * (GELU_A + GELU_B * (pre * pre)))
        part = 0.5 * pre
        u_buf[...] = (part + part * bent).astype(jnp.bfloat16)
        y_val = jnp.dot(u_buf[...], w_out[...], preferred_element_type=jnp.float32) + b_out[...]
        y_buf[lax.rem(it, 2), half * SUB:half * SUB + SUB, :] = y_val.astype(jnp.bfloat16)

    load_act(0).wait()
    lookup(0, 0, h_one, rows_one)

    moves = []
    for n, (source, target) in enumerate(((m_in, m_out), (v_in, v_out), (master_in, master_out))):
        moves.append(pltpu.make_async_copy(source, state_buf, state_sem.at[2 * n]))
        moves.append(pltpu.make_async_copy(state_buf, target, state_sem.at[2 * n + 1]))

    def body(it, carry):
        @pl.when(it + 1 < steps)
        def _():
            load_act(it + 1).wait()

        @pl.when(it + 2 < steps)
        def _():
            load_act(it + 2).start()

        @pl.when(it >= 2)
        def _():
            store_y(it - 2).wait()
            store_emb(it - 2).wait()
            store_attn(it - 2).wait()

        for n, move in enumerate(moves):
            @pl.when(it == 1 + 2 * n)
            def _(n=n, move=move):
                if n:
                    moves[n - 1].wait()
                move.start()

        lookup(it, 1, h_two, rows_two)
        multiply(it, 0, h_one, u_one)
        lookup(it + 1, 0, h_one, rows_one)
        multiply(it, 1, h_two, u_two)
        for t in range(emb_rows // 16):
            relayout(TENSORS[0][2], D // LANES, it * emb_rows + t * 16, emb_buf.at[lax.rem(it, 2)], t * 16)
        for t in range(attn_rows // 16):
            relayout(TENSORS[1][2], D // LANES, it * attn_rows + t * 16, attn_buf.at[lax.rem(it, 2)], t * 16)
        store_y(it).start()
        store_emb(it).start()
        store_attn(it).start()
        return carry

    lax.fori_loop(0, steps, body, 0)
    for it in (steps - 2, steps - 1):
        store_y(it).wait()
        store_emb(it).wait()
        store_attn(it).wait()
    moves[-1].wait()
    pltpu.make_async_copy(w_in, o_in, weight_sem.at[0]).wait()
    pltpu.make_async_copy(w_out, o_out, weight_sem.at[1]).wait()
    pltpu.make_async_copy(vecd_buf, o_vecd, weight_sem.at[2]).wait()
    pltpu.make_async_copy(vecf_buf, o_vecf, weight_sem.at[3]).wait()


def ffn(ids, act, flat, m_new, v_new, w_new):
    tokens = act.shape[0]
    steps = tokens // CHUNK
    f32, bf16 = jnp.float32, jnp.bfloat16
    shape = jax.ShapeDtypeStruct
    dma = pltpu.SemaphoreType.DMA
    anywhere = pl.BlockSpec(memory_space=pl.ANY)
    state = shape((SHARD, LANES), f32)
    return pl.pallas_call(
        functools.partial(ffn_kernel, steps),
        out_shape=(shape((tokens, D), bf16), shape((VOCAB, D), bf16), shape((4 * D, D), bf16), shape((D, FF), bf16),
                   shape((FF, D), bf16), shape((9, D), bf16), shape((1, FF), bf16), state, state, state),
        in_specs=[pl.BlockSpec(memory_space=pltpu.SMEM)] + [anywhere] * 5,
        out_specs=(anywhere,) * 10,
        scratch_shapes=[
            pltpu.VMEM((DEVICES * SHARD, LANES), f32),
            pltpu.VMEM((RING, PAD, LANES), bf16),
            pltpu.VMEM((ACT_SLOTS, CHUNK, D), bf16),
            pltpu.VMEM((2, CHUNK, D), bf16),
            pltpu.VMEM((D, FF), bf16),
            pltpu.VMEM((FF, D), bf16),
            pltpu.VMEM((1, FF), f32),
            pltpu.VMEM((1, D), f32),
            pltpu.VMEM((9, D), f32),
            pltpu.VMEM((9, D), bf16),
            pltpu.VMEM((1, FF), bf16),
            pltpu.VMEM((SUB * 7 + 8, LANES), f32),
            pltpu.VMEM((SUB * 7 + 8, LANES), f32),
            pltpu.VMEM((SUB, D), bf16),
            pltpu.VMEM((SUB, D), bf16),
            pltpu.VMEM((SUB, FF), bf16),
            pltpu.VMEM((SUB, FF), bf16),
            pltpu.VMEM((2, VOCAB // steps, D), bf16),
            pltpu.VMEM((2, 4 * D // steps, D), bf16),
            pltpu.VMEM((SHARD, LANES), f32),
            dma((RING,)), dma((ACT_SLOTS,)), dma((2,)), dma((2,)), dma((2,)), dma((4,)), dma((6,)),
        ],
        compiler_params=pltpu.CompilerParams(vmem_limit_bytes=VMEM_MAX),
        name="ffn",
    )(ids, act, flat, m_new, v_new, w_new)


def solution(mesh):
    def device_step(g_emb, g_attn, g_in, g_out, g_vecd, g_vecf, opt_m, opt_v, master, tok_ids, act_in):
        vec = jnp.concatenate([
            g_vecd.reshape(-1, LANES), g_vecf.reshape(-1, LANES),
            jnp.zeros((VEC_ROWS - (9 * D + FF) // LANES, LANES), jnp.float32)], axis=0)
        def tiles(grad, cols):
            split = grad.reshape(-1, 8, cols // LANES, LANES)
            return split.transpose(0, 2, 1, 3).reshape(-1, 8, LANES)

        m_new, v_new, w_new, gathered = exchange(
            tiles(g_emb, D), tiles(g_attn, D), tiles(g_in, FF), tiles(g_out, D), vec, opt_m.reshape(SHARD, LANES),
            opt_v.reshape(SHARD, LANES), master.reshape(SHARD, LANES))
        flat = gathered.reshape(DEVICES, PAD, LANES)
        y_out, wb_emb, wb_attn, wb_in, wb_out, wb_vecd, wb_vecf, m_new, v_new, w_new = ffn(
            tok_ids, act_in, flat, m_new, v_new, w_new)
        return (m_new.reshape(-1), v_new.reshape(-1), w_new.reshape(-1), wb_emb, wb_attn.reshape(1, 4, D, D),
                wb_in[None], wb_out[None], wb_vecd[None], wb_vecf, y_out)

    grad_specs = tuple(P(AXES, *([None] * (grad_rank - 1))) for grad_rank in GRAD_RANKS)
    in_specs = grad_specs + (P(AXES), P(AXES), P(AXES), P(AXES), P(AXES, None))
    out_specs = (P(AXES), P(AXES), P(AXES), P(), P(), P(), P(), P(), P(), P(AXES, None))
    return jax.shard_map(device_step, mesh=mesh, in_specs=in_specs, out_specs=out_specs, check_vma=False)
```

```python
import functools
import math

import jax
import jax.numpy as jnp
from jax import lax
from jax.experimental import pallas as pl
from jax.experimental.pallas import tpu as pltpu
from jax.sharding import PartitionSpec as P

LEARN_RATE = 0.002
BETA_ONE = 0.9
BETA_TWO = 0.95
ADAM_EPS = 1e-8
ADAM_STEP = 2
AXES = ("dz", "dy", "dx")
GRAD_RANKS = (3, 5, 4, 4, 4, 3)
MESH = pl.DeviceIdType.MESH

D = 768
FF = 2048
VOCAB = 2048
DEVICES = 16
LANES = 128
SHARD = 3461
PAD = 3472
PART_START = (0, 576, 1152, 1728, 2304, 2880)
PART_ROWS = (576, 576, 576, 576, 576, 592)
PART_MAX = 592
PARTS = 6
VMEM_MAX = 67_000_000

TENSORS = (
    (VOCAB, D, 0),
    (4 * D, D, VOCAB * D // LANES),
    (D, FF, (VOCAB * D + 4 * D * D) // LANES),
    (FF, D, (VOCAB * D + 4 * D * D + D * FF) // LANES),
)
TILES = 48
FLAT_ROWS = 8 * TILES
CHUNKS = 144
SPAN = 11
MARGIN = FLAT_ROWS
SLOT = 2 * MARGIN + 3464
STAGES = 4
VEC_BASE = (VOCAB * D + 4 * D * D + 2 * D * FF) // LANES
VEC_ROWS = DEVICES * SHARD - VEC_BASE


ORDERS = (("x", "y", "z"), ("y", "z", "x"), ("z", "x", "y")) * 2
WEIGHT = {"z": 4, "y": 2, "x": 1}
CHIP_ORDER = ("xyz", "xy", "yz", "zx", "x", "y", "z", "")
HALF_ORDER = ((1, 1), (1, 0), (0, 1), (0, 0))
GATHER_ORDER = ((1, 0, 0), (0, 1, 0), (0, 0, 1), (1, 1, 0), (1, 0, 1), (0, 1, 1), (1, 1, 1))


def exchange_kernel(g_emb, g_attn, g_in, g_out, g_vecd, g_vecf, opt_m, opt_v, master, m_new, v_new, w_new, gathered,
                    stage, vecd_buf, vecf_buf, acc, pair, half, quarter, eighth, m_buf, v_buf, w_buf, wb,
                    stage_sem, vec_sem, pair_send, pair_recv, half_send, half_recv, quarter_send, quarter_recv,
                    eighth_send, eighth_recv, state_sem, store_sem,
                    ring_send, ring_recv, share_send, share_recv, keep_sem):
    z, y, dx = lax.axis_index("dz"), lax.axis_index("dy"), lax.axis_index("dx")
    x, c = dx // 2, dx % 2
    mine = {"z": z, "y": y, "x": x}
    peers = {
        "c": {"dz": z, "dy": y, "dx": 2 * x + (1 - c)},
        "x": {"dz": z, "dy": y, "dx": 2 * (1 - x) + c},
        "y": {"dz": z, "dy": 1 - y, "dx": dx},
        "z": {"dz": 1 - z, "dy": y, "dx": dx},
    }

    def chip(part, bits):
        index = 0
        for axis, bit in zip(ORDERS[part], bits):
            index = index + WEIGHT[axis] * ((1 - mine[axis]) if bit else mine[axis])
        return index

    def rows(part):
        return pl.ds(PART_START[part], PART_ROWS[part])

    def acc_rows(part):
        return pl.ds(MARGIN + PART_START[part], PART_ROWS[part])

    vec_loads = [
        pltpu.make_async_copy(g_vecd, vecd_buf, vec_sem.at[0]), pltpu.make_async_copy(g_vecf, vecf_buf, vec_sem.at[1])]
    state = [
        pltpu.make_async_copy(opt_m, m_buf, state_sem.at[0]),
        pltpu.make_async_copy(opt_v, v_buf, state_sem.at[1]),
        pltpu.make_async_copy(master, w_buf, state_sem.at[2]),
    ]

    parts = range(PARTS)

    def chip_at(n):
        index = 0
        for axis in "zyx":
            index = index + WEIGHT[axis] * ((1 - mine[axis]) if axis in CHIP_ORDER[n] else mine[axis])
        return index

    sequence = [(False, 0)]
    for n in range(1, 8):
        sequence += [(False, n), (True, n - 1)]
    sequence.append((True, 7))

    def shard_at(place):
        own, n = sequence[place]
        return 2 * chip_at(n) + (c if own else 1 - c)

    def chunk_bounds(owner):
        low = (owner * SHARD) // FLAT_ROWS
        high = (owner * SHARD + SHARD + FLAT_ROWS - 1 - (owner // (DEVICES - 1)) * VEC_ROWS) // FLAT_ROWS
        return low, high

    def by_tensor(k, act):
        @pl.when(k < 32)
        def _():
            act(0, 0)

        @pl.when(k >= 32)
        def _():
            @pl.when(k < 80)
            def _():
                act(1, 32)

            @pl.when(k >= 80)
            def _():
                @pl.when(k < 112)
                def _():
                    act(2, 80)

                @pl.when(k >= 112)
                def _():
                    act(3, 112)

    grads = (g_emb, g_attn, g_in, g_out)

    def load_shard(place):
        low, high = chunk_bounds(shard_at(place))
        slot = place % STAGES

        def one(k, carry):
            where = k - low

            def start(tensor, first):
                pltpu.make_async_copy(
                    grads[tensor].at[pl.ds((k - first) * TILES, TILES)], stage.at[slot, pl.ds(where * TILES, TILES)],
                    stage_sem.at[slot, where]).start()

            by_tensor(k, start)
            return carry

        lax.fori_loop(low, high, one, 0)

    def flatten_shard(place):
        owner = shard_at(place)
        low, high = chunk_bounds(owner)
        slot = place % STAGES
        where = chip_at(sequence[place][1])

        def one(k, carry):
            at = k - low
            pltpu.make_async_copy(
                g_emb.at[pl.ds(0, TILES)], stage.at[slot, pl.ds(at * TILES, TILES)], stage_sem.at[slot, at]).wait()
            base = MARGIN + k * FLAT_ROWS - owner * SHARD

            def spread(tensor, first):
                groups = TENSORS[tensor][1] // LANES
                bands = TILES // groups
                for j in range(groups):
                    tile = stage[slot, pl.ds(at * TILES + j, bands, stride=groups)]
                    acc[where, pl.ds(base + j, 8 * bands, stride=groups), :] = tile.reshape(8 * bands, LANES)

            by_tensor(k, spread)
            return carry

        lax.fori_loop(low, high, one, 0)

        @pl.when(owner == DEVICES - 1)
        def _():
            first = MARGIN + SHARD - VEC_ROWS
            second = first + 9 * D // LANES
            third = second + FF // LANES
            acc[where, first:second, :] = vecd_buf[...]
            acc[where, second:third, :] = vecf_buf[...]
            acc[where, third:MARGIN + SHARD, :] = jnp.zeros((MARGIN + SHARD - third, LANES), jnp.float32)

    def pair_copy(n, part):
        where = chip_at(n)
        return pltpu.make_async_remote_copy(
            src_ref=acc.at[where, acc_rows(part)], dst_ref=pair.at[where, rows(part)],
            send_sem=pair_send.at[n, part], recv_sem=pair_recv.at[n, part],
            device_id=peers["c"], device_id_type=MESH)

    def half_copy(k, part):
        return pltpu.make_async_remote_copy(
            src_ref=acc.at[chip(part, (1,) + HALF_ORDER[k]), acc_rows(part)],
            dst_ref=half.at[part, k, pl.ds(0, PART_ROWS[part])],
            send_sem=half_send.at[k, part], recv_sem=half_recv.at[k, part],
            device_id=peers[ORDERS[part][0]], device_id_type=MESH)

    def quarter_copy(k, part):
        return pltpu.make_async_remote_copy(
            src_ref=acc.at[chip(part, (0, 1, 1 - k)), acc_rows(part)],
            dst_ref=quarter.at[part, k, pl.ds(0, PART_ROWS[part])],
            send_sem=quarter_send.at[k, part], recv_sem=quarter_recv.at[k, part],
            device_id=peers[ORDERS[part][1]], device_id_type=MESH)

    def eighth_copy(part):
        return pltpu.make_async_remote_copy(
            src_ref=acc.at[chip(part, (0, 0, 1)), acc_rows(part)],
            dst_ref=eighth.at[part, pl.ds(0, PART_ROWS[part])],
            send_sem=eighth_send.at[part], recv_sem=eighth_recv.at[part],
            device_id=peers[ORDERS[part][2]], device_id_type=MESH)

    for place in range(STAGES):
        load_shard(place)
    for copy in vec_loads:
        copy.start()
    barrier = pltpu.get_barrier_semaphore()
    for peer in peers.values():
        pl.semaphore_signal(barrier, inc=1, device_id=peer, device_id_type=MESH)
    pl.semaphore_wait(barrier, 4)
    for copy in vec_loads:
        copy.wait()

    for place, (own, n) in enumerate(sequence):
        if own:
            for part in parts:
                pair_copy(n, part).wait_send()
        flatten_shard(place)
        if place + STAGES < len(sequence):
            load_shard(place + STAGES)
        where = chip_at(n)
        for part in parts:
            if not own:
                pair_copy(n, part).start()
                continue
            pair_copy(n, part).wait_recv()
            acc[where, acc_rows(part)] += pair[where, rows(part)]
            bits = tuple(int(axis in CHIP_ORDER[n]) for axis in ORDERS[part])
            if bits[0]:
                half_copy(HALF_ORDER.index(bits[1:]), part).start()
    for copy in state:
        copy.start()
    for k in range(4):
        for part in parts:
            half_copy(k, part).wait_recv()
            where = chip(part, (0,) + HALF_ORDER[k])
            acc[where, acc_rows(part)] += half[part, k, pl.ds(0, PART_ROWS[part])]
            if k < 2:
                quarter_copy(k, part).start()
    for k in range(2):
        for part in parts:
            quarter_copy(k, part).wait_recv()
            where = chip(part, (0, 0, 1 - k))
            acc[where, acc_rows(part)] += quarter[part, k, pl.ds(0, PART_ROWS[part])]
            if k == 0:
                eighth_copy(part).start()

    for copy in state:
        copy.wait()

    here = 4 * z + 2 * y + x

    def ring_copy(bits, hop, part):
        flipped = tuple(1 - bit if n == hop else bit for n, bit in enumerate(bits))
        slot = flipped[0] * 4 + flipped[1] * 2 + flipped[2]
        where = chip(part, bits)
        return pltpu.make_async_remote_copy(
            src_ref=wb.at[where, rows(part)], dst_ref=wb.at[where, rows(part)],
            send_sem=ring_send.at[slot, part], recv_sem=ring_recv.at[slot, part],
            device_id=peers[ORDERS[part][hop]], device_id_type=MESH)

    def share_copy(bits, part):
        slot = bits[0] * 4 + bits[1] * 2 + bits[2]
        where = chip(part, bits)
        return pltpu.make_async_remote_copy(
            src_ref=wb.at[where, rows(part)], dst_ref=gathered.at[where, c, rows(part)],
            send_sem=share_send.at[slot, part], recv_sem=share_recv.at[slot, part],
            device_id=peers["c"], device_id_type=MESH)

    def keep_copy(bits, part):
        slot = bits[0] * 4 + bits[1] * 2 + bits[2]
        where = chip(part, bits)
        return pltpu.make_async_copy(
            wb.at[where, rows(part)], gathered.at[where, c, rows(part)], keep_sem.at[slot, part])

    for part in parts:
        eighth_copy(part).wait_recv()
        start, count = PART_START[part], min(PART_ROWS[part], SHARD - PART_START[part])
        pieces = [(start, count)] if count % 16 == 0 else [(start, count // 16 * 16), (start + count // 16 * 16, count % 16)]
        for first, size in pieces:
            span = pl.ds(first, size)
            grad_sum = (acc[here, pl.ds(MARGIN + first, size)] + eighth[part, pl.ds(first - start, size)]) / DEVICES
            m_val = BETA_ONE * m_buf[span] + (1.0 - BETA_ONE) * grad_sum
            v_val = BETA_TWO * v_buf[span] + (1.0 - BETA_TWO) * grad_sum * grad_sum
            m_hat = m_val / (1.0 - BETA_ONE ** ADAM_STEP)
            v_hat = v_val / (1.0 - BETA_TWO ** ADAM_STEP)
            w_val = w_buf[span] - LEARN_RATE * m_hat / (jnp.sqrt(v_hat) + ADAM_EPS)
            m_buf[span] = m_val
            v_buf[span] = v_val
            w_buf[span] = w_val
            if size % 16:
                w_val = jnp.concatenate([w_val, jnp.zeros((16 - size % 16, LANES), jnp.float32)], axis=0)
                span = pl.ds(first, 16)
            wb[here, span] = w_val.astype(jnp.bfloat16)
        for hop in range(3):
            ring_copy((0, 0, 0), hop, part).start()
        share_copy((0, 0, 0), part).start()
        keep_copy((0, 0, 0), part).start()

    store = [
        pltpu.make_async_copy(m_buf, m_new, store_sem.at[0]),
        pltpu.make_async_copy(v_buf, v_new, store_sem.at[1]),
        pltpu.make_async_copy(w_buf, w_new, store_sem.at[2]),
    ]
    for copy in store:
        copy.start()

    def last_hop(bits):
        return max(n for n in range(3) if bits[n])

    for bits in GATHER_ORDER:
        hop = last_hop(bits)
        came = tuple(1 - bit if n == hop else bit for n, bit in enumerate(bits))
        for part in parts:
            ring_copy(came, hop, part).wait_recv()
            for later in range(hop + 1, 3):
                ring_copy(bits, later, part).start()
            share_copy(bits, part).start()
            keep_copy(bits, part).start()

    for part in parts:
        for k in range(4):
            half_copy(k, part).wait_send()
        for k in range(2):
            quarter_copy(k, part).wait_send()
        eighth_copy(part).wait_send()
        for bits in ((0, 0, 0),) + GATHER_ORDER:
            for later in range(0 if not any(bits) else last_hop(bits) + 1, 3):
                ring_copy(bits, later, part).wait_send()
            share_copy(bits, part).wait()
            keep_copy(bits, part).wait()
    for copy in store:
        copy.wait()


def exchange(*operands):
    shape = jax.ShapeDtypeStruct
    state_shape = shape((SHARD, LANES), jnp.float32)
    f32 = functools.partial(pltpu.VMEM, dtype=jnp.float32)
    dma = pltpu.SemaphoreType.DMA
    scratch = [
        f32((STAGES, SPAN * TILES, 8, LANES)), f32((9 * D // LANES, LANES)), f32((FF // LANES, LANES)),
        f32((8, SLOT, LANES)), f32((8, PAD, LANES)),
        f32((PARTS, 4, PART_MAX, LANES)), f32((PARTS, 2, PART_MAX, LANES)), f32((PARTS, PART_MAX, LANES)),
        f32((SHARD, LANES)), f32((SHARD, LANES)), f32((SHARD, LANES)),
        pltpu.VMEM((8, PAD, LANES), jnp.bfloat16),
        dma((STAGES, SPAN)), dma((2,)), dma((8, PARTS)), dma((8, PARTS)),
        dma((4, PARTS)), dma((4, PARTS)), dma((2, PARTS)), dma((2, PARTS)),
        dma((PARTS,)), dma((PARTS,)), dma((3,)), dma((3,)),
        dma((8, PARTS)), dma((8, PARTS)), dma((8, PARTS)), dma((8, PARTS)), dma((8, PARTS)),
    ]
    return pl.pallas_call(
        exchange_kernel,
        out_shape=(state_shape, state_shape, state_shape, shape((8, 2, PAD, LANES), jnp.bfloat16)),
        in_specs=[pl.BlockSpec(memory_space=pl.ANY)] * 9,
        out_specs=(pl.BlockSpec(memory_space=pl.ANY),) * 4,
        scratch_shapes=scratch,
        compiler_params=pltpu.CompilerParams(vmem_limit_bytes=VMEM_MAX, collective_id=0, has_side_effects=True),
        name="exchange",
    )(*operands)


SUB = 512
UNROLL = 2
CHUNK = UNROLL * SUB
RING = 6
ACT_SLOTS = 2 * UNROLL
GELU_A = math.sqrt(2.0 / math.pi)
GELU_B = GELU_A * 0.044715
WIDEN_ORDER = (8, 9, 10, 11, 12, 13, 14, 15, 0, 1, 2, 3, 4, 5, 6, 7)


def ffn_kernel(steps, ids, act, flat, m_in, v_in, master_in,
               y_out, o_emb, o_attn, o_in, o_out, o_vecd, o_vecf, m_out, v_out, master_out,
               dense, ring, act_buf, y_buf, w_in, w_out, b_in, b_out, vecd_wide, vecd_buf, vecf_buf,
               rows_one, rows_two, h_one, h_two, u_one, u_two, emb_buf, attn_buf, state_buf,
               ring_sem, act_sem, y_sem, emb_sem, attn_sem, weight_sem, state_sem):
    emb_rows, attn_rows = VOCAB // steps, 4 * D // steps

    blocks = steps * UNROLL

    def load_act(block):
        slot = lax.rem(block, ACT_SLOTS)
        return pltpu.make_async_copy(act.at[pl.ds(block * SUB, SUB)], act_buf.at[slot], act_sem.at[slot])

    def store_y(it):
        return pltpu.make_async_copy(
            y_buf.at[lax.rem(it, 2)], y_out.at[pl.ds(it * CHUNK, CHUNK)], y_sem.at[lax.rem(it, 2)])

    def store_emb(it):
        return pltpu.make_async_copy(
            emb_buf.at[lax.rem(it, 2)], o_emb.at[pl.ds(it * emb_rows, emb_rows)], emb_sem.at[lax.rem(it, 2)])

    def store_attn(it):
        return pltpu.make_async_copy(
            attn_buf.at[lax.rem(it, 2)], o_attn.at[pl.ds(it * attn_rows, attn_rows)], attn_sem.at[lax.rem(it, 2)])

    def load_flat(n):
        return pltpu.make_async_copy(flat.at[WIDEN_ORDER[n]], ring.at[n % RING], ring_sem.at[n % RING])

    for n in range(RING):
        load_flat(n).start()
    for block in range(UNROLL + 1):
        load_act(block).start()

    def relayout(base, groups, row, buf, at):
        for j in range(groups):
            q = base + row * groups + j
            top = dense[pl.ds(q, 8, stride=groups), :]
            low = dense[pl.ds(q + 8 * groups, 8, stride=groups), :]
            buf[pl.ds(at, 16), j * LANES:(j + 1) * LANES] = jnp.concatenate([top, low], axis=0).astype(jnp.bfloat16)

    for n, owner in enumerate(WIDEN_ORDER):
        load_flat(n).wait()
        at = owner * SHARD
        whole = SHARD // 16

        def widen(t, carry, at=at, slot=n % RING):
            row = pl.multiple_of(t * 16, 16)
            dense[pl.ds(at + row, 16), :] = ring[slot, pl.ds(row, 16), :].astype(jnp.float32)
            return carry

        lax.fori_loop(0, whole, widen, 0, unroll=24)
        tail = ring[n % RING, whole * 16:whole * 16 + 16, :].astype(jnp.float32)
        dense[at + whole * 16:at + SHARD, :] = tail[:SHARD - whole * 16]
        if n + RING < DEVICES:
            load_flat(n + RING).start()
        if owner == 12:
            def fill_in(t, carry):
                row = pl.multiple_of(t * 16, 16)
                relayout(TENSORS[2][2], FF // LANES, row, w_in, row)
                return carry

            lax.fori_loop(0, D // 16, fill_in, 0, unroll=2)
            pltpu.make_async_copy(w_in, o_in, weight_sem.at[0]).start()
        if owner == 15:
            def fill_out(t, carry):
                row = pl.multiple_of(t * 16, 16)
                relayout(TENSORS[3][2], D // LANES, row, w_out, row)
                return carry

            lax.fori_loop(0, FF // 16, fill_out, 0, unroll=4)
            pltpu.make_async_copy(w_out, o_out, weight_sem.at[1]).start()
            for i in range(9):
                for j in range(D // LANES):
                    q = VEC_BASE + i * (D // LANES) + j
                    vecd_wide[i:i + 1, j * LANES:(j + 1) * LANES] = dense[q:q + 1, :]
            for j in range(D // LANES):
                q = VEC_BASE + 8 * (D // LANES) + j
                b_out[:, j * LANES:(j + 1) * LANES] = dense[q:q + 1, :]
            for j in range(FF // LANES):
                q = VEC_BASE + 9 * (D // LANES) + j
                b_in[:, j * LANES:(j + 1) * LANES] = dense[q:q + 1, :]
            vecd_buf[...] = vecd_wide[...].astype(jnp.bfloat16)
            vecf_buf[...] = b_in[...].astype(jnp.bfloat16)
            pltpu.make_async_copy(vecd_buf, o_vecd, weight_sem.at[2]).start()
            pltpu.make_async_copy(vecf_buf, o_vecf, weight_sem.at[3]).start()

    def lookup(block, h_buf, rows_buf):
        slot = lax.rem(block, ACT_SLOTS)
        token = jnp.minimum(block, blocks - 1) * SUB
        for tile in range(SUB // 8):
            for i in range(8):
                row = ids[token + tile * 8 + i] * (D // LANES)
                rows_buf[pl.ds(tile * 56 + i * 7, 8), :] = dense[pl.ds(row, 8), :]
        for pair in range(SUB // 16):
            for j in range(D // LANES):
                top = rows_buf[pl.ds(pair * 112 + j, 8, stride=7), :]
                low = rows_buf[pl.ds(pair * 112 + 56 + j, 8, stride=7), :]
                both = jnp.concatenate([top, low], axis=0) * math.sqrt(D)
                a_val = act_buf[slot, pair * 16:pair * 16 + 16, j * LANES:(j + 1) * LANES].astype(jnp.float32)
                h_buf[pair * 16:pair * 16 + 16, j * LANES:(j + 1) * LANES] = (both + a_val).astype(jnp.bfloat16)

    def multiply(it, part, h_buf, u_buf):
        pre = jnp.dot(h_buf[...], w_in[...], preferred_element_type=jnp.float32) + b_in[...]
        bent = jnp.tanh(pre * (GELU_A + GELU_B * (pre * pre)))
        flat_half = 0.5 * pre
        u_buf[...] = (flat_half + flat_half * bent).astype(jnp.bfloat16)
        y_val = jnp.dot(u_buf[...], w_out[...], preferred_element_type=jnp.float32) + b_out[...]
        y_buf[lax.rem(it, 2), part * SUB:part * SUB + SUB, :] = y_val.astype(jnp.bfloat16)

    load_act(0).wait()
    lookup(0, h_one, rows_one)

    moves = []
    for n, (source, target) in enumerate(((m_in, m_out), (v_in, v_out), (master_in, master_out))):
        moves.append(pltpu.make_async_copy(source, state_buf, state_sem.at[2 * n]))
        moves.append(pltpu.make_async_copy(state_buf, target, state_sem.at[2 * n + 1]))

    def body(it, carry):
        for part in range(1, UNROLL):
            load_act(it * UNROLL + part).wait()

        @pl.when(it + 1 < steps)
        def _():
            load_act(it * UNROLL + UNROLL).wait()
            for part in range(UNROLL + 1, 2 * UNROLL):
                load_act(it * UNROLL + part).start()

        @pl.when(it + 2 < steps)
        def _():
            load_act(it * UNROLL + 2 * UNROLL).start()

        @pl.when(it >= 2)
        def _():
            store_y(it - 2).wait()
            store_emb(it - 2).wait()
            store_attn(it - 2).wait()

        for n, move in enumerate(moves):
            @pl.when(it == 1 + n)
            def _(n=n, move=move):
                if n:
                    moves[n - 1].wait()
                move.start()

        buffers = ((h_one, rows_one, u_one), (h_two, rows_two, u_two))
        for part in range(UNROLL):
            h_now, _, u_now = buffers[part % 2]
            h_next, rows_next, _ = buffers[(part + 1) % 2]
            lookup(it * UNROLL + part + 1, h_next, rows_next)
            multiply(it, part, h_now, u_now)
        for t in range(emb_rows // 16):
            relayout(TENSORS[0][2], D // LANES, it * emb_rows + t * 16, emb_buf.at[lax.rem(it, 2)], t * 16)
        for t in range(attn_rows // 16):
            relayout(TENSORS[1][2], D // LANES, it * attn_rows + t * 16, attn_buf.at[lax.rem(it, 2)], t * 16)
        store_y(it).start()
        store_emb(it).start()
        store_attn(it).start()
        return carry

    lax.fori_loop(0, steps, body, 0)
    for it in (steps - 2, steps - 1):
        store_y(it).wait()
        store_emb(it).wait()
        store_attn(it).wait()
    moves[-1].wait()
    pltpu.make_async_copy(w_in, o_in, weight_sem.at[0]).wait()
    pltpu.make_async_copy(w_out, o_out, weight_sem.at[1]).wait()
    pltpu.make_async_copy(vecd_buf, o_vecd, weight_sem.at[2]).wait()
    pltpu.make_async_copy(vecf_buf, o_vecf, weight_sem.at[3]).wait()


def ffn(ids, act, flat, m_new, v_new, w_new):
    tokens = act.shape[0]
    steps = tokens // CHUNK
    f32, bf16 = jnp.float32, jnp.bfloat16
    shape = jax.ShapeDtypeStruct
    dma = pltpu.SemaphoreType.DMA
    anywhere = pl.BlockSpec(memory_space=pl.ANY)
    state = shape((SHARD, LANES), f32)
    return pl.pallas_call(
        functools.partial(ffn_kernel, steps),
        out_shape=(shape((tokens, D), bf16), shape((VOCAB, D), bf16), shape((4 * D, D), bf16), shape((D, FF), bf16),
                   shape((FF, D), bf16), shape((9, D), bf16), shape((1, FF), bf16), state, state, state),
        in_specs=[pl.BlockSpec(memory_space=pltpu.SMEM)] + [anywhere] * 5,
        out_specs=(anywhere,) * 10,
        scratch_shapes=[
            pltpu.VMEM((DEVICES * SHARD, LANES), f32),
            pltpu.VMEM((RING, PAD, LANES), bf16),
            pltpu.VMEM((ACT_SLOTS, SUB, D), bf16),
            pltpu.VMEM((2, CHUNK, D), bf16),
            pltpu.VMEM((D, FF), bf16),
            pltpu.VMEM((FF, D), bf16),
            pltpu.VMEM((1, FF), f32),
            pltpu.VMEM((1, D), f32),
            pltpu.VMEM((9, D), f32),
            pltpu.VMEM((9, D), bf16),
            pltpu.VMEM((1, FF), bf16),
            pltpu.VMEM((SUB * 7 + 8, LANES), f32),
            pltpu.VMEM((SUB * 7 + 8, LANES), f32),
            pltpu.VMEM((SUB, D), bf16),
            pltpu.VMEM((SUB, D), bf16),
            pltpu.VMEM((SUB, FF), bf16),
            pltpu.VMEM((SUB, FF), bf16),
            pltpu.VMEM((2, VOCAB // steps, D), bf16),
            pltpu.VMEM((2, 4 * D // steps, D), bf16),
            pltpu.VMEM((SHARD, LANES), f32),
            dma((RING,)), dma((ACT_SLOTS,)), dma((2,)), dma((2,)), dma((2,)), dma((4,)), dma((6,)),
        ],
        compiler_params=pltpu.CompilerParams(vmem_limit_bytes=VMEM_MAX),
        name="ffn",
    )(ids, act, flat, m_new, v_new, w_new)


def solution(mesh):
    def device_step(g_emb, g_attn, g_in, g_out, g_vecd, g_vecf, opt_m, opt_v, master, tok_ids, act_in):
        def tiles(grad, cols):
            split = grad.reshape(-1, 8, cols // LANES, LANES)
            return split.transpose(0, 2, 1, 3).reshape(-1, 8, LANES)

        m_new, v_new, w_new, gathered = exchange(
            tiles(g_emb, D), tiles(g_attn, D), tiles(g_in, FF), tiles(g_out, D),
            g_vecd.reshape(-1, LANES), g_vecf.reshape(-1, LANES), opt_m.reshape(SHARD, LANES),
            opt_v.reshape(SHARD, LANES), master.reshape(SHARD, LANES))
        flat = gathered.reshape(DEVICES, PAD, LANES)
        y_out, wb_emb, wb_attn, wb_in, wb_out, wb_vecd, wb_vecf, m_new, v_new, w_new = ffn(
            tok_ids, act_in, flat, m_new, v_new, w_new)
        return (m_new.reshape(-1), v_new.reshape(-1), w_new.reshape(-1), wb_emb, wb_attn.reshape(1, 4, D, D),
                wb_in[None], wb_out[None], wb_vecd[None], wb_vecf, y_out)

    grad_specs = tuple(P(AXES, *([None] * (grad_rank - 1))) for grad_rank in GRAD_RANKS)
    in_specs = grad_specs + (P(AXES), P(AXES), P(AXES), P(AXES), P(AXES, None))
    out_specs = (P(AXES), P(AXES), P(AXES), P(), P(), P(), P(), P(), P(), P(AXES, None))
    return jax.shard_map(device_step, mesh=mesh, in_specs=in_specs, out_specs=out_specs, check_vma=False)
```

```python
import functools
import math

import jax
import jax.numpy as jnp
from jax import lax
from jax.experimental import pallas as pl
from jax.experimental.pallas import tpu as pltpu
from jax.sharding import PartitionSpec as P

LEARN_RATE = 0.002
BETA_ONE = 0.9
BETA_TWO = 0.95
ADAM_EPS = 1e-8
ADAM_STEP = 2
AXES = ("dz", "dy", "dx")
GRAD_RANKS = (3, 5, 4, 4, 4, 3)
MESH = pl.DeviceIdType.MESH

D = 768
FF = 2048
VOCAB = 2048
DEVICES = 16
LANES = 128
SHARD = 3461
PAD = 3472
PART_START = (0, 576, 1152, 1728, 2304, 2880)
PART_ROWS = (576, 576, 576, 576, 576, 592)
PART_MAX = 592
PARTS = 6
VMEM_MAX = 67_000_000

TENSORS = (
    (VOCAB, D, 0),
    (4 * D, D, VOCAB * D // LANES),
    (D, FF, (VOCAB * D + 4 * D * D) // LANES),
    (FF, D, (VOCAB * D + 4 * D * D + D * FF) // LANES),
)
TILES = 48
FLAT_ROWS = 8 * TILES
CHUNKS = 144
SPAN = 11
MARGIN = FLAT_ROWS
SLOT = 2 * MARGIN + 3464
STAGES = 4
VEC_BASE = (VOCAB * D + 4 * D * D + 2 * D * FF) // LANES
VEC_ROWS = DEVICES * SHARD - VEC_BASE


ORDERS = (("x", "y", "z"), ("y", "z", "x"), ("z", "x", "y")) * 2
WEIGHT = {"z": 4, "y": 2, "x": 1}
CHIP_ORDER = ("xyz", "xy", "yz", "zx", "x", "y", "z", "")
HALF_ORDER = ((1, 1), (1, 0), (0, 1), (0, 0))
GATHER_ORDER = ((1, 0, 0), (0, 1, 0), (0, 0, 1), (1, 1, 0), (1, 0, 1), (0, 1, 1), (1, 1, 1))


def exchange_kernel(g_emb, g_attn, g_in, g_out, g_vecd, g_vecf, opt_m, opt_v, master, m_new, v_new, w_new, gathered,
                    stage, vecd_buf, vecf_buf, acc, pair, half, quarter, eighth, m_buf, v_buf, w_buf, wb,
                    stage_sem, vec_sem, pair_send, pair_recv, half_send, half_recv, quarter_send, quarter_recv,
                    eighth_send, eighth_recv, state_sem, store_sem,
                    ring_send, ring_recv, share_send, share_recv, keep_sem):
    z, y, dx = lax.axis_index("dz"), lax.axis_index("dy"), lax.axis_index("dx")
    x, c = dx // 2, dx % 2
    mine = {"z": z, "y": y, "x": x}
    peers = {
        "c": {"dz": z, "dy": y, "dx": 2 * x + (1 - c)},
        "x": {"dz": z, "dy": y, "dx": 2 * (1 - x) + c},
        "y": {"dz": z, "dy": 1 - y, "dx": dx},
        "z": {"dz": 1 - z, "dy": y, "dx": dx},
    }

    def chip(part, bits):
        index = 0
        for axis, bit in zip(ORDERS[part], bits):
            index = index + WEIGHT[axis] * ((1 - mine[axis]) if bit else mine[axis])
        return index

    def rows(part):
        return pl.ds(PART_START[part], PART_ROWS[part])

    def acc_rows(part):
        return pl.ds(MARGIN + PART_START[part], PART_ROWS[part])

    vec_loads = [
        pltpu.make_async_copy(g_vecd, vecd_buf, vec_sem.at[0]), pltpu.make_async_copy(g_vecf, vecf_buf, vec_sem.at[1])]
    state = [
        pltpu.make_async_copy(opt_m, m_buf, state_sem.at[0]),
        pltpu.make_async_copy(opt_v, v_buf, state_sem.at[1]),
        pltpu.make_async_copy(master, w_buf, state_sem.at[2]),
    ]

    parts = range(PARTS)

    def chip_at(n):
        index = 0
        for axis in "zyx":
            index = index + WEIGHT[axis] * ((1 - mine[axis]) if axis in CHIP_ORDER[n] else mine[axis])
        return index

    sequence = [(False, 0)]
    for n in range(1, 8):
        sequence += [(False, n), (True, n - 1)]
    sequence.append((True, 7))

    def shard_at(place):
        own, n = sequence[place]
        return 2 * chip_at(n) + (c if own else 1 - c)

    def chunk_bounds(owner):
        low = (owner * SHARD) // FLAT_ROWS
        high = (owner * SHARD + SHARD + FLAT_ROWS - 1 - (owner // (DEVICES - 1)) * VEC_ROWS) // FLAT_ROWS
        return low, high

    def by_tensor(k, act):
        @pl.when(k < 32)
        def _():
            act(0, 0)

        @pl.when(k >= 32)
        def _():
            @pl.when(k < 80)
            def _():
                act(1, 32)

            @pl.when(k >= 80)
            def _():
                @pl.when(k < 112)
                def _():
                    act(2, 80)

                @pl.when(k >= 112)
                def _():
                    act(3, 112)

    grads = (g_emb, g_attn, g_in, g_out)

    def load_shard(place):
        low, high = chunk_bounds(shard_at(place))
        slot = place % STAGES

        def one(k, carry):
            where = k - low

            def start(tensor, first):
                pltpu.make_async_copy(
                    grads[tensor].at[pl.ds((k - first) * TILES, TILES)], stage.at[slot, pl.ds(where * TILES, TILES)],
                    stage_sem.at[slot, where]).start()

            by_tensor(k, start)
            return carry

        lax.fori_loop(low, high, one, 0)

    def flatten_shard(place):
        owner = shard_at(place)
        low, high = chunk_bounds(owner)
        slot = place % STAGES
        where = chip_at(sequence[place][1])

        def one(k, carry):
            at = k - low
            pltpu.make_async_copy(
                g_emb.at[pl.ds(0, TILES)], stage.at[slot, pl.ds(at * TILES, TILES)], stage_sem.at[slot, at]).wait()
            base = MARGIN + k * FLAT_ROWS - owner * SHARD

            def spread(tensor, first):
                groups = TENSORS[tensor][1] // LANES
                bands = TILES // groups
                for j in range(groups):
                    tile = stage[slot, pl.ds(at * TILES + j, bands, stride=groups)]
                    acc[where, pl.ds(base + j, 8 * bands, stride=groups), :] = tile.reshape(8 * bands, LANES)

            by_tensor(k, spread)
            return carry

        lax.fori_loop(low, high, one, 0)

        @pl.when(owner == DEVICES - 1)
        def _():
            first = MARGIN + SHARD - VEC_ROWS
            second = first + 9 * D // LANES
            third = second + FF // LANES
            acc[where, first:second, :] = vecd_buf[...]
            acc[where, second:third, :] = vecf_buf[...]
            acc[where, third:MARGIN + SHARD, :] = jnp.zeros((MARGIN + SHARD - third, LANES), jnp.float32)

    def pair_copy(n, part):
        where = chip_at(n)
        return pltpu.make_async_remote_copy(
            src_ref=acc.at[where, acc_rows(part)], dst_ref=pair.at[where, rows(part)],
            send_sem=pair_send.at[n, part], recv_sem=pair_recv.at[n, part],
            device_id=peers["c"], device_id_type=MESH)

    def half_copy(k, part):
        return pltpu.make_async_remote_copy(
            src_ref=acc.at[chip(part, (1,) + HALF_ORDER[k]), acc_rows(part)],
            dst_ref=half.at[part, k, pl.ds(0, PART_ROWS[part])],
            send_sem=half_send.at[k, part], recv_sem=half_recv.at[k, part],
            device_id=peers[ORDERS[part][0]], device_id_type=MESH)

    def quarter_copy(k, part):
        return pltpu.make_async_remote_copy(
            src_ref=acc.at[chip(part, (0, 1, 1 - k)), acc_rows(part)],
            dst_ref=quarter.at[part, k, pl.ds(0, PART_ROWS[part])],
            send_sem=quarter_send.at[k, part], recv_sem=quarter_recv.at[k, part],
            device_id=peers[ORDERS[part][1]], device_id_type=MESH)

    def eighth_copy(part):
        return pltpu.make_async_remote_copy(
            src_ref=acc.at[chip(part, (0, 0, 1)), acc_rows(part)],
            dst_ref=eighth.at[part, pl.ds(0, PART_ROWS[part])],
            send_sem=eighth_send.at[part], recv_sem=eighth_recv.at[part],
            device_id=peers[ORDERS[part][2]], device_id_type=MESH)

    for place in range(STAGES):
        load_shard(place)
    for copy in vec_loads:
        copy.start()
    barrier = pltpu.get_barrier_semaphore()
    for peer in peers.values():
        pl.semaphore_signal(barrier, inc=1, device_id=peer, device_id_type=MESH)
    pl.semaphore_wait(barrier, 4)
    for copy in vec_loads:
        copy.wait()

    for place, (own, n) in enumerate(sequence):
        if own:
            for part in parts:
                pair_copy(n, part).wait_send()
        flatten_shard(place)
        if place + STAGES < len(sequence):
            load_shard(place + STAGES)
        where = chip_at(n)
        for part in parts:
            if not own:
                pair_copy(n, part).start()
                continue
            pair_copy(n, part).wait_recv()
            acc[where, acc_rows(part)] += pair[where, rows(part)]
            bits = tuple(int(axis in CHIP_ORDER[n]) for axis in ORDERS[part])
            if bits[0]:
                half_copy(HALF_ORDER.index(bits[1:]), part).start()
    for copy in state:
        copy.start()
    for k in range(4):
        for part in parts:
            half_copy(k, part).wait_recv()
            where = chip(part, (0,) + HALF_ORDER[k])
            acc[where, acc_rows(part)] += half[part, k, pl.ds(0, PART_ROWS[part])]
            if k < 2:
                quarter_copy(k, part).start()
    for k in range(2):
        for part in parts:
            quarter_copy(k, part).wait_recv()
            where = chip(part, (0, 0, 1 - k))
            acc[where, acc_rows(part)] += quarter[part, k, pl.ds(0, PART_ROWS[part])]
            if k == 0:
                eighth_copy(part).start()

    for copy in state:
        copy.wait()

    here = 4 * z + 2 * y + x

    def ring_copy(bits, hop, part):
        flipped = tuple(1 - bit if n == hop else bit for n, bit in enumerate(bits))
        slot = flipped[0] * 4 + flipped[1] * 2 + flipped[2]
        where = chip(part, bits)
        return pltpu.make_async_remote_copy(
            src_ref=wb.at[where, rows(part)], dst_ref=wb.at[where, rows(part)],
            send_sem=ring_send.at[slot, part], recv_sem=ring_recv.at[slot, part],
            device_id=peers[ORDERS[part][hop]], device_id_type=MESH)

    def share_copy(bits, part):
        slot = bits[0] * 4 + bits[1] * 2 + bits[2]
        where = chip(part, bits)
        return pltpu.make_async_remote_copy(
            src_ref=wb.at[where, rows(part)], dst_ref=gathered.at[where, c, rows(part)],
            send_sem=share_send.at[slot, part], recv_sem=share_recv.at[slot, part],
            device_id=peers["c"], device_id_type=MESH)

    def keep_copy(bits, part):
        slot = bits[0] * 4 + bits[1] * 2 + bits[2]
        where = chip(part, bits)
        return pltpu.make_async_copy(
            wb.at[where, rows(part)], gathered.at[where, c, rows(part)], keep_sem.at[slot, part])

    for part in parts:
        eighth_copy(part).wait_recv()
        start, count = PART_START[part], min(PART_ROWS[part], SHARD - PART_START[part])
        pieces = [(start, count)] if count % 16 == 0 else [(start, count // 16 * 16), (start + count // 16 * 16, count % 16)]
        for first, size in pieces:
            span = pl.ds(first, size)
            grad_sum = (acc[here, pl.ds(MARGIN + first, size)] + eighth[part, pl.ds(first - start, size)]) / DEVICES
            m_val = BETA_ONE * m_buf[span] + (1.0 - BETA_ONE) * grad_sum
            v_val = BETA_TWO * v_buf[span] + (1.0 - BETA_TWO) * grad_sum * grad_sum
            m_hat = m_val / (1.0 - BETA_ONE ** ADAM_STEP)
            v_hat = v_val / (1.0 - BETA_TWO ** ADAM_STEP)
            w_val = w_buf[span] - LEARN_RATE * m_hat / (jnp.sqrt(v_hat) + ADAM_EPS)
            m_buf[span] = m_val
            v_buf[span] = v_val
            w_buf[span] = w_val
            if size % 16:
                w_val = jnp.concatenate([w_val, jnp.zeros((16 - size % 16, LANES), jnp.float32)], axis=0)
                span = pl.ds(first, 16)
            wb[here, span] = w_val.astype(jnp.bfloat16)
        for hop in range(3):
            ring_copy((0, 0, 0), hop, part).start()
        share_copy((0, 0, 0), part).start()
        keep_copy((0, 0, 0), part).start()

    store = [
        pltpu.make_async_copy(m_buf, m_new, store_sem.at[0]),
        pltpu.make_async_copy(v_buf, v_new, store_sem.at[1]),
        pltpu.make_async_copy(w_buf, w_new, store_sem.at[2]),
    ]
    for copy in store:
        copy.start()

    def last_hop(bits):
        return max(n for n in range(3) if bits[n])

    for bits in GATHER_ORDER:
        hop = last_hop(bits)
        came = tuple(1 - bit if n == hop else bit for n, bit in enumerate(bits))
        for part in parts:
            ring_copy(came, hop, part).wait_recv()
            for later in range(hop + 1, 3):
                ring_copy(bits, later, part).start()
            share_copy(bits, part).start()
            keep_copy(bits, part).start()

    for part in parts:
        for k in range(4):
            half_copy(k, part).wait_send()
        for k in range(2):
            quarter_copy(k, part).wait_send()
        eighth_copy(part).wait_send()
        for bits in ((0, 0, 0),) + GATHER_ORDER:
            for later in range(0 if not any(bits) else last_hop(bits) + 1, 3):
                ring_copy(bits, later, part).wait_send()
            share_copy(bits, part).wait()
            keep_copy(bits, part).wait()
    for copy in store:
        copy.wait()


def exchange(*operands):
    shape = jax.ShapeDtypeStruct
    state_shape = shape((SHARD, LANES), jnp.float32)
    f32 = functools.partial(pltpu.VMEM, dtype=jnp.float32)
    dma = pltpu.SemaphoreType.DMA
    scratch = [
        f32((STAGES, SPAN * TILES, 8, LANES)), f32((9 * D // LANES, LANES)), f32((FF // LANES, LANES)),
        f32((8, SLOT, LANES)), f32((8, PAD, LANES)),
        f32((PARTS, 4, PART_MAX, LANES)), f32((PARTS, 2, PART_MAX, LANES)), f32((PARTS, PART_MAX, LANES)),
        f32((SHARD, LANES)), f32((SHARD, LANES)), f32((SHARD, LANES)),
        pltpu.VMEM((8, PAD, LANES), jnp.bfloat16),
        dma((STAGES, SPAN)), dma((2,)), dma((8, PARTS)), dma((8, PARTS)),
        dma((4, PARTS)), dma((4, PARTS)), dma((2, PARTS)), dma((2, PARTS)),
        dma((PARTS,)), dma((PARTS,)), dma((3,)), dma((3,)),
        dma((8, PARTS)), dma((8, PARTS)), dma((8, PARTS)), dma((8, PARTS)), dma((8, PARTS)),
    ]
    return pl.pallas_call(
        exchange_kernel,
        out_shape=(state_shape, state_shape, state_shape, shape((8, 2, PAD, LANES), jnp.bfloat16)),
        in_specs=[pl.BlockSpec(memory_space=pl.ANY)] * 9,
        out_specs=(pl.BlockSpec(memory_space=pl.ANY),) * 4,
        scratch_shapes=scratch,
        compiler_params=pltpu.CompilerParams(vmem_limit_bytes=VMEM_MAX, collective_id=0, has_side_effects=True),
        name="exchange",
    )(*operands)


SUB = 512
UNROLL = 2
CHUNK = UNROLL * SUB
RING = 6
ACT_SLOTS = 2 * UNROLL
GELU_A = math.sqrt(2.0 / math.pi)
GELU_B = GELU_A * 0.044715
WIDEN_ORDER = (8, 9, 10, 11, 12, 13, 14, 15, 0, 1, 2, 3, 4, 5, 6, 7)


def ffn_kernel(steps, ids, act, flat, m_in, v_in, master_in,
               y_out, o_emb, o_attn, o_in, o_out, o_vecd, o_vecf, m_out, v_out, master_out,
               dense, ring, act_buf, y_buf, w_in, w_out, b_in, b_out, vecd_wide, vecd_buf, vecf_buf,
               rows_one, rows_two, h_one, h_two, u_one, u_two, emb_buf, attn_buf, state_buf,
               ring_sem, act_sem, y_sem, emb_sem, attn_sem, weight_sem, state_sem):
    emb_rows, attn_rows = VOCAB // steps, 4 * D // steps

    blocks = steps * UNROLL

    def load_act(block):
        slot = lax.rem(block, ACT_SLOTS)
        return pltpu.make_async_copy(act.at[pl.ds(block * SUB, SUB)], act_buf.at[slot], act_sem.at[slot])

    def store_y(it):
        return pltpu.make_async_copy(
            y_buf.at[lax.rem(it, 2)], y_out.at[pl.ds(it * CHUNK - SUB, CHUNK)], y_sem.at[lax.rem(it, 2)])

    store_first = pltpu.make_async_copy(
        y_buf.at[0, pl.ds(SUB, CHUNK - SUB)], y_out.at[pl.ds(0, CHUNK - SUB)], y_sem.at[0])
    store_last = pltpu.make_async_copy(
        y_buf.at[steps % 2, pl.ds(0, SUB)], y_out.at[pl.ds(steps * CHUNK - SUB, SUB)], y_sem.at[steps % 2])

    def store_emb(it):
        return pltpu.make_async_copy(
            emb_buf.at[lax.rem(it, 2)], o_emb.at[pl.ds(it * emb_rows, emb_rows)], emb_sem.at[lax.rem(it, 2)])

    def store_attn(it):
        return pltpu.make_async_copy(
            attn_buf.at[lax.rem(it, 2)], o_attn.at[pl.ds(it * attn_rows, attn_rows)], attn_sem.at[lax.rem(it, 2)])

    def load_flat(n):
        return pltpu.make_async_copy(flat.at[WIDEN_ORDER[n]], ring.at[n % RING], ring_sem.at[n % RING])

    for n in range(RING):
        load_flat(n).start()
    for block in range(UNROLL + 1):
        load_act(block).start()

    def relayout(base, groups, row, buf, at):
        for j in range(groups):
            q = base + row * groups + j
            top = dense[pl.ds(q, 8, stride=groups), :]
            low = dense[pl.ds(q + 8 * groups, 8, stride=groups), :]
            buf[pl.ds(at, 16), j * LANES:(j + 1) * LANES] = jnp.concatenate([top, low], axis=0).astype(jnp.bfloat16)

    for n, owner in enumerate(WIDEN_ORDER):
        load_flat(n).wait()
        at = owner * SHARD
        whole = SHARD // 16

        def widen(t, carry, at=at, slot=n % RING):
            row = pl.multiple_of(t * 16, 16)
            dense[pl.ds(at + row, 16), :] = ring[slot, pl.ds(row, 16), :].astype(jnp.float32)
            return carry

        lax.fori_loop(0, whole, widen, 0, unroll=24)
        tail = ring[n % RING, whole * 16:whole * 16 + 16, :].astype(jnp.float32)
        dense[at + whole * 16:at + SHARD, :] = tail[:SHARD - whole * 16]
        if n + RING < DEVICES:
            load_flat(n + RING).start()
        if owner == 12:
            def fill_in(t, carry):
                row = pl.multiple_of(t * 16, 16)
                relayout(TENSORS[2][2], FF // LANES, row, w_in, row)
                return carry

            lax.fori_loop(0, D // 16, fill_in, 0, unroll=2)
            pltpu.make_async_copy(w_in, o_in, weight_sem.at[0]).start()
        if owner == 15:
            def fill_out(t, carry):
                row = pl.multiple_of(t * 16, 16)
                relayout(TENSORS[3][2], D // LANES, row, w_out, row)
                return carry

            lax.fori_loop(0, FF // 16, fill_out, 0, unroll=4)
            pltpu.make_async_copy(w_out, o_out, weight_sem.at[1]).start()
            for i in range(9):
                for j in range(D // LANES):
                    q = VEC_BASE + i * (D // LANES) + j
                    vecd_wide[i:i + 1, j * LANES:(j + 1) * LANES] = dense[q:q + 1, :]
            for j in range(D // LANES):
                q = VEC_BASE + 8 * (D // LANES) + j
                b_out[:, j * LANES:(j + 1) * LANES] = dense[q:q + 1, :]
            for j in range(FF // LANES):
                q = VEC_BASE + 9 * (D // LANES) + j
                b_in[:, j * LANES:(j + 1) * LANES] = dense[q:q + 1, :]
            vecd_buf[...] = vecd_wide[...].astype(jnp.bfloat16)
            vecf_buf[...] = b_in[...].astype(jnp.bfloat16)
            pltpu.make_async_copy(vecd_buf, o_vecd, weight_sem.at[2]).start()
            pltpu.make_async_copy(vecf_buf, o_vecf, weight_sem.at[3]).start()

    def lookup(block, h_buf, rows_buf):
        slot = lax.rem(block, ACT_SLOTS)
        token = jnp.minimum(block, blocks - 1) * SUB
        for tile in range(SUB // 8):
            for i in range(8):
                row = ids[token + tile * 8 + i] * (D // LANES)
                rows_buf[pl.ds(tile * 56 + i * 7, 8), :] = dense[pl.ds(row, 8), :]
        for pair in range(SUB // 16):
            for j in range(D // LANES):
                top = rows_buf[pl.ds(pair * 112 + j, 8, stride=7), :]
                low = rows_buf[pl.ds(pair * 112 + 56 + j, 8, stride=7), :]
                both = jnp.concatenate([top, low], axis=0) * math.sqrt(D)
                a_val = act_buf[slot, pair * 16:pair * 16 + 16, j * LANES:(j + 1) * LANES].astype(jnp.float32)
                h_buf[pair * 16:pair * 16 + 16, j * LANES:(j + 1) * LANES] = (both + a_val).astype(jnp.bfloat16)

    def widen_tokens(h_buf, u_buf):
        pre = jnp.dot(h_buf[...], w_in[...], preferred_element_type=jnp.float32) + b_in[...]
        bent = jnp.tanh(pre * (GELU_A + GELU_B * (pre * pre)))
        flat_half = 0.5 * pre
        u_buf[...] = (flat_half + flat_half * bent).astype(jnp.bfloat16)

    def narrow_tokens(it, part, u_buf):
        y_val = jnp.dot(u_buf[...], w_out[...], preferred_element_type=jnp.float32) + b_out[...]
        y_buf[lax.rem(it, 2), part * SUB:part * SUB + SUB, :] = y_val.astype(jnp.bfloat16)

    load_act(0).wait()
    lookup(0, h_one, rows_one)

    moves = []
    for n, (source, target) in enumerate(((m_in, m_out), (v_in, v_out), (master_in, master_out))):
        moves.append(pltpu.make_async_copy(source, state_buf, state_sem.at[2 * n]))
        moves.append(pltpu.make_async_copy(state_buf, target, state_sem.at[2 * n + 1]))

    def body(it, carry):
        for part in range(1, UNROLL):
            load_act(it * UNROLL + part).wait()

        @pl.when(it + 1 < steps)
        def _():
            load_act(it * UNROLL + UNROLL).wait()
            for part in range(UNROLL + 1, 2 * UNROLL):
                load_act(it * UNROLL + part).start()

        @pl.when(it + 2 < steps)
        def _():
            load_act(it * UNROLL + 2 * UNROLL).start()

        @pl.when(it == 2)
        def _():
            store_first.wait()

        @pl.when(it > 2)
        def _():
            store_y(it - 2).wait()

        @pl.when(it >= 2)
        def _():
            store_emb(it - 2).wait()
            store_attn(it - 2).wait()

        for n, move in enumerate(moves):
            @pl.when(it == 1 + n)
            def _(n=n, move=move):
                if n:
                    moves[n - 1].wait()
                move.start()

        buffers = ((h_one, rows_one, u_one), (h_two, rows_two, u_two))
        for part in range(UNROLL):
            h_now, _, u_now = buffers[part % 2]
            h_next, rows_next, u_before = buffers[(part + 1) % 2]
            lookup(it * UNROLL + part + 1, h_next, rows_next)
            widen_tokens(h_now, u_now)
            narrow_tokens(it, part, u_before)
        for t in range(emb_rows // 16):
            relayout(TENSORS[0][2], D // LANES, it * emb_rows + t * 16, emb_buf.at[lax.rem(it, 2)], t * 16)
        for t in range(attn_rows // 16):
            relayout(TENSORS[1][2], D // LANES, it * attn_rows + t * 16, attn_buf.at[lax.rem(it, 2)], t * 16)
        @pl.when(it == 0)
        def _():
            store_first.start()

        @pl.when(it > 0)
        def _():
            store_y(it).start()

        store_emb(it).start()
        store_attn(it).start()
        return carry

    lax.fori_loop(0, steps, body, 0)
    store_y(steps - 2).wait()
    narrow_tokens(steps, 0, u_two)
    store_last.start()
    store_y(steps - 1).wait()
    store_last.wait()
    for it in (steps - 2, steps - 1):
        store_emb(it).wait()
        store_attn(it).wait()
    moves[-1].wait()
    pltpu.make_async_copy(w_in, o_in, weight_sem.at[0]).wait()
    pltpu.make_async_copy(w_out, o_out, weight_sem.at[1]).wait()
    pltpu.make_async_copy(vecd_buf, o_vecd, weight_sem.at[2]).wait()
    pltpu.make_async_copy(vecf_buf, o_vecf, weight_sem.at[3]).wait()


def ffn(ids, act, flat, m_new, v_new, w_new):
    tokens = act.shape[0]
    steps = tokens // CHUNK
    f32, bf16 = jnp.float32, jnp.bfloat16
    shape = jax.ShapeDtypeStruct
    dma = pltpu.SemaphoreType.DMA
    anywhere = pl.BlockSpec(memory_space=pl.ANY)
    state = shape((SHARD, LANES), f32)
    return pl.pallas_call(
        functools.partial(ffn_kernel, steps),
        out_shape=(shape((tokens, D), bf16), shape((VOCAB, D), bf16), shape((4 * D, D), bf16), shape((D, FF), bf16),
                   shape((FF, D), bf16), shape((9, D), bf16), shape((1, FF), bf16), state, state, state),
        in_specs=[pl.BlockSpec(memory_space=pltpu.SMEM)] + [anywhere] * 5,
        out_specs=(anywhere,) * 10,
        scratch_shapes=[
            pltpu.VMEM((DEVICES * SHARD, LANES), f32),
            pltpu.VMEM((RING, PAD, LANES), bf16),
            pltpu.VMEM((ACT_SLOTS, SUB, D), bf16),
            pltpu.VMEM((2, CHUNK, D), bf16),
            pltpu.VMEM((D, FF), bf16),
            pltpu.VMEM((FF, D), bf16),
            pltpu.VMEM((1, FF), f32),
            pltpu.VMEM((1, D), f32),
            pltpu.VMEM((9, D), f32),
            pltpu.VMEM((9, D), bf16),
            pltpu.VMEM((1, FF), bf16),
            pltpu.VMEM((SUB * 7 + 8, LANES), f32),
            pltpu.VMEM((SUB * 7 + 8, LANES), f32),
            pltpu.VMEM((SUB, D), bf16),
            pltpu.VMEM((SUB, D), bf16),
            pltpu.VMEM((SUB, FF), bf16),
            pltpu.VMEM((SUB, FF), bf16),
            pltpu.VMEM((2, VOCAB // steps, D), bf16),
            pltpu.VMEM((2, 4 * D // steps, D), bf16),
            pltpu.VMEM((SHARD, LANES), f32),
            dma((RING,)), dma((ACT_SLOTS,)), dma((2,)), dma((2,)), dma((2,)), dma((4,)), dma((6,)),
        ],
        compiler_params=pltpu.CompilerParams(vmem_limit_bytes=VMEM_MAX),
        name="ffn",
    )(ids, act, flat, m_new, v_new, w_new)


def solution(mesh):
    def device_step(g_emb, g_attn, g_in, g_out, g_vecd, g_vecf, opt_m, opt_v, master, tok_ids, act_in):
        def tiles(grad, cols):
            split = grad.reshape(-1, 8, cols // LANES, LANES)
            return split.transpose(0, 2, 1, 3).reshape(-1, 8, LANES)

        m_new, v_new, w_new, gathered = exchange(
            tiles(g_emb, D), tiles(g_attn, D), tiles(g_in, FF), tiles(g_out, D),
            g_vecd.reshape(-1, LANES), g_vecf.reshape(-1, LANES), opt_m.reshape(SHARD, LANES),
            opt_v.reshape(SHARD, LANES), master.reshape(SHARD, LANES))
        flat = gathered.reshape(DEVICES, PAD, LANES)
        y_out, wb_emb, wb_attn, wb_in, wb_out, wb_vecd, wb_vecf, m_new, v_new, w_new = ffn(
            tok_ids, act_in, flat, m_new, v_new, w_new)
        return (m_new.reshape(-1), v_new.reshape(-1), w_new.reshape(-1), wb_emb, wb_attn.reshape(1, 4, D, D),
                wb_in[None], wb_out[None], wb_vecd[None], wb_vecf, y_out)

    grad_specs = tuple(P(AXES, *([None] * (grad_rank - 1))) for grad_rank in GRAD_RANKS)
    in_specs = grad_specs + (P(AXES), P(AXES), P(AXES), P(AXES), P(AXES, None))
    out_specs = (P(AXES), P(AXES), P(AXES), P(), P(), P(), P(), P(), P(), P(AXES, None))
    return jax.shard_map(device_step, mesh=mesh, in_specs=in_specs, out_specs=out_specs, check_vma=False)
```

```python
import functools
import math

import jax
import jax.numpy as jnp
from jax import lax
from jax.experimental import pallas as pl
from jax.experimental.pallas import tpu as pltpu
from jax.sharding import PartitionSpec as P

LEARN_RATE = 0.002
BETA_ONE = 0.9
BETA_TWO = 0.95
ADAM_EPS = 1e-8
ADAM_STEP = 2
AXES = ("dz", "dy", "dx")
GRAD_RANKS = (3, 5, 4, 4, 4, 3)
MESH = pl.DeviceIdType.MESH

D = 768
FF = 2048
VOCAB = 2048
DEVICES = 16
LANES = 128
SHARD = 3461
PAD = 3472
PART_START = (0, 576, 1152, 1728, 2304, 2880)
PART_ROWS = (576, 576, 576, 576, 576, 592)
PART_MAX = 592
PARTS = 6
VMEM_MAX = 67_000_000

TENSORS = (
    (VOCAB, D, 0),
    (4 * D, D, VOCAB * D // LANES),
    (D, FF, (VOCAB * D + 4 * D * D) // LANES),
    (FF, D, (VOCAB * D + 4 * D * D + D * FF) // LANES),
)
TILES = 48
FLAT_ROWS = 8 * TILES
CHUNKS = 144
SPAN = 11
MARGIN = FLAT_ROWS
SLOT = 2 * MARGIN + 3464
STAGES = 4
VEC_BASE = (VOCAB * D + 4 * D * D + 2 * D * FF) // LANES
VEC_ROWS = DEVICES * SHARD - VEC_BASE


ORDERS = (("x", "y", "z"), ("y", "z", "x"), ("z", "x", "y")) * 2
WEIGHT = {"z": 4, "y": 2, "x": 1}
CHIP_ORDER = ("xyz", "xy", "yz", "zx", "x", "y", "z", "")
HALF_ORDER = ((1, 1), (1, 0), (0, 1), (0, 0))
GATHER_ORDER = ((1, 0, 0), (0, 1, 0), (0, 0, 1), (1, 1, 0), (1, 0, 1), (0, 1, 1), (1, 1, 1))


def exchange_kernel(g_emb, g_attn, g_in, g_out, g_vecd, g_vecf, opt_m, opt_v, master, m_new, v_new, w_new, gathered,
                    stage, vecd_raw, vecd_buf, vecf_buf, acc, pair, half, quarter, eighth, m_buf, v_buf, w_buf, wb,
                    stage_sem, vec_sem, pair_send, pair_recv, half_send, half_recv, quarter_send, quarter_recv,
                    eighth_send, eighth_recv, state_sem, store_sem,
                    ring_send, ring_recv, share_send, share_recv, keep_sem):
    z, y, dx = lax.axis_index("dz"), lax.axis_index("dy"), lax.axis_index("dx")
    x, c = dx // 2, dx % 2
    mine = {"z": z, "y": y, "x": x}
    peers = {
        "c": {"dz": z, "dy": y, "dx": 2 * x + (1 - c)},
        "x": {"dz": z, "dy": y, "dx": 2 * (1 - x) + c},
        "y": {"dz": z, "dy": 1 - y, "dx": dx},
        "z": {"dz": 1 - z, "dy": y, "dx": dx},
    }

    def chip(part, bits):
        index = 0
        for axis, bit in zip(ORDERS[part], bits):
            index = index + WEIGHT[axis] * ((1 - mine[axis]) if bit else mine[axis])
        return index

    def rows(part):
        return pl.ds(PART_START[part], PART_ROWS[part])

    def acc_rows(part):
        return pl.ds(MARGIN + PART_START[part], PART_ROWS[part])

    vec_loads = [
        pltpu.make_async_copy(g_vecd, vecd_raw, vec_sem.at[0]), pltpu.make_async_copy(g_vecf, vecf_buf, vec_sem.at[1])]
    state = [
        pltpu.make_async_copy(opt_m, m_buf, state_sem.at[0]),
        pltpu.make_async_copy(opt_v, v_buf, state_sem.at[1]),
        pltpu.make_async_copy(master, w_buf, state_sem.at[2]),
    ]

    parts = range(PARTS)

    def chip_at(n):
        index = 0
        for axis in "zyx":
            index = index + WEIGHT[axis] * ((1 - mine[axis]) if axis in CHIP_ORDER[n] else mine[axis])
        return index

    sequence = [(False, 0)]
    for n in range(1, 8):
        sequence += [(False, n), (True, n - 1)]
    sequence.append((True, 7))

    def shard_at(place):
        own, n = sequence[place]
        return 2 * chip_at(n) + (c if own else 1 - c)

    def chunk_bounds(owner):
        low = (owner * SHARD) // FLAT_ROWS
        high = (owner * SHARD + SHARD + FLAT_ROWS - 1 - (owner // (DEVICES - 1)) * VEC_ROWS) // FLAT_ROWS
        return low, high

    def by_tensor(k, act):
        @pl.when(k < 32)
        def _():
            act(0, 0)

        @pl.when(k >= 32)
        def _():
            @pl.when(k < 80)
            def _():
                act(1, 32)

            @pl.when(k >= 80)
            def _():
                @pl.when(k < 112)
                def _():
                    act(2, 80)

                @pl.when(k >= 112)
                def _():
                    act(3, 112)

    grads = (g_emb, g_attn, g_in, g_out)

    def load_shard(place):
        low, high = chunk_bounds(shard_at(place))
        slot = place % STAGES

        def one(k, carry):
            where = k - low

            def start(tensor, first):
                pltpu.make_async_copy(
                    grads[tensor].at[pl.ds((k - first) * TILES, TILES)], stage.at[slot, pl.ds(where * TILES, TILES)],
                    stage_sem.at[slot, where]).start()

            by_tensor(k, start)
            return carry

        lax.fori_loop(low, high, one, 0)

    def flatten_shard(place):
        owner = shard_at(place)
        low, high = chunk_bounds(owner)
        slot = place % STAGES
        where = chip_at(sequence[place][1])

        def one(k, carry):
            at = k - low
            pltpu.make_async_copy(
                g_emb.at[pl.ds(0, TILES)], stage.at[slot, pl.ds(at * TILES, TILES)], stage_sem.at[slot, at]).wait()
            base = MARGIN + k * FLAT_ROWS - owner * SHARD

            def spread(tensor, first):
                groups = TENSORS[tensor][1] // LANES
                bands = TILES // groups
                for j in range(groups):
                    tile = stage[slot, pl.ds(at * TILES + j, bands, stride=groups)]
                    acc[where, pl.ds(base + j, 8 * bands, stride=groups), :] = tile.reshape(8 * bands, LANES)

            by_tensor(k, spread)
            return carry

        lax.fori_loop(low, high, one, 0)

        @pl.when(owner == DEVICES - 1)
        def _():
            first = MARGIN + SHARD - VEC_ROWS
            second = first + 9 * D // LANES
            third = second + FF // LANES
            acc[where, first:second, :] = vecd_buf[...]
            acc[where, second:third, :] = vecf_buf[...]
            acc[where, third:MARGIN + SHARD, :] = jnp.zeros((MARGIN + SHARD - third, LANES), jnp.float32)

    def pair_copy(n, part):
        where = chip_at(n)
        return pltpu.make_async_remote_copy(
            src_ref=acc.at[where, acc_rows(part)], dst_ref=pair.at[where, rows(part)],
            send_sem=pair_send.at[n, part], recv_sem=pair_recv.at[n, part],
            device_id=peers["c"], device_id_type=MESH)

    def half_copy(k, part):
        return pltpu.make_async_remote_copy(
            src_ref=acc.at[chip(part, (1,) + HALF_ORDER[k]), acc_rows(part)],
            dst_ref=half.at[part, k, pl.ds(0, PART_ROWS[part])],
            send_sem=half_send.at[k, part], recv_sem=half_recv.at[k, part],
            device_id=peers[ORDERS[part][0]], device_id_type=MESH)

    def quarter_copy(k, part):
        return pltpu.make_async_remote_copy(
            src_ref=acc.at[chip(part, (0, 1, 1 - k)), acc_rows(part)],
            dst_ref=quarter.at[part, k, pl.ds(0, PART_ROWS[part])],
            send_sem=quarter_send.at[k, part], recv_sem=quarter_recv.at[k, part],
            device_id=peers[ORDERS[part][1]], device_id_type=MESH)

    def eighth_copy(part):
        return pltpu.make_async_remote_copy(
            src_ref=acc.at[chip(part, (0, 0, 1)), acc_rows(part)],
            dst_ref=eighth.at[part, pl.ds(0, PART_ROWS[part])],
            send_sem=eighth_send.at[part], recv_sem=eighth_recv.at[part],
            device_id=peers[ORDERS[part][2]], device_id_type=MESH)

    for place in range(STAGES):
        load_shard(place)
    for copy in vec_loads:
        copy.start()
    barrier = pltpu.get_barrier_semaphore()
    for peer in peers.values():
        pl.semaphore_signal(barrier, inc=1, device_id=peer, device_id_type=MESH)
    pl.semaphore_wait(barrier, 4)
    for copy in vec_loads:
        copy.wait()
    for i in range(9):
        for j in range(D // LANES):
            row = i * (D // LANES) + j
            vecd_buf[row:row + 1, :] = vecd_raw[i, :, j * LANES:(j + 1) * LANES]

    for place, (own, n) in enumerate(sequence):
        if own:
            for part in parts:
                pair_copy(n, part).wait_send()
        flatten_shard(place)
        if place + STAGES < len(sequence):
            load_shard(place + STAGES)
        where = chip_at(n)
        for part in parts:
            if not own:
                pair_copy(n, part).start()
                continue
            pair_copy(n, part).wait_recv()
            acc[where, acc_rows(part)] += pair[where, rows(part)]
            bits = tuple(int(axis in CHIP_ORDER[n]) for axis in ORDERS[part])
            if bits[0]:
                half_copy(HALF_ORDER.index(bits[1:]), part).start()
    for copy in state:
        copy.start()
    for k in range(4):
        for part in parts:
            half_copy(k, part).wait_recv()
            where = chip(part, (0,) + HALF_ORDER[k])
            acc[where, acc_rows(part)] += half[part, k, pl.ds(0, PART_ROWS[part])]
            if k < 2:
                quarter_copy(k, part).start()
    for k in range(2):
        for part in parts:
            quarter_copy(k, part).wait_recv()
            where = chip(part, (0, 0, 1 - k))
            acc[where, acc_rows(part)] += quarter[part, k, pl.ds(0, PART_ROWS[part])]
            if k == 0:
                eighth_copy(part).start()

    for copy in state:
        copy.wait()

    here = 4 * z + 2 * y + x

    def ring_copy(bits, hop, part):
        flipped = tuple(1 - bit if n == hop else bit for n, bit in enumerate(bits))
        slot = flipped[0] * 4 + flipped[1] * 2 + flipped[2]
        where = chip(part, bits)
        return pltpu.make_async_remote_copy(
            src_ref=wb.at[where, rows(part)], dst_ref=wb.at[where, rows(part)],
            send_sem=ring_send.at[slot, part], recv_sem=ring_recv.at[slot, part],
            device_id=peers[ORDERS[part][hop]], device_id_type=MESH)

    def share_copy(bits, part):
        slot = bits[0] * 4 + bits[1] * 2 + bits[2]
        where = chip(part, bits)
        return pltpu.make_async_remote_copy(
            src_ref=wb.at[where, rows(part)], dst_ref=gathered.at[where, c, rows(part)],
            send_sem=share_send.at[slot, part], recv_sem=share_recv.at[slot, part],
            device_id=peers["c"], device_id_type=MESH)

    def keep_copy(bits, part):
        slot = bits[0] * 4 + bits[1] * 2 + bits[2]
        where = chip(part, bits)
        return pltpu.make_async_copy(
            wb.at[where, rows(part)], gathered.at[where, c, rows(part)], keep_sem.at[slot, part])

    for part in parts:
        eighth_copy(part).wait_recv()
        start, count = PART_START[part], min(PART_ROWS[part], SHARD - PART_START[part])
        pieces = [(start, count)] if count % 16 == 0 else [(start, count // 16 * 16), (start + count // 16 * 16, count % 16)]
        for first, size in pieces:
            span = pl.ds(first, size)
            grad_sum = (acc[here, pl.ds(MARGIN + first, size)] + eighth[part, pl.ds(first - start, size)]) / DEVICES
            m_val = BETA_ONE * m_buf[span] + (1.0 - BETA_ONE) * grad_sum
            v_val = BETA_TWO * v_buf[span] + (1.0 - BETA_TWO) * grad_sum * grad_sum
            m_hat = m_val / (1.0 - BETA_ONE ** ADAM_STEP)
            v_hat = v_val / (1.0 - BETA_TWO ** ADAM_STEP)
            w_val = w_buf[span] - LEARN_RATE * m_hat / (jnp.sqrt(v_hat) + ADAM_EPS)
            m_buf[span] = m_val
            v_buf[span] = v_val
            w_buf[span] = w_val
            if size % 16:
                w_val = jnp.concatenate([w_val, jnp.zeros((16 - size % 16, LANES), jnp.float32)], axis=0)
                span = pl.ds(first, 16)
            wb[here, span] = w_val.astype(jnp.bfloat16)
        for hop in range(3):
            ring_copy((0, 0, 0), hop, part).start()
        share_copy((0, 0, 0), part).start()
        keep_copy((0, 0, 0), part).start()

    store = [
        pltpu.make_async_copy(m_buf, m_new, store_sem.at[0]),
        pltpu.make_async_copy(v_buf, v_new, store_sem.at[1]),
        pltpu.make_async_copy(w_buf, w_new, store_sem.at[2]),
    ]
    for copy in store:
        copy.start()

    def last_hop(bits):
        return max(n for n in range(3) if bits[n])

    for bits in GATHER_ORDER:
        hop = last_hop(bits)
        came = tuple(1 - bit if n == hop else bit for n, bit in enumerate(bits))
        for part in parts:
            ring_copy(came, hop, part).wait_recv()
            for later in range(hop + 1, 3):
                ring_copy(bits, later, part).start()
            share_copy(bits, part).start()
            keep_copy(bits, part).start()

    for part in parts:
        for k in range(4):
            half_copy(k, part).wait_send()
        for k in range(2):
            quarter_copy(k, part).wait_send()
        eighth_copy(part).wait_send()
        for bits in ((0, 0, 0),) + GATHER_ORDER:
            for later in range(0 if not any(bits) else last_hop(bits) + 1, 3):
                ring_copy(bits, later, part).wait_send()
            share_copy(bits, part).wait()
            keep_copy(bits, part).wait()
    for copy in store:
        copy.wait()


def exchange(*operands):
    shape = jax.ShapeDtypeStruct
    state_shape = shape((SHARD, LANES), jnp.float32)
    f32 = functools.partial(pltpu.VMEM, dtype=jnp.float32)
    dma = pltpu.SemaphoreType.DMA
    scratch = [
        f32((STAGES, SPAN * TILES, 8, LANES)), f32((9, 1, D)), f32((9 * D // LANES, LANES)),
        f32((FF // LANES, LANES)),
        f32((8, SLOT, LANES)), f32((8, PAD, LANES)),
        f32((PARTS, 4, PART_MAX, LANES)), f32((PARTS, 2, PART_MAX, LANES)), f32((PARTS, PART_MAX, LANES)),
        f32((SHARD, LANES)), f32((SHARD, LANES)), f32((SHARD, LANES)),
        pltpu.VMEM((8, PAD, LANES), jnp.bfloat16),
        dma((STAGES, SPAN)), dma((2,)), dma((8, PARTS)), dma((8, PARTS)),
        dma((4, PARTS)), dma((4, PARTS)), dma((2, PARTS)), dma((2, PARTS)),
        dma((PARTS,)), dma((PARTS,)), dma((3,)), dma((3,)),
        dma((8, PARTS)), dma((8, PARTS)), dma((8, PARTS)), dma((8, PARTS)), dma((8, PARTS)),
    ]
    return pl.pallas_call(
        exchange_kernel,
        out_shape=(state_shape, state_shape, state_shape, shape((8, 2, PAD, LANES), jnp.bfloat16)),
        in_specs=[pl.BlockSpec(memory_space=pl.ANY)] * 9,
        out_specs=(pl.BlockSpec(memory_space=pl.ANY),) * 4,
        scratch_shapes=scratch,
        compiler_params=pltpu.CompilerParams(vmem_limit_bytes=VMEM_MAX, collective_id=0, has_side_effects=True),
        name="exchange",
    )(*operands)


SUB = 512
UNROLL = 2
CHUNK = UNROLL * SUB
RING = 6
ACT_SLOTS = 2 * UNROLL
GELU_A = math.sqrt(2.0 / math.pi)
GELU_B = GELU_A * 0.044715
WIDEN_ORDER = (8, 9, 10, 11, 12, 13, 14, 15, 0, 1, 2, 3, 4, 5, 6, 7)


def ffn_kernel(steps, ids_in, act, flat, m_in, v_in, master_in,
               y_out, o_emb, o_attn, o_in, o_out, o_vecd, o_vecf, m_out, v_out, master_out,
               ids, dense, ring, act_buf, y_buf, w_in, w_out, b_in, b_out, vecd_wide, vecd_buf, vecf_buf,
               rows_one, rows_two, h_one, h_two, u_one, u_two, emb_buf, attn_buf, state_buf,
               ring_sem, act_sem, y_sem, emb_sem, attn_sem, weight_sem, state_sem, ids_sem):
    emb_rows, attn_rows = VOCAB // steps, 4 * D // steps

    blocks = steps * UNROLL

    def load_act(block):
        slot = lax.rem(block, ACT_SLOTS)
        return pltpu.make_async_copy(act.at[pl.ds(block * SUB, SUB)], act_buf.at[slot], act_sem.at[slot])

    def store_y(it):
        return pltpu.make_async_copy(
            y_buf.at[lax.rem(it, 2)], y_out.at[pl.ds(it * CHUNK - SUB, CHUNK)], y_sem.at[lax.rem(it, 2)])

    store_first = pltpu.make_async_copy(
        y_buf.at[0, pl.ds(SUB, CHUNK - SUB)], y_out.at[pl.ds(0, CHUNK - SUB)], y_sem.at[0])
    store_last = pltpu.make_async_copy(
        y_buf.at[steps % 2, pl.ds(0, SUB)], y_out.at[pl.ds(steps * CHUNK - SUB, SUB)], y_sem.at[steps % 2])

    def store_emb(it):
        return pltpu.make_async_copy(
            emb_buf.at[lax.rem(it, 2)], o_emb.at[pl.ds(it * emb_rows, emb_rows)], emb_sem.at[lax.rem(it, 2)])

    def store_attn(it):
        return pltpu.make_async_copy(
            attn_buf.at[lax.rem(it, 2)], o_attn.at[pl.ds(it * attn_rows, attn_rows)], attn_sem.at[lax.rem(it, 2)])

    def load_flat(n):
        return pltpu.make_async_copy(flat.at[WIDEN_ORDER[n]], ring.at[n % RING], ring_sem.at[n % RING])

    for n in range(RING):
        load_flat(n).start()
    load_ids = pltpu.make_async_copy(ids_in, ids, ids_sem)
    load_ids.start()
    for block in range(UNROLL + 1):
        load_act(block).start()

    def relayout(base, groups, row, buf, at):
        for j in range(groups):
            q = base + row * groups + j
            top = dense[pl.ds(q, 8, stride=groups), :]
            low = dense[pl.ds(q + 8 * groups, 8, stride=groups), :]
            buf[pl.ds(at, 16), j * LANES:(j + 1) * LANES] = jnp.concatenate([top, low], axis=0).astype(jnp.bfloat16)

    for n, owner in enumerate(WIDEN_ORDER):
        load_flat(n).wait()
        at = owner * SHARD
        whole = SHARD // 16

        def widen(t, carry, at=at, slot=n % RING):
            row = pl.multiple_of(t * 16, 16)
            dense[pl.ds(at + row, 16), :] = ring[slot, pl.ds(row, 16), :].astype(jnp.float32)
            return carry

        lax.fori_loop(0, whole, widen, 0, unroll=24)
        tail = ring[n % RING, whole * 16:whole * 16 + 16, :].astype(jnp.float32)
        dense[at + whole * 16:at + SHARD, :] = tail[:SHARD - whole * 16]
        if n + RING < DEVICES:
            load_flat(n + RING).start()
        if owner == 12:
            def fill_in(t, carry):
                row = pl.multiple_of(t * 16, 16)
                relayout(TENSORS[2][2], FF // LANES, row, w_in, row)
                return carry

            lax.fori_loop(0, D // 16, fill_in, 0, unroll=4)
            pltpu.make_async_copy(w_in, o_in, weight_sem.at[0]).start()
        if owner == 15:
            def fill_out(t, carry):
                row = pl.multiple_of(t * 16, 16)
                relayout(TENSORS[3][2], D // LANES, row, w_out, row)
                return carry

            lax.fori_loop(0, FF // 16, fill_out, 0, unroll=8)
            pltpu.make_async_copy(w_out, o_out, weight_sem.at[1]).start()
            for i in range(9):
                for j in range(D // LANES):
                    q = VEC_BASE + i * (D // LANES) + j
                    vecd_wide[i:i + 1, j * LANES:(j + 1) * LANES] = dense[q:q + 1, :]
            for j in range(D // LANES):
                q = VEC_BASE + 8 * (D // LANES) + j
                b_out[:, j * LANES:(j + 1) * LANES] = dense[q:q + 1, :]
            for j in range(FF // LANES):
                q = VEC_BASE + 9 * (D // LANES) + j
                b_in[:, j * LANES:(j + 1) * LANES] = dense[q:q + 1, :]
            vecd_buf[...] = vecd_wide[...].astype(jnp.bfloat16)
            vecf_buf[...] = b_in[...].astype(jnp.bfloat16)
            pltpu.make_async_copy(vecd_buf, o_vecd, weight_sem.at[2]).start()
            pltpu.make_async_copy(vecf_buf, o_vecf, weight_sem.at[3]).start()

    def lookup(block, h_buf, rows_buf):
        slot = lax.rem(block, ACT_SLOTS)
        token = jnp.minimum(block, blocks - 1) * SUB
        for tile in range(SUB // 8):
            for i in range(8):
                row = ids[token + tile * 8 + i] * (D // LANES)
                rows_buf[pl.ds(tile * 56 + i * 7, 8), :] = dense[pl.ds(row, 8), :]
        for pair in range(SUB // 16):
            for j in range(D // LANES):
                top = rows_buf[pl.ds(pair * 112 + j, 8, stride=7), :]
                low = rows_buf[pl.ds(pair * 112 + 56 + j, 8, stride=7), :]
                both = jnp.concatenate([top, low], axis=0) * math.sqrt(D)
                a_val = act_buf[slot, pair * 16:pair * 16 + 16, j * LANES:(j + 1) * LANES].astype(jnp.float32)
                h_buf[pair * 16:pair * 16 + 16, j * LANES:(j + 1) * LANES] = (both + a_val).astype(jnp.bfloat16)

    def widen_tokens(h_buf, u_buf):
        pre = jnp.dot(h_buf[...], w_in[...], preferred_element_type=jnp.float32) + b_in[...]
        bent = jnp.tanh(pre * (GELU_A + GELU_B * (pre * pre)))
        flat_half = 0.5 * pre
        u_buf[...] = (flat_half + flat_half * bent).astype(jnp.bfloat16)

    def narrow_tokens(it, part, u_buf):
        y_val = jnp.dot(u_buf[...], w_out[...], preferred_element_type=jnp.float32) + b_out[...]
        y_buf[lax.rem(it, 2), part * SUB:part * SUB + SUB, :] = y_val.astype(jnp.bfloat16)

    load_ids.wait()
    load_act(0).wait()
    lookup(0, h_one, rows_one)

    moves = []
    for n, (source, target) in enumerate(((m_in, m_out), (v_in, v_out), (master_in, master_out))):
        moves.append(pltpu.make_async_copy(source, state_buf, state_sem.at[2 * n]))
        moves.append(pltpu.make_async_copy(state_buf, target, state_sem.at[2 * n + 1]))

    def body(it, carry):
        for part in range(1, UNROLL):
            load_act(it * UNROLL + part).wait()

        @pl.when(it + 1 < steps)
        def _():
            load_act(it * UNROLL + UNROLL).wait()
            for part in range(UNROLL + 1, 2 * UNROLL):
                load_act(it * UNROLL + part).start()

        @pl.when(it + 2 < steps)
        def _():
            load_act(it * UNROLL + 2 * UNROLL).start()

        @pl.when(it == 2)
        def _():
            store_first.wait()

        @pl.when(it > 2)
        def _():
            store_y(it - 2).wait()

        @pl.when(it >= 2)
        def _():
            store_emb(it - 2).wait()
            store_attn(it - 2).wait()

        for n, move in enumerate(moves):
            @pl.when(it == 1 + n)
            def _(n=n, move=move):
                if n:
                    moves[n - 1].wait()
                move.start()

        buffers = ((h_one, rows_one, u_one), (h_two, rows_two, u_two))
        for part in range(UNROLL):
            h_now, _, u_now = buffers[part % 2]
            h_next, rows_next, u_before = buffers[(part + 1) % 2]
            lookup(it * UNROLL + part + 1, h_next, rows_next)
            widen_tokens(h_now, u_now)
            narrow_tokens(it, part, u_before)
        for t in range(emb_rows // 16):
            relayout(TENSORS[0][2], D // LANES, it * emb_rows + t * 16, emb_buf.at[lax.rem(it, 2)], t * 16)
        for t in range(attn_rows // 16):
            relayout(TENSORS[1][2], D // LANES, it * attn_rows + t * 16, attn_buf.at[lax.rem(it, 2)], t * 16)
        @pl.when(it == 0)
        def _():
            store_first.start()

        @pl.when(it > 0)
        def _():
            store_y(it).start()

        store_emb(it).start()
        store_attn(it).start()
        return carry

    lax.fori_loop(0, steps, body, 0)
    store_y(steps - 2).wait()
    narrow_tokens(steps, 0, u_two)
    store_last.start()
    store_y(steps - 1).wait()
    store_last.wait()
    for it in (steps - 2, steps - 1):
        store_emb(it).wait()
        store_attn(it).wait()
    moves[-1].wait()
    pltpu.make_async_copy(w_in, o_in, weight_sem.at[0]).wait()
    pltpu.make_async_copy(w_out, o_out, weight_sem.at[1]).wait()
    pltpu.make_async_copy(vecd_buf, o_vecd, weight_sem.at[2]).wait()
    pltpu.make_async_copy(vecf_buf, o_vecf, weight_sem.at[3]).wait()


def ffn(ids, act, flat, m_new, v_new, w_new):
    tokens = act.shape[0]
    steps = tokens // CHUNK
    f32, bf16 = jnp.float32, jnp.bfloat16
    shape = jax.ShapeDtypeStruct
    dma = pltpu.SemaphoreType.DMA
    anywhere = pl.BlockSpec(memory_space=pl.ANY)
    state = shape((SHARD, LANES), f32)
    return pl.pallas_call(
        functools.partial(ffn_kernel, steps),
        out_shape=(shape((tokens, D), bf16), shape((VOCAB, D), bf16), shape((4 * D, D), bf16), shape((D, FF), bf16),
                   shape((FF, D), bf16), shape((9, D), bf16), shape((1, FF), bf16), state, state, state),
        in_specs=[anywhere] * 6,
        out_specs=(anywhere,) * 10,
        scratch_shapes=[
            pltpu.SMEM((tokens,), jnp.int32),
            pltpu.VMEM((DEVICES * SHARD, LANES), f32),
            pltpu.VMEM((RING, PAD, LANES), bf16),
            pltpu.VMEM((ACT_SLOTS, SUB, D), bf16),
            pltpu.VMEM((2, CHUNK, D), bf16),
            pltpu.VMEM((D, FF), bf16),
            pltpu.VMEM((FF, D), bf16),
            pltpu.VMEM((1, FF), f32),
            pltpu.VMEM((1, D), f32),
            pltpu.VMEM((9, D), f32),
            pltpu.VMEM((9, D), bf16),
            pltpu.VMEM((1, FF), bf16),
            pltpu.VMEM((SUB * 7 + 8, LANES), f32),
            pltpu.VMEM((SUB * 7 + 8, LANES), f32),
            pltpu.VMEM((SUB, D), bf16),
            pltpu.VMEM((SUB, D), bf16),
            pltpu.VMEM((SUB, FF), bf16),
            pltpu.VMEM((SUB, FF), bf16),
            pltpu.VMEM((2, VOCAB // steps, D), bf16),
            pltpu.VMEM((2, 4 * D // steps, D), bf16),
            pltpu.VMEM((SHARD, LANES), f32),
            dma((RING,)), dma((ACT_SLOTS,)), dma((2,)), dma((2,)), dma((2,)), dma((4,)), dma((6,)), dma,
        ],
        compiler_params=pltpu.CompilerParams(vmem_limit_bytes=VMEM_MAX),
        name="ffn",
    )(ids, act, flat, m_new, v_new, w_new)


def solution(mesh):
    def device_step(g_emb, g_attn, g_in, g_out, g_vecd, g_vecf, opt_m, opt_v, master, tok_ids, act_in):
        def tiles(grad, cols):
            split = grad.reshape(-1, 8, cols // LANES, LANES)
            return split.transpose(0, 2, 1, 3).reshape(-1, 8, LANES)

        m_new, v_new, w_new, gathered = exchange(
            tiles(g_emb, D), tiles(g_attn, D), tiles(g_in, FF), tiles(g_out, D),
            g_vecd.reshape(9, 1, D), g_vecf.reshape(-1, LANES), opt_m.reshape(SHARD, LANES),
            opt_v.reshape(SHARD, LANES), master.reshape(SHARD, LANES))
        flat = gathered.reshape(DEVICES, PAD, LANES)
        y_out, wb_emb, wb_attn, wb_in, wb_out, wb_vecd, wb_vecf, m_new, v_new, w_new = ffn(
            tok_ids, act_in, flat, m_new, v_new, w_new)
        return (m_new.reshape(-1), v_new.reshape(-1), w_new.reshape(-1), wb_emb, wb_attn.reshape(1, 4, D, D),
                wb_in[None], wb_out[None], wb_vecd[None], wb_vecf, y_out)

    grad_specs = tuple(P(AXES, *([None] * (grad_rank - 1))) for grad_rank in GRAD_RANKS)
    in_specs = grad_specs + (P(AXES), P(AXES), P(AXES), P(AXES), P(AXES, None))
    out_specs = (P(AXES), P(AXES), P(AXES), P(), P(), P(), P(), P(), P(), P(AXES, None))
    return jax.shard_map(device_step, mesh=mesh, in_specs=in_specs, out_specs=out_specs, check_vma=False)
```

```python
import functools
import math

import jax
import jax.numpy as jnp
from jax import lax
from jax.experimental import pallas as pl
from jax.experimental.pallas import tpu as pltpu
from jax.sharding import PartitionSpec as P

LEARN_RATE = 0.002
BETA_ONE = 0.9
BETA_TWO = 0.95
ADAM_EPS = 1e-8
ADAM_STEP = 2
AXES = ("dz", "dy", "dx")
GRAD_RANKS = (3, 5, 4, 4, 4, 3)
MESH = pl.DeviceIdType.MESH

D = 768
FF = 2048
VOCAB = 2048
DEVICES = 16
LANES = 128
SHARD = 3461
PAD = 3472
PART_START = (0, 576, 1152, 1728, 2304, 2880)
PART_ROWS = (576, 576, 576, 576, 576, 592)
PART_MAX = 592
PARTS = 6
VMEM_MAX = 67_000_000

TENSORS = (
    (VOCAB, D, 0),
    (4 * D, D, VOCAB * D // LANES),
    (D, FF, (VOCAB * D + 4 * D * D) // LANES),
    (FF, D, (VOCAB * D + 4 * D * D + D * FF) // LANES),
)
TILES = 48
FLAT_ROWS = 8 * TILES
CHUNKS = 144
SPAN = 11
MARGIN = FLAT_ROWS
SLOT = 2 * MARGIN + 3464
STAGES = 4
VEC_BASE = (VOCAB * D + 4 * D * D + 2 * D * FF) // LANES
VEC_ROWS = DEVICES * SHARD - VEC_BASE


ORDERS = (("x", "y", "z"), ("y", "z", "x"), ("z", "x", "y")) * 2
WEIGHT = {"z": 4, "y": 2, "x": 1}
CHIP_ORDER = ("xyz", "xy", "yz", "zx", "x", "y", "z", "")
HALF_ORDER = ((1, 1), (1, 0), (0, 1), (0, 0))
GATHER_ORDER = ((1, 0, 0), (0, 1, 0), (0, 0, 1), (1, 1, 0), (1, 0, 1), (0, 1, 1), (1, 1, 1))


def exchange_kernel(g_emb, g_attn, g_in, g_out, g_vecd, g_vecf, opt_m, opt_v, master, m_new, v_new, w_new, gathered,
                    stage, vecd_raw, vecd_buf, vecf_buf, acc, pair, half, quarter, eighth, m_buf, v_buf, w_buf, wb,
                    stage_sem, vec_sem, pair_send, pair_recv, half_send, half_recv, quarter_send, quarter_recv,
                    eighth_send, eighth_recv, state_sem, store_sem,
                    ring_send, ring_recv, share_send, share_recv, keep_sem):
    z, y, dx = lax.axis_index("dz"), lax.axis_index("dy"), lax.axis_index("dx")
    x, c = dx // 2, dx % 2
    mine = {"z": z, "y": y, "x": x}
    peers = {
        "c": {"dz": z, "dy": y, "dx": 2 * x + (1 - c)},
        "x": {"dz": z, "dy": y, "dx": 2 * (1 - x) + c},
        "y": {"dz": z, "dy": 1 - y, "dx": dx},
        "z": {"dz": 1 - z, "dy": y, "dx": dx},
    }

    def chip(part, bits):
        index = 0
        for axis, bit in zip(ORDERS[part], bits):
            index = index + WEIGHT[axis] * ((1 - mine[axis]) if bit else mine[axis])
        return index

    def rows(part):
        return pl.ds(PART_START[part], PART_ROWS[part])

    def acc_rows(part):
        return pl.ds(MARGIN + PART_START[part], PART_ROWS[part])

    vec_loads = [
        pltpu.make_async_copy(g_vecd, vecd_raw, vec_sem.at[0]), pltpu.make_async_copy(g_vecf, vecf_buf, vec_sem.at[1])]
    state = [
        pltpu.make_async_copy(opt_m, m_buf, state_sem.at[0]),
        pltpu.make_async_copy(opt_v, v_buf, state_sem.at[1]),
        pltpu.make_async_copy(master, w_buf, state_sem.at[2]),
    ]

    parts = range(PARTS)

    def chip_at(n):
        index = 0
        for axis in "zyx":
            index = index + WEIGHT[axis] * ((1 - mine[axis]) if axis in CHIP_ORDER[n] else mine[axis])
        return index

    sequence = [(False, 0), (True, 0), (False, 1)]
    for n in range(2, 8):
        sequence += [(False, n), (True, n - 1)]
    sequence.append((True, 7))

    def slot_at(own, n):
        return chip_at(7 if n == 0 and not own else n)

    def shard_at(place):
        own, n = sequence[place]
        return 2 * chip_at(n) + (c if own else 1 - c)

    def chunk_bounds(owner):
        low = (owner * SHARD) // FLAT_ROWS
        high = (owner * SHARD + SHARD + FLAT_ROWS - 1 - (owner // (DEVICES - 1)) * VEC_ROWS) // FLAT_ROWS
        return low, high

    def by_tensor(k, act):
        @pl.when(k < 32)
        def _():
            act(0, 0)

        @pl.when(k >= 32)
        def _():
            @pl.when(k < 80)
            def _():
                act(1, 32)

            @pl.when(k >= 80)
            def _():
                @pl.when(k < 112)
                def _():
                    act(2, 80)

                @pl.when(k >= 112)
                def _():
                    act(3, 112)

    grads = (g_emb, g_attn, g_in, g_out)

    def load_shard(place):
        low, high = chunk_bounds(shard_at(place))
        slot = place % STAGES

        def one(k, carry):
            where = k - low

            def start(tensor, first):
                pltpu.make_async_copy(
                    grads[tensor].at[pl.ds((k - first) * TILES, TILES)], stage.at[slot, pl.ds(where * TILES, TILES)],
                    stage_sem.at[slot, where]).start()

            by_tensor(k, start)
            return carry

        lax.fori_loop(low, high, one, 0)

    def flatten_shard(place):
        owner = shard_at(place)
        low, high = chunk_bounds(owner)
        slot = place % STAGES
        where = slot_at(*sequence[place])

        def one(k, carry):
            at = k - low
            pltpu.make_async_copy(
                g_emb.at[pl.ds(0, TILES)], stage.at[slot, pl.ds(at * TILES, TILES)], stage_sem.at[slot, at]).wait()
            base = MARGIN + k * FLAT_ROWS - owner * SHARD

            def spread(tensor, first):
                groups = TENSORS[tensor][1] // LANES
                bands = TILES // groups
                for j in range(groups):
                    tile = stage[slot, pl.ds(at * TILES + j, bands, stride=groups)]
                    acc[where, pl.ds(base + j, 8 * bands, stride=groups), :] = tile.reshape(8 * bands, LANES)

            by_tensor(k, spread)
            return carry

        lax.fori_loop(low, high, one, 0)

        @pl.when(owner == DEVICES - 1)
        def _():
            first = MARGIN + SHARD - VEC_ROWS
            second = first + 9 * D // LANES
            third = second + FF // LANES
            acc[where, first:second, :] = vecd_buf[...]
            acc[where, second:third, :] = vecf_buf[...]
            acc[where, third:MARGIN + SHARD, :] = jnp.zeros((MARGIN + SHARD - third, LANES), jnp.float32)

    def pair_copy(n, part):
        return pltpu.make_async_remote_copy(
            src_ref=acc.at[slot_at(False, n), acc_rows(part)], dst_ref=pair.at[chip_at(n), rows(part)],
            send_sem=pair_send.at[n, part], recv_sem=pair_recv.at[n, part],
            device_id=peers["c"], device_id_type=MESH)

    def half_copy(k, part):
        return pltpu.make_async_remote_copy(
            src_ref=acc.at[chip(part, (1,) + HALF_ORDER[k]), acc_rows(part)],
            dst_ref=half.at[part, k, pl.ds(0, PART_ROWS[part])],
            send_sem=half_send.at[k, part], recv_sem=half_recv.at[k, part],
            device_id=peers[ORDERS[part][0]], device_id_type=MESH)

    def quarter_copy(k, part):
        return pltpu.make_async_remote_copy(
            src_ref=acc.at[chip(part, (0, 1, 1 - k)), acc_rows(part)],
            dst_ref=quarter.at[part, k, pl.ds(0, PART_ROWS[part])],
            send_sem=quarter_send.at[k, part], recv_sem=quarter_recv.at[k, part],
            device_id=peers[ORDERS[part][1]], device_id_type=MESH)

    def eighth_copy(part):
        return pltpu.make_async_remote_copy(
            src_ref=acc.at[chip(part, (0, 0, 1)), acc_rows(part)],
            dst_ref=eighth.at[part, pl.ds(0, PART_ROWS[part])],
            send_sem=eighth_send.at[part], recv_sem=eighth_recv.at[part],
            device_id=peers[ORDERS[part][2]], device_id_type=MESH)

    barrier = pltpu.get_barrier_semaphore()
    for peer in peers.values():
        pl.semaphore_signal(barrier, inc=1, device_id=peer, device_id_type=MESH)
    for copy in vec_loads:
        copy.start()
    for place in range(STAGES):
        load_shard(place)
    for copy in vec_loads:
        copy.wait()
    for i in range(9):
        for j in range(D // LANES):
            row = i * (D // LANES) + j
            vecd_buf[row:row + 1, :] = vecd_raw[i, :, j * LANES:(j + 1) * LANES]

    def join(n):
        where = chip_at(n)
        for part in parts:
            pair_copy(n, part).wait_recv()
            acc[where, acc_rows(part)] += pair[where, rows(part)]
            bits = tuple(int(axis in CHIP_ORDER[n]) for axis in ORDERS[part])
            if bits[0]:
                half_copy(HALF_ORDER.index(bits[1:]), part).start()

    for place, (own, n) in enumerate(sequence):
        sent = n if own else 0
        if (own and n > 0) or (not own and n == 7):
            for part in parts:
                pair_copy(sent, part).wait_send()
        flatten_shard(place)
        if place == 0:
            pl.semaphore_wait(barrier, 4)
        if not own:
            for part in parts:
                pair_copy(n, part).start()
        if place + STAGES < len(sequence):
            load_shard(place + STAGES)
        if own and n > 0:
            join(n)
        elif (own, n) == (False, 1):
            join(0)
    for copy in state:
        copy.start()
    for k in range(4):
        for part in parts:
            half_copy(k, part).wait_recv()
            where = chip(part, (0,) + HALF_ORDER[k])
            acc[where, acc_rows(part)] += half[part, k, pl.ds(0, PART_ROWS[part])]
            if k < 2:
                quarter_copy(k, part).start()
    for k in range(2):
        for part in parts:
            quarter_copy(k, part).wait_recv()
            where = chip(part, (0, 0, 1 - k))
            acc[where, acc_rows(part)] += quarter[part, k, pl.ds(0, PART_ROWS[part])]
            if k == 0:
                eighth_copy(part).start()

    for copy in state:
        copy.wait()

    here = 4 * z + 2 * y + x

    def ring_copy(bits, hop, part):
        flipped = tuple(1 - bit if n == hop else bit for n, bit in enumerate(bits))
        slot = flipped[0] * 4 + flipped[1] * 2 + flipped[2]
        where = chip(part, bits)
        return pltpu.make_async_remote_copy(
            src_ref=wb.at[where, rows(part)], dst_ref=wb.at[where, rows(part)],
            send_sem=ring_send.at[slot, part], recv_sem=ring_recv.at[slot, part],
            device_id=peers[ORDERS[part][hop]], device_id_type=MESH)

    def share_copy(bits, part):
        slot = bits[0] * 4 + bits[1] * 2 + bits[2]
        where = chip(part, bits)
        return pltpu.make_async_remote_copy(
            src_ref=wb.at[where, rows(part)], dst_ref=gathered.at[where, c, rows(part)],
            send_sem=share_send.at[slot, part], recv_sem=share_recv.at[slot, part],
            device_id=peers["c"], device_id_type=MESH)

    def keep_copy(bits, part):
        slot = bits[0] * 4 + bits[1] * 2 + bits[2]
        where = chip(part, bits)
        return pltpu.make_async_copy(
            wb.at[where, rows(part)], gathered.at[where, c, rows(part)], keep_sem.at[slot, part])

    for part in parts:
        eighth_copy(part).wait_recv()
        start, count = PART_START[part], min(PART_ROWS[part], SHARD - PART_START[part])
        pieces = [(start, count)] if count % 16 == 0 else [(start, count // 16 * 16), (start + count // 16 * 16, count % 16)]
        for first, size in pieces:
            span = pl.ds(first, size)
            grad_sum = (acc[here, pl.ds(MARGIN + first, size)] + eighth[part, pl.ds(first - start, size)]) / DEVICES
            m_val = BETA_ONE * m_buf[span] + (1.0 - BETA_ONE) * grad_sum
            v_val = BETA_TWO * v_buf[span] + (1.0 - BETA_TWO) * grad_sum * grad_sum
            m_hat = m_val / (1.0 - BETA_ONE ** ADAM_STEP)
            v_hat = v_val / (1.0 - BETA_TWO ** ADAM_STEP)
            w_val = w_buf[span] - LEARN_RATE * m_hat / (jnp.sqrt(v_hat) + ADAM_EPS)
            m_buf[span] = m_val
            v_buf[span] = v_val
            w_buf[span] = w_val
            if size % 16:
                w_val = jnp.concatenate([w_val, jnp.zeros((16 - size % 16, LANES), jnp.float32)], axis=0)
                span = pl.ds(first, 16)
            wb[here, span] = w_val.astype(jnp.bfloat16)
        for hop in range(3):
            ring_copy((0, 0, 0), hop, part).start()
        share_copy((0, 0, 0), part).start()
        keep_copy((0, 0, 0), part).start()

    store = [
        pltpu.make_async_copy(m_buf, m_new, store_sem.at[0]),
        pltpu.make_async_copy(v_buf, v_new, store_sem.at[1]),
        pltpu.make_async_copy(w_buf, w_new, store_sem.at[2]),
    ]
    for copy in store:
        copy.start()

    def last_hop(bits):
        return max(n for n in range(3) if bits[n])

    for bits in GATHER_ORDER:
        hop = last_hop(bits)
        came = tuple(1 - bit if n == hop else bit for n, bit in enumerate(bits))
        for part in parts:
            ring_copy(came, hop, part).wait_recv()
            for later in range(hop + 1, 3):
                ring_copy(bits, later, part).start()
            share_copy(bits, part).start()
            keep_copy(bits, part).start()

    for part in parts:
        for k in range(4):
            half_copy(k, part).wait_send()
        for k in range(2):
            quarter_copy(k, part).wait_send()
        eighth_copy(part).wait_send()
        for bits in ((0, 0, 0),) + GATHER_ORDER:
            for later in range(0 if not any(bits) else last_hop(bits) + 1, 3):
                ring_copy(bits, later, part).wait_send()
            share_copy(bits, part).wait()
            keep_copy(bits, part).wait()
    for copy in store:
        copy.wait()


def exchange(*operands):
    shape = jax.ShapeDtypeStruct
    state_shape = shape((SHARD, LANES), jnp.float32)
    f32 = functools.partial(pltpu.VMEM, dtype=jnp.float32)
    dma = pltpu.SemaphoreType.DMA
    scratch = [
        f32((STAGES, SPAN * TILES, 8, LANES)), f32((9, 1, D)), f32((9 * D // LANES, LANES)),
        f32((FF // LANES, LANES)),
        f32((8, SLOT, LANES)), f32((8, PAD, LANES)),
        f32((PARTS, 4, PART_MAX, LANES)), f32((PARTS, 2, PART_MAX, LANES)), f32((PARTS, PART_MAX, LANES)),
        f32((SHARD, LANES)), f32((SHARD, LANES)), f32((SHARD, LANES)),
        pltpu.VMEM((8, PAD, LANES), jnp.bfloat16),
        dma((STAGES, SPAN)), dma((2,)), dma((8, PARTS)), dma((8, PARTS)),
        dma((4, PARTS)), dma((4, PARTS)), dma((2, PARTS)), dma((2, PARTS)),
        dma((PARTS,)), dma((PARTS,)), dma((3,)), dma((3,)),
        dma((8, PARTS)), dma((8, PARTS)), dma((8, PARTS)), dma((8, PARTS)), dma((8, PARTS)),
    ]
    return pl.pallas_call(
        exchange_kernel,
        out_shape=(state_shape, state_shape, state_shape, shape((8, 2, PAD, LANES), jnp.bfloat16)),
        in_specs=[pl.BlockSpec(memory_space=pl.ANY)] * 9,
        out_specs=(pl.BlockSpec(memory_space=pl.ANY),) * 4,
        scratch_shapes=scratch,
        compiler_params=pltpu.CompilerParams(vmem_limit_bytes=VMEM_MAX, collective_id=0, has_side_effects=True),
        name="exchange",
    )(*operands)


SUB = 512
UNROLL = 2
CHUNK = UNROLL * SUB
RING = 6
ACT_SLOTS = 2 * UNROLL
GELU_A = math.sqrt(2.0 / math.pi)
GELU_B = GELU_A * 0.044715
WIDEN_ORDER = (8, 9, 10, 11, 12, 13, 14, 15, 0, 1, 2, 3, 4, 5, 6, 7)


def ffn_kernel(steps, ids_in, act, flat, m_in, v_in, master_in,
               y_out, o_emb, o_attn, o_in, o_out, o_vecd, o_vecf, m_out, v_out, master_out,
               ids, dense, ring, act_buf, y_buf, w_in, w_out, b_in, b_out, vecd_wide, vecd_buf, vecf_buf,
               rows_one, rows_two, h_one, h_two, u_one, u_two, emb_buf, attn_buf, state_buf,
               ring_sem, act_sem, y_sem, emb_sem, attn_sem, weight_sem, state_sem, ids_sem):
    emb_rows, attn_rows = VOCAB // steps, 4 * D // steps

    blocks = steps * UNROLL

    def load_act(block):
        slot = lax.rem(block, ACT_SLOTS)
        return pltpu.make_async_copy(act.at[pl.ds(block * SUB, SUB)], act_buf.at[slot], act_sem.at[slot])

    def store_y(it):
        return pltpu.make_async_copy(
            y_buf.at[lax.rem(it, 2)], y_out.at[pl.ds(it * CHUNK - SUB, CHUNK)], y_sem.at[lax.rem(it, 2)])

    store_first = pltpu.make_async_copy(
        y_buf.at[0, pl.ds(SUB, CHUNK - SUB)], y_out.at[pl.ds(0, CHUNK - SUB)], y_sem.at[0])
    store_last = pltpu.make_async_copy(
        y_buf.at[steps % 2, pl.ds(0, SUB)], y_out.at[pl.ds(steps * CHUNK - SUB, SUB)], y_sem.at[steps % 2])

    def store_emb(it):
        return pltpu.make_async_copy(
            emb_buf.at[lax.rem(it, 2)], o_emb.at[pl.ds(it * emb_rows, emb_rows)], emb_sem.at[lax.rem(it, 2)])

    def store_attn(it):
        return pltpu.make_async_copy(
            attn_buf.at[lax.rem(it, 2)], o_attn.at[pl.ds(it * attn_rows, attn_rows)], attn_sem.at[lax.rem(it, 2)])

    def load_flat(n):
        return pltpu.make_async_copy(flat.at[WIDEN_ORDER[n]], ring.at[n % RING], ring_sem.at[n % RING])

    for n in range(RING):
        load_flat(n).start()
    load_ids = pltpu.make_async_copy(ids_in, ids, ids_sem)
    load_ids.start()
    for block in range(UNROLL + 1):
        load_act(block).start()

    def relayout(base, groups, row, buf, at):
        for j in range(groups):
            q = base + row * groups + j
            top = dense[pl.ds(q, 8, stride=groups), :]
            low = dense[pl.ds(q + 8 * groups, 8, stride=groups), :]
            buf[pl.ds(at, 16), j * LANES:(j + 1) * LANES] = jnp.concatenate([top, low], axis=0).astype(jnp.bfloat16)

    for n, owner in enumerate(WIDEN_ORDER):
        load_flat(n).wait()
        at = owner * SHARD
        whole = SHARD // 16

        def widen(t, carry, at=at, slot=n % RING):
            row = pl.multiple_of(t * 16, 16)
            dense[pl.ds(at + row, 16), :] = ring[slot, pl.ds(row, 16), :].astype(jnp.float32)
            return carry

        lax.fori_loop(0, whole, widen, 0, unroll=24)
        tail = ring[n % RING, whole * 16:whole * 16 + 16, :].astype(jnp.float32)
        dense[at + whole * 16:at + SHARD, :] = tail[:SHARD - whole * 16]
        if n + RING < DEVICES:
            load_flat(n + RING).start()
        if owner == 12:
            def fill_in(t, carry):
                row = pl.multiple_of(t * 16, 16)
                relayout(TENSORS[2][2], FF // LANES, row, w_in, row)
                return carry

            lax.fori_loop(0, D // 16, fill_in, 0, unroll=4)
            pltpu.make_async_copy(w_in, o_in, weight_sem.at[0]).start()
        if owner == 15:
            def fill_out(t, carry):
                row = pl.multiple_of(t * 16, 16)
                relayout(TENSORS[3][2], D // LANES, row, w_out, row)
                return carry

            lax.fori_loop(0, FF // 16, fill_out, 0, unroll=8)
            pltpu.make_async_copy(w_out, o_out, weight_sem.at[1]).start()
            for i in range(9):
                for j in range(D // LANES):
                    q = VEC_BASE + i * (D // LANES) + j
                    vecd_wide[i:i + 1, j * LANES:(j + 1) * LANES] = dense[q:q + 1, :]
            for j in range(D // LANES):
                q = VEC_BASE + 8 * (D // LANES) + j
                b_out[:, j * LANES:(j + 1) * LANES] = dense[q:q + 1, :]
            for j in range(FF // LANES):
                q = VEC_BASE + 9 * (D // LANES) + j
                b_in[:, j * LANES:(j + 1) * LANES] = dense[q:q + 1, :]
            vecd_buf[...] = vecd_wide[...].astype(jnp.bfloat16)
            vecf_buf[...] = b_in[...].astype(jnp.bfloat16)
            pltpu.make_async_copy(vecd_buf, o_vecd, weight_sem.at[2]).start()
            pltpu.make_async_copy(vecf_buf, o_vecf, weight_sem.at[3]).start()

    def lookup(block, h_buf, rows_buf):
        slot = lax.rem(block, ACT_SLOTS)
        token = jnp.minimum(block, blocks - 1) * SUB
        for tile in range(SUB // 8):
            for i in range(8):
                row = ids[token + tile * 8 + i] * (D // LANES)
                rows_buf[pl.ds(tile * 56 + i * 7, 8), :] = dense[pl.ds(row, 8), :]
        for pair in range(SUB // 16):
            for j in range(D // LANES):
                top = rows_buf[pl.ds(pair * 112 + j, 8, stride=7), :]
                low = rows_buf[pl.ds(pair * 112 + 56 + j, 8, stride=7), :]
                both = jnp.concatenate([top, low], axis=0) * math.sqrt(D)
                a_val = act_buf[slot, pair * 16:pair * 16 + 16, j * LANES:(j + 1) * LANES].astype(jnp.float32)
                h_buf[pair * 16:pair * 16 + 16, j * LANES:(j + 1) * LANES] = (both + a_val).astype(jnp.bfloat16)

    def widen_tokens(h_buf, u_buf):
        pre = jnp.dot(h_buf[...], w_in[...], preferred_element_type=jnp.float32) + b_in[...]
        bent = jnp.tanh(pre * (GELU_A + GELU_B * (pre * pre)))
        flat_half = 0.5 * pre
        u_buf[...] = (flat_half + flat_half * bent).astype(jnp.bfloat16)

    def narrow_tokens(it, part, u_buf):
        y_val = jnp.dot(u_buf[...], w_out[...], preferred_element_type=jnp.float32) + b_out[...]
        y_buf[lax.rem(it, 2), part * SUB:part * SUB + SUB, :] = y_val.astype(jnp.bfloat16)

    load_ids.wait()
    load_act(0).wait()
    lookup(0, h_one, rows_one)

    moves = []
    for n, (source, target) in enumerate(((m_in, m_out), (v_in, v_out), (master_in, master_out))):
        moves.append(pltpu.make_async_copy(source, state_buf, state_sem.at[2 * n]))
        moves.append(pltpu.make_async_copy(state_buf, target, state_sem.at[2 * n + 1]))

    def body(it, carry):
        for part in range(1, UNROLL):
            load_act(it * UNROLL + part).wait()

        @pl.when(it + 1 < steps)
        def _():
            load_act(it * UNROLL + UNROLL).wait()
            for part in range(UNROLL + 1, 2 * UNROLL):
                load_act(it * UNROLL + part).start()

        @pl.when(it + 2 < steps)
        def _():
            load_act(it * UNROLL + 2 * UNROLL).start()

        @pl.when(it == 2)
        def _():
            store_first.wait()

        @pl.when(it > 2)
        def _():
            store_y(it - 2).wait()

        @pl.when(it >= 2)
        def _():
            store_emb(it - 2).wait()
            store_attn(it - 2).wait()

        for n, move in enumerate(moves):
            @pl.when(it == 1 + n)
            def _(n=n, move=move):
                if n:
                    moves[n - 1].wait()
                move.start()

        buffers = ((h_one, rows_one, u_one), (h_two, rows_two, u_two))
        for part in range(UNROLL):
            h_now, _, u_now = buffers[part % 2]
            h_next, rows_next, u_before = buffers[(part + 1) % 2]
            lookup(it * UNROLL + part + 1, h_next, rows_next)
            widen_tokens(h_now, u_now)
            narrow_tokens(it, part, u_before)
        for t in range(emb_rows // 16):
            relayout(TENSORS[0][2], D // LANES, it * emb_rows + t * 16, emb_buf.at[lax.rem(it, 2)], t * 16)
        for t in range(attn_rows // 16):
            relayout(TENSORS[1][2], D // LANES, it * attn_rows + t * 16, attn_buf.at[lax.rem(it, 2)], t * 16)
        @pl.when(it == 0)
        def _():
            store_first.start()

        @pl.when(it > 0)
        def _():
            store_y(it).start()

        store_emb(it).start()
        store_attn(it).start()
        return carry

    lax.fori_loop(0, steps, body, 0)
    store_y(steps - 2).wait()
    narrow_tokens(steps, 0, u_two)
    store_last.start()
    store_y(steps - 1).wait()
    store_last.wait()
    for it in (steps - 2, steps - 1):
        store_emb(it).wait()
        store_attn(it).wait()
    moves[-1].wait()
    pltpu.make_async_copy(w_in, o_in, weight_sem.at[0]).wait()
    pltpu.make_async_copy(w_out, o_out, weight_sem.at[1]).wait()
    pltpu.make_async_copy(vecd_buf, o_vecd, weight_sem.at[2]).wait()
    pltpu.make_async_copy(vecf_buf, o_vecf, weight_sem.at[3]).wait()


def ffn(ids, act, flat, m_new, v_new, w_new):
    tokens = act.shape[0]
    steps = tokens // CHUNK
    f32, bf16 = jnp.float32, jnp.bfloat16
    shape = jax.ShapeDtypeStruct
    dma = pltpu.SemaphoreType.DMA
    anywhere = pl.BlockSpec(memory_space=pl.ANY)
    state = shape((SHARD, LANES), f32)
    return pl.pallas_call(
        functools.partial(ffn_kernel, steps),
        out_shape=(shape((tokens, D), bf16), shape((VOCAB, D), bf16), shape((4 * D, D), bf16), shape((D, FF), bf16),
                   shape((FF, D), bf16), shape((9, D), bf16), shape((1, FF), bf16), state, state, state),
        in_specs=[anywhere] * 6,
        out_specs=(anywhere,) * 10,
        scratch_shapes=[
            pltpu.SMEM((tokens,), jnp.int32),
            pltpu.VMEM((DEVICES * SHARD, LANES), f32),
            pltpu.VMEM((RING, PAD, LANES), bf16),
            pltpu.VMEM((ACT_SLOTS, SUB, D), bf16),
            pltpu.VMEM((2, CHUNK, D), bf16),
            pltpu.VMEM((D, FF), bf16),
            pltpu.VMEM((FF, D), bf16),
            pltpu.VMEM((1, FF), f32),
            pltpu.VMEM((1, D), f32),
            pltpu.VMEM((9, D), f32),
            pltpu.VMEM((9, D), bf16),
            pltpu.VMEM((1, FF), bf16),
            pltpu.VMEM((SUB * 7 + 8, LANES), f32),
            pltpu.VMEM((SUB * 7 + 8, LANES), f32),
            pltpu.VMEM((SUB, D), bf16),
            pltpu.VMEM((SUB, D), bf16),
            pltpu.VMEM((SUB, FF), bf16),
            pltpu.VMEM((SUB, FF), bf16),
            pltpu.VMEM((2, VOCAB // steps, D), bf16),
            pltpu.VMEM((2, 4 * D // steps, D), bf16),
            pltpu.VMEM((SHARD, LANES), f32),
            dma((RING,)), dma((ACT_SLOTS,)), dma((2,)), dma((2,)), dma((2,)), dma((4,)), dma((6,)), dma,
        ],
        compiler_params=pltpu.CompilerParams(vmem_limit_bytes=VMEM_MAX),
        name="ffn",
    )(ids, act, flat, m_new, v_new, w_new)


def solution(mesh):
    def device_step(g_emb, g_attn, g_in, g_out, g_vecd, g_vecf, opt_m, opt_v, master, tok_ids, act_in):
        def tiles(grad, cols):
            split = grad.reshape(-1, 8, cols // LANES, LANES)
            return split.transpose(0, 2, 1, 3).reshape(-1, 8, LANES)

        m_new, v_new, w_new, gathered = exchange(
            tiles(g_emb, D), tiles(g_attn, D), tiles(g_in, FF), tiles(g_out, D),
            g_vecd.reshape(9, 1, D), g_vecf.reshape(-1, LANES), opt_m.reshape(SHARD, LANES),
            opt_v.reshape(SHARD, LANES), master.reshape(SHARD, LANES))
        flat = gathered.reshape(DEVICES, PAD, LANES)
        y_out, wb_emb, wb_attn, wb_in, wb_out, wb_vecd, wb_vecf, m_new, v_new, w_new = ffn(
            tok_ids, act_in, flat, m_new, v_new, w_new)
        return (m_new.reshape(-1), v_new.reshape(-1), w_new.reshape(-1), wb_emb, wb_attn.reshape(1, 4, D, D),
                wb_in[None], wb_out[None], wb_vecd[None], wb_vecf, y_out)

    grad_specs = tuple(P(AXES, *([None] * (grad_rank - 1))) for grad_rank in GRAD_RANKS)
    in_specs = grad_specs + (P(AXES), P(AXES), P(AXES), P(AXES), P(AXES, None))
    out_specs = (P(AXES), P(AXES), P(AXES), P(), P(), P(), P(), P(), P(), P(AXES, None))
    return jax.shard_map(device_step, mesh=mesh, in_specs=in_specs, out_specs=out_specs, check_vma=False)
```

```python
import functools
import math

import jax
import jax.numpy as jnp
from jax import lax
from jax.experimental import pallas as pl
from jax.experimental.pallas import tpu as pltpu
from jax.sharding import PartitionSpec as P

LEARN_RATE = 0.002
BETA_ONE = 0.9
BETA_TWO = 0.95
ADAM_EPS = 1e-8
ADAM_STEP = 2
AXES = ("dz", "dy", "dx")
GRAD_RANKS = (3, 5, 4, 4, 4, 3)
MESH = pl.DeviceIdType.MESH

D = 768
FF = 2048
VOCAB = 2048
DEVICES = 16
LANES = 128
SHARD = 3461
PAD = 3472
PART_START = (0, 576, 1152, 1728, 2304, 2880)
PART_ROWS = (576, 576, 576, 576, 576, 592)
PART_MAX = 592
PARTS = 6
VMEM_MAX = 67_000_000

TENSORS = (
    (VOCAB, D, 0),
    (4 * D, D, VOCAB * D // LANES),
    (D, FF, (VOCAB * D + 4 * D * D) // LANES),
    (FF, D, (VOCAB * D + 4 * D * D + D * FF) // LANES),
)
TILES = 48
FLAT_ROWS = 8 * TILES
CHUNKS = 144
SPAN = 11
MARGIN = FLAT_ROWS
SLOT = 2 * MARGIN + 3464
STAGES = 4
VEC_BASE = (VOCAB * D + 4 * D * D + 2 * D * FF) // LANES
VEC_ROWS = DEVICES * SHARD - VEC_BASE


ORDERS = (("x", "y", "z"), ("y", "z", "x"), ("z", "x", "y")) * 2
WEIGHT = {"z": 4, "y": 2, "x": 1}
CHIP_ORDER = ("xyz", "xy", "yz", "zx", "x", "y", "z", "")
HALF_ORDER = ((1, 1), (1, 0), (0, 1), (0, 0))
GATHER_ORDER = ((1, 0, 0), (0, 1, 0), (0, 0, 1), (1, 1, 0), (1, 0, 1), (0, 1, 1), (1, 1, 1))


def exchange_kernel(g_emb, g_attn, g_in, g_out, g_vecd, g_vecf, opt_m, opt_v, master, m_new, v_new, w_new, gathered,
                    stage, vecd_raw, vecd_buf, vecf_buf, acc, pair, half, quarter, eighth, m_buf, v_buf, w_buf, wb,
                    stage_sem, vec_sem, pair_send, pair_recv, half_send, half_recv, quarter_send, quarter_recv,
                    eighth_send, eighth_recv, state_sem, store_sem,
                    ring_send, ring_recv, share_send, share_recv, keep_sem):
    z, y, dx = lax.axis_index("dz"), lax.axis_index("dy"), lax.axis_index("dx")
    x, c = dx // 2, dx % 2
    mine = {"z": z, "y": y, "x": x}
    peers = {
        "c": {"dz": z, "dy": y, "dx": 2 * x + (1 - c)},
        "x": {"dz": z, "dy": y, "dx": 2 * (1 - x) + c},
        "y": {"dz": z, "dy": 1 - y, "dx": dx},
        "z": {"dz": 1 - z, "dy": y, "dx": dx},
    }

    def chip(part, bits):
        index = 0
        for axis, bit in zip(ORDERS[part], bits):
            index = index + WEIGHT[axis] * ((1 - mine[axis]) if bit else mine[axis])
        return index

    def rows(part):
        return pl.ds(PART_START[part], PART_ROWS[part])

    def acc_rows(part):
        return pl.ds(MARGIN + PART_START[part], PART_ROWS[part])

    vec_loads = [
        pltpu.make_async_copy(g_vecd, vecd_raw, vec_sem.at[0]), pltpu.make_async_copy(g_vecf, vecf_buf, vec_sem.at[1])]
    state = [
        pltpu.make_async_copy(opt_m, m_buf, state_sem.at[0]),
        pltpu.make_async_copy(opt_v, v_buf, state_sem.at[1]),
        pltpu.make_async_copy(master, w_buf, state_sem.at[2]),
    ]

    parts = range(PARTS)

    def chip_at(n):
        index = 0
        for axis in "zyx":
            index = index + WEIGHT[axis] * ((1 - mine[axis]) if axis in CHIP_ORDER[n] else mine[axis])
        return index

    sequence = [(False, 0), (True, 0), (False, 1)]
    for n in range(2, 8):
        sequence += [(False, n), (True, n - 1)]
    sequence.append((True, 7))

    def slot_at(own, n):
        return chip_at(7 if n == 0 and not own else n)

    def shard_at(place):
        own, n = sequence[place]
        return 2 * chip_at(n) + (c if own else 1 - c)

    def chunk_bounds(owner):
        low = (owner * SHARD) // FLAT_ROWS
        high = (owner * SHARD + SHARD + FLAT_ROWS - 1 - (owner // (DEVICES - 1)) * VEC_ROWS) // FLAT_ROWS
        return low, high

    def by_tensor(k, act):
        @pl.when(k < 32)
        def _():
            act(0, 0)

        @pl.when(k >= 32)
        def _():
            @pl.when(k < 80)
            def _():
                act(1, 32)

            @pl.when(k >= 80)
            def _():
                @pl.when(k < 112)
                def _():
                    act(2, 80)

                @pl.when(k >= 112)
                def _():
                    act(3, 112)

    grads = (g_emb, g_attn, g_in, g_out)

    def load_shard(place):
        low, high = chunk_bounds(shard_at(place))
        slot = place % STAGES

        def one(k, carry):
            where = k - low

            def start(tensor, first):
                pltpu.make_async_copy(
                    grads[tensor].at[pl.ds((k - first) * TILES, TILES)], stage.at[slot, pl.ds(where * TILES, TILES)],
                    stage_sem.at[slot, where]).start()

            by_tensor(k, start)
            return carry

        lax.fori_loop(low, high, one, 0)

    def flatten_shard(place):
        owner = shard_at(place)
        low, high = chunk_bounds(owner)
        slot = place % STAGES
        where = slot_at(*sequence[place])

        def one(k, carry):
            at = k - low
            pltpu.make_async_copy(
                g_emb.at[pl.ds(0, TILES)], stage.at[slot, pl.ds(at * TILES, TILES)], stage_sem.at[slot, at]).wait()
            base = MARGIN + k * FLAT_ROWS - owner * SHARD

            def spread(tensor, first):
                groups = TENSORS[tensor][1] // LANES
                bands = TILES // groups
                for j in range(groups):
                    tile = stage[slot, pl.ds(at * TILES + j, bands, stride=groups)]
                    acc[where, pl.ds(base + j, 8 * bands, stride=groups), :] = tile.reshape(8 * bands, LANES)

            by_tensor(k, spread)
            return carry

        lax.fori_loop(low, high, one, 0)

        @pl.when(owner == DEVICES - 1)
        def _():
            first = MARGIN + SHARD - VEC_ROWS
            second = first + 9 * D // LANES
            third = second + FF // LANES
            acc[where, first:second, :] = vecd_buf[...]
            acc[where, second:third, :] = vecf_buf[...]
            acc[where, third:MARGIN + SHARD, :] = jnp.zeros((MARGIN + SHARD - third, LANES), jnp.float32)

    def pair_copy(n, part):
        return pltpu.make_async_remote_copy(
            src_ref=acc.at[slot_at(False, n), acc_rows(part)], dst_ref=pair.at[chip_at(n), rows(part)],
            send_sem=pair_send.at[n, part], recv_sem=pair_recv.at[n, part],
            device_id=peers["c"], device_id_type=MESH)

    def half_copy(k, part):
        return pltpu.make_async_remote_copy(
            src_ref=acc.at[chip(part, (1,) + HALF_ORDER[k]), acc_rows(part)],
            dst_ref=half.at[part, k, pl.ds(0, PART_ROWS[part])],
            send_sem=half_send.at[k, part], recv_sem=half_recv.at[k, part],
            device_id=peers[ORDERS[part][0]], device_id_type=MESH)

    def quarter_copy(k, part):
        return pltpu.make_async_remote_copy(
            src_ref=acc.at[chip(part, (0, 1, 1 - k)), acc_rows(part)],
            dst_ref=quarter.at[part, k, pl.ds(0, PART_ROWS[part])],
            send_sem=quarter_send.at[k, part], recv_sem=quarter_recv.at[k, part],
            device_id=peers[ORDERS[part][1]], device_id_type=MESH)

    def eighth_copy(part):
        return pltpu.make_async_remote_copy(
            src_ref=acc.at[chip(part, (0, 0, 1)), acc_rows(part)],
            dst_ref=eighth.at[part, pl.ds(0, PART_ROWS[part])],
            send_sem=eighth_send.at[part], recv_sem=eighth_recv.at[part],
            device_id=peers[ORDERS[part][2]], device_id_type=MESH)

    barrier = pltpu.get_barrier_semaphore()
    for peer in peers.values():
        pl.semaphore_signal(barrier, inc=1, device_id=peer, device_id_type=MESH)
    for copy in vec_loads:
        copy.start()
    for place in range(STAGES):
        load_shard(place)
    for copy in vec_loads:
        copy.wait()
    for i in range(9):
        for j in range(D // LANES):
            row = i * (D // LANES) + j
            vecd_buf[row:row + 1, :] = vecd_raw[i, :, j * LANES:(j + 1) * LANES]

    def join(n):
        where = chip_at(n)
        for part in parts:
            pair_copy(n, part).wait_recv()
            acc[where, acc_rows(part)] += pair[where, rows(part)]
            bits = tuple(int(axis in CHIP_ORDER[n]) for axis in ORDERS[part])
            if bits[0]:
                half_copy(HALF_ORDER.index(bits[1:]), part).start()

    for place, (own, n) in enumerate(sequence):
        sent = n if own else 0
        if (own and n > 0) or (not own and n == 7):
            for part in parts:
                pair_copy(sent, part).wait_send()
        flatten_shard(place)
        if place == 0:
            pl.semaphore_wait(barrier, 4)
        if not own:
            for part in parts:
                pair_copy(n, part).start()
        if place + STAGES < len(sequence):
            load_shard(place + STAGES)
        if own and n > 0:
            join(n)
        elif (own, n) == (False, 1):
            join(0)
    for copy in state:
        copy.start()
    for k in range(4):
        for part in parts:
            half_copy(k, part).wait_recv()
            where = chip(part, (0,) + HALF_ORDER[k])
            acc[where, acc_rows(part)] += half[part, k, pl.ds(0, PART_ROWS[part])]
            if k < 2:
                quarter_copy(k, part).start()
    for k in range(2):
        for part in parts:
            quarter_copy(k, part).wait_recv()
            where = chip(part, (0, 0, 1 - k))
            acc[where, acc_rows(part)] += quarter[part, k, pl.ds(0, PART_ROWS[part])]
            if k == 0:
                eighth_copy(part).start()

    for copy in state:
        copy.wait()

    here = 4 * z + 2 * y + x

    def ring_copy(bits, hop, part):
        flipped = tuple(1 - bit if n == hop else bit for n, bit in enumerate(bits))
        slot = flipped[0] * 4 + flipped[1] * 2 + flipped[2]
        where = chip(part, bits)
        return pltpu.make_async_remote_copy(
            src_ref=wb.at[where, rows(part)], dst_ref=wb.at[where, rows(part)],
            send_sem=ring_send.at[slot, part], recv_sem=ring_recv.at[slot, part],
            device_id=peers[ORDERS[part][hop]], device_id_type=MESH)

    def share_copy(bits, part):
        slot = bits[0] * 4 + bits[1] * 2 + bits[2]
        where = chip(part, bits)
        return pltpu.make_async_remote_copy(
            src_ref=wb.at[where, rows(part)], dst_ref=gathered.at[where, c, rows(part)],
            send_sem=share_send.at[slot, part], recv_sem=share_recv.at[slot, part],
            device_id=peers["c"], device_id_type=MESH)

    def keep_copy(bits, part):
        slot = bits[0] * 4 + bits[1] * 2 + bits[2]
        where = chip(part, bits)
        return pltpu.make_async_copy(
            wb.at[where, rows(part)], gathered.at[where, c, rows(part)], keep_sem.at[slot, part])

    for part in parts:
        eighth_copy(part).wait_recv()
        start, count = PART_START[part], min(PART_ROWS[part], SHARD - PART_START[part])
        pieces = [(start, count)] if count % 16 == 0 else [(start, count // 16 * 16), (start + count // 16 * 16, count % 16)]
        for first, size in pieces:
            span = pl.ds(first, size)
            grad_sum = (acc[here, pl.ds(MARGIN + first, size)] + eighth[part, pl.ds(first - start, size)]) / DEVICES
            m_val = BETA_ONE * m_buf[span] + (1.0 - BETA_ONE) * grad_sum
            v_val = BETA_TWO * v_buf[span] + (1.0 - BETA_TWO) * grad_sum * grad_sum
            m_hat = m_val / (1.0 - BETA_ONE ** ADAM_STEP)
            v_hat = v_val / (1.0 - BETA_TWO ** ADAM_STEP)
            w_val = w_buf[span] - LEARN_RATE * m_hat / (jnp.sqrt(v_hat) + ADAM_EPS)
            m_buf[span] = m_val
            v_buf[span] = v_val
            w_buf[span] = w_val
            if size % 16:
                w_val = jnp.concatenate([w_val, jnp.zeros((16 - size % 16, LANES), jnp.float32)], axis=0)
                span = pl.ds(first, 16)
            wb[here, span] = w_val.astype(jnp.bfloat16)
        for hop in range(3):
            ring_copy((0, 0, 0), hop, part).start()
        share_copy((0, 0, 0), part).start()
        keep_copy((0, 0, 0), part).start()

    store = [
        pltpu.make_async_copy(m_buf, m_new, store_sem.at[0]),
        pltpu.make_async_copy(v_buf, v_new, store_sem.at[1]),
        pltpu.make_async_copy(w_buf, w_new, store_sem.at[2]),
    ]
    for copy in store:
        copy.start()

    def last_hop(bits):
        return max(n for n in range(3) if bits[n])

    for bits in GATHER_ORDER:
        hop = last_hop(bits)
        came = tuple(1 - bit if n == hop else bit for n, bit in enumerate(bits))
        for part in parts:
            ring_copy(came, hop, part).wait_recv()
            for later in range(hop + 1, 3):
                ring_copy(bits, later, part).start()
            share_copy(bits, part).start()
            keep_copy(bits, part).start()

    for part in parts:
        for k in range(4):
            half_copy(k, part).wait_send()
        for k in range(2):
            quarter_copy(k, part).wait_send()
        eighth_copy(part).wait_send()
        for bits in ((0, 0, 0),) + GATHER_ORDER:
            for later in range(0 if not any(bits) else last_hop(bits) + 1, 3):
                ring_copy(bits, later, part).wait_send()
            share_copy(bits, part).wait()
            keep_copy(bits, part).wait()
    for copy in store:
        copy.wait()


def exchange(*operands):
    shape = jax.ShapeDtypeStruct
    state_shape = shape((SHARD, LANES), jnp.float32)
    f32 = functools.partial(pltpu.VMEM, dtype=jnp.float32)
    dma = pltpu.SemaphoreType.DMA
    scratch = [
        f32((STAGES, SPAN * TILES, 8, LANES)), f32((9, 1, D)), f32((9 * D // LANES, LANES)),
        f32((FF // LANES, LANES)),
        f32((8, SLOT, LANES)), f32((8, PAD, LANES)),
        f32((PARTS, 4, PART_MAX, LANES)), f32((PARTS, 2, PART_MAX, LANES)), f32((PARTS, PART_MAX, LANES)),
        f32((SHARD, LANES)), f32((SHARD, LANES)), f32((SHARD, LANES)),
        pltpu.VMEM((8, PAD, LANES), jnp.bfloat16),
        dma((STAGES, SPAN)), dma((2,)), dma((8, PARTS)), dma((8, PARTS)),
        dma((4, PARTS)), dma((4, PARTS)), dma((2, PARTS)), dma((2, PARTS)),
        dma((PARTS,)), dma((PARTS,)), dma((3,)), dma((3,)),
        dma((8, PARTS)), dma((8, PARTS)), dma((8, PARTS)), dma((8, PARTS)), dma((8, PARTS)),
    ]
    return pl.pallas_call(
        exchange_kernel,
        out_shape=(state_shape, state_shape, state_shape, shape((8, 2, PAD, LANES), jnp.bfloat16)),
        in_specs=[pl.BlockSpec(memory_space=pl.ANY)] * 9,
        out_specs=(pl.BlockSpec(memory_space=pl.ANY),) * 4,
        scratch_shapes=scratch,
        compiler_params=pltpu.CompilerParams(vmem_limit_bytes=VMEM_MAX, collective_id=0, has_side_effects=True),
        name="exchange",
    )(*operands)


SUB = 512
UNROLL = 2
CHUNK = UNROLL * SUB
RING = 6
ACT_SLOTS = 2 * UNROLL
GELU_A = math.sqrt(2.0 / math.pi)
GELU_B = GELU_A * 0.044715
WIDEN_ORDER = (8, 9, 10, 11, 12, 13, 14, 15, 0, 1, 2, 3, 4, 5, 6, 7)


def ffn_kernel(steps, ids_in, act, flat, m_in, v_in, master_in,
               y_out, o_emb, o_attn, o_in, o_out, o_vecd, o_vecf, m_out, v_out, master_out,
               ids, dense, ring, act_buf, y_buf, w_in, w_out, b_in, b_out, vecd_wide, vecd_buf, vecf_buf,
               rows_one, rows_two, h_one, h_two, u_one, u_two, emb_buf, attn_buf, state_buf,
               ring_sem, act_sem, y_sem, emb_sem, attn_sem, weight_sem, state_sem, ids_sem):
    emb_rows, attn_rows = VOCAB // steps, 4 * D // steps

    blocks = steps * UNROLL

    def load_act(block):
        slot = lax.rem(block, ACT_SLOTS)
        return pltpu.make_async_copy(act.at[pl.ds(block * SUB, SUB)], act_buf.at[slot], act_sem.at[slot])

    def store_y(it):
        return pltpu.make_async_copy(
            y_buf.at[lax.rem(it, 2)], y_out.at[pl.ds(it * CHUNK, CHUNK)], y_sem.at[lax.rem(it, 2)])

    def store_emb(it):
        return pltpu.make_async_copy(
            emb_buf.at[lax.rem(it, 2)], o_emb.at[pl.ds(it * emb_rows, emb_rows)], emb_sem.at[lax.rem(it, 2)])

    def store_attn(it):
        return pltpu.make_async_copy(
            attn_buf.at[lax.rem(it, 2)], o_attn.at[pl.ds(it * attn_rows, attn_rows)], attn_sem.at[lax.rem(it, 2)])

    def load_flat(n):
        return pltpu.make_async_copy(flat.at[WIDEN_ORDER[n]], ring.at[n % RING], ring_sem.at[n % RING])

    for n in range(RING):
        load_flat(n).start()
    load_ids = pltpu.make_async_copy(ids_in, ids, ids_sem)
    load_ids.start()
    for block in range(UNROLL + 1):
        load_act(block).start()

    def relayout(base, groups, row, buf, at):
        for j in range(groups):
            q = base + row * groups + j
            top = dense[pl.ds(q, 8, stride=groups), :]
            low = dense[pl.ds(q + 8 * groups, 8, stride=groups), :]
            buf[pl.ds(at, 16), j * LANES:(j + 1) * LANES] = jnp.concatenate([top, low], axis=0).astype(jnp.bfloat16)

    for n, owner in enumerate(WIDEN_ORDER):
        load_flat(n).wait()
        at = owner * SHARD
        whole = SHARD // 16

        def widen(t, carry, at=at, slot=n % RING):
            row = pl.multiple_of(t * 16, 16)
            dense[pl.ds(at + row, 16), :] = ring[slot, pl.ds(row, 16), :].astype(jnp.float32)
            return carry

        lax.fori_loop(0, whole, widen, 0, unroll=31)
        tail = ring[n % RING, whole * 16:whole * 16 + 16, :].astype(jnp.float32)
        dense[at + whole * 16:at + SHARD, :] = tail[:SHARD - whole * 16]
        if n + RING < DEVICES:
            load_flat(n + RING).start()
        if owner == 12:
            def fill_in(t, carry):
                row = pl.multiple_of(t * 16, 16)
                relayout(TENSORS[2][2], FF // LANES, row, w_in, row)
                return carry

            lax.fori_loop(0, D // 16, fill_in, 0, unroll=4)
            pltpu.make_async_copy(w_in, o_in, weight_sem.at[0]).start()
        if owner == 15:
            def fill_out(t, carry):
                row = pl.multiple_of(t * 16, 16)
                relayout(TENSORS[3][2], D // LANES, row, w_out, row)
                return carry

            lax.fori_loop(0, FF // 16, fill_out, 0, unroll=8)
            pltpu.make_async_copy(w_out, o_out, weight_sem.at[1]).start()
            for i in range(9):
                for j in range(D // LANES):
                    q = VEC_BASE + i * (D // LANES) + j
                    vecd_wide[i:i + 1, j * LANES:(j + 1) * LANES] = dense[q:q + 1, :]
            for j in range(D // LANES):
                q = VEC_BASE + 8 * (D // LANES) + j
                b_out[:, j * LANES:(j + 1) * LANES] = dense[q:q + 1, :]
            for j in range(FF // LANES):
                q = VEC_BASE + 9 * (D // LANES) + j
                b_in[:, j * LANES:(j + 1) * LANES] = dense[q:q + 1, :]
            vecd_buf[...] = vecd_wide[...].astype(jnp.bfloat16)
            vecf_buf[...] = b_in[...].astype(jnp.bfloat16)
            pltpu.make_async_copy(vecd_buf, o_vecd, weight_sem.at[2]).start()
            pltpu.make_async_copy(vecf_buf, o_vecf, weight_sem.at[3]).start()

    def lookup(block, h_buf, rows_buf):
        slot = lax.rem(block, ACT_SLOTS)
        token = jnp.minimum(block, blocks - 1) * SUB
        for tile in range(SUB // 8):
            for i in range(8):
                row = ids[token + tile * 8 + i] * (D // LANES)
                rows_buf[pl.ds(tile * 56 + i * 7, 8), :] = dense[pl.ds(row, 8), :]
        for pair in range(SUB // 16):
            for j in range(D // LANES):
                top = rows_buf[pl.ds(pair * 112 + j, 8, stride=7), :]
                low = rows_buf[pl.ds(pair * 112 + 56 + j, 8, stride=7), :]
                both = jnp.concatenate([top, low], axis=0) * math.sqrt(D)
                a_val = act_buf[slot, pair * 16:pair * 16 + 16, j * LANES:(j + 1) * LANES].astype(jnp.float32)
                h_buf[pair * 16:pair * 16 + 16, j * LANES:(j + 1) * LANES] = (both + a_val).astype(jnp.bfloat16)

    def widen_tokens(h_buf, u_buf):
        pre = jnp.dot(h_buf[...], w_in[...], preferred_element_type=jnp.float32) + b_in[...]
        bent = jnp.tanh(pre * (GELU_A + GELU_B * (pre * pre)))
        flat_half = 0.5 * pre
        u_buf[...] = (flat_half + flat_half * bent).astype(jnp.bfloat16)

    def narrow_tokens(it, part, u_buf):
        y_val = jnp.dot(u_buf[...], w_out[...], preferred_element_type=jnp.float32) + b_out[...]
        y_buf[lax.rem(it, 2), part * SUB:part * SUB + SUB, :] = y_val.astype(jnp.bfloat16)

    load_ids.wait()
    load_act(0).wait()
    lookup(0, h_one, rows_one)

    moves = []
    for n, (source, target) in enumerate(((m_in, m_out), (v_in, v_out), (master_in, master_out))):
        moves.append(pltpu.make_async_copy(source, state_buf, state_sem.at[2 * n]))
        moves.append(pltpu.make_async_copy(state_buf, target, state_sem.at[2 * n + 1]))

    def body(it, carry):
        for part in range(1, UNROLL):
            load_act(it * UNROLL + part).wait()

        @pl.when(it + 1 < steps)
        def _():
            load_act(it * UNROLL + UNROLL).wait()
            for part in range(UNROLL + 1, 2 * UNROLL):
                load_act(it * UNROLL + part).start()

        @pl.when(it + 2 < steps)
        def _():
            load_act(it * UNROLL + 2 * UNROLL).start()

        @pl.when(it >= 2)
        def _():
            store_y(it - 2).wait()
            store_emb(it - 2).wait()
            store_attn(it - 2).wait()

        for n, move in enumerate(moves):
            @pl.when(it == 1 + n)
            def _(n=n, move=move):
                if n:
                    moves[n - 1].wait()
                move.start()

        buffers = ((h_one, rows_one, u_one), (h_two, rows_two, u_two))
        for part in range(UNROLL):
            h_now, _, u_now = buffers[part % 2]
            h_next, rows_next, _ = buffers[(part + 1) % 2]
            lookup(it * UNROLL + part + 1, h_next, rows_next)
            widen_tokens(h_now, u_now)
            narrow_tokens(it, part, u_now)
        for t in range(emb_rows // 16):
            relayout(TENSORS[0][2], D // LANES, it * emb_rows + t * 16, emb_buf.at[lax.rem(it, 2)], t * 16)
        for t in range(attn_rows // 16):
            relayout(TENSORS[1][2], D // LANES, it * attn_rows + t * 16, attn_buf.at[lax.rem(it, 2)], t * 16)
        store_y(it).start()
        store_emb(it).start()
        store_attn(it).start()
        return carry

    lax.fori_loop(0, steps, body, 0)
    for it in (steps - 2, steps - 1):
        store_y(it).wait()
        store_emb(it).wait()
        store_attn(it).wait()
    moves[-1].wait()
    pltpu.make_async_copy(w_in, o_in, weight_sem.at[0]).wait()
    pltpu.make_async_copy(w_out, o_out, weight_sem.at[1]).wait()
    pltpu.make_async_copy(vecd_buf, o_vecd, weight_sem.at[2]).wait()
    pltpu.make_async_copy(vecf_buf, o_vecf, weight_sem.at[3]).wait()


def ffn(ids, act, flat, m_new, v_new, w_new):
    tokens = act.shape[0]
    steps = tokens // CHUNK
    f32, bf16 = jnp.float32, jnp.bfloat16
    shape = jax.ShapeDtypeStruct
    dma = pltpu.SemaphoreType.DMA
    anywhere = pl.BlockSpec(memory_space=pl.ANY)
    state = shape((SHARD, LANES), f32)
    return pl.pallas_call(
        functools.partial(ffn_kernel, steps),
        out_shape=(shape((tokens, D), bf16), shape((VOCAB, D), bf16), shape((4 * D, D), bf16), shape((D, FF), bf16),
                   shape((FF, D), bf16), shape((9, D), bf16), shape((1, FF), bf16), state, state, state),
        in_specs=[anywhere] * 6,
        out_specs=(anywhere,) * 10,
        scratch_shapes=[
            pltpu.SMEM((tokens,), jnp.int32),
            pltpu.VMEM((DEVICES * SHARD, LANES), f32),
            pltpu.VMEM((RING, PAD, LANES), bf16),
            pltpu.VMEM((ACT_SLOTS, SUB, D), bf16),
            pltpu.VMEM((2, CHUNK, D), bf16),
            pltpu.VMEM((D, FF), bf16),
            pltpu.VMEM((FF, D), bf16),
            pltpu.VMEM((1, FF), f32),
            pltpu.VMEM((1, D), f32),
            pltpu.VMEM((9, D), f32),
            pltpu.VMEM((9, D), bf16),
            pltpu.VMEM((1, FF), bf16),
            pltpu.VMEM((SUB * 7 + 8, LANES), f32),
            pltpu.VMEM((SUB * 7 + 8, LANES), f32),
            pltpu.VMEM((SUB, D), bf16),
            pltpu.VMEM((SUB, D), bf16),
            pltpu.VMEM((SUB, FF), bf16),
            pltpu.VMEM((SUB, FF), bf16),
            pltpu.VMEM((2, VOCAB // steps, D), bf16),
            pltpu.VMEM((2, 4 * D // steps, D), bf16),
            pltpu.VMEM((SHARD, LANES), f32),
            dma((RING,)), dma((ACT_SLOTS,)), dma((2,)), dma((2,)), dma((2,)), dma((4,)), dma((6,)), dma,
        ],
        compiler_params=pltpu.CompilerParams(vmem_limit_bytes=VMEM_MAX),
        name="ffn",
    )(ids, act, flat, m_new, v_new, w_new)


def solution(mesh):
    def device_step(g_emb, g_attn, g_in, g_out, g_vecd, g_vecf, opt_m, opt_v, master, tok_ids, act_in):
        def tiles(grad, cols):
            split = grad.reshape(-1, 8, cols // LANES, LANES)
            return split.transpose(0, 2, 1, 3).reshape(-1, 8, LANES)

        m_new, v_new, w_new, gathered = exchange(
            tiles(g_emb, D), tiles(g_attn, D), tiles(g_in, FF), tiles(g_out, D),
            g_vecd.reshape(9, 1, D), g_vecf.reshape(-1, LANES), opt_m.reshape(SHARD, LANES),
            opt_v.reshape(SHARD, LANES), master.reshape(SHARD, LANES))
        flat = gathered.reshape(DEVICES, PAD, LANES)
        y_out, wb_emb, wb_attn, wb_in, wb_out, wb_vecd, wb_vecf, m_new, v_new, w_new = ffn(
            tok_ids, act_in, flat, m_new, v_new, w_new)
        return (m_new.reshape(-1), v_new.reshape(-1), w_new.reshape(-1), wb_emb, wb_attn.reshape(1, 4, D, D),
                wb_in[None], wb_out[None], wb_vecd[None], wb_vecf, y_out)

    grad_specs = tuple(P(AXES, *([None] * (grad_rank - 1))) for grad_rank in GRAD_RANKS)
    in_specs = grad_specs + (P(AXES), P(AXES), P(AXES), P(AXES), P(AXES, None))
    out_specs = (P(AXES), P(AXES), P(AXES), P(), P(), P(), P(), P(), P(), P(AXES, None))
    return jax.shard_map(device_step, mesh=mesh, in_specs=in_specs, out_specs=out_specs, check_vma=False)
```
